8 devices in a mesh: dp: 1 (over z), ty: 2 (over y), tx: 4 (over x, core).
Axes of the slice: x: 2, y: 2, z: 1, core: 2. Of those that a mesh axis runs over, the one named last changes fastest.
Arguments:
- x_in: bfloat16 [2, 128, 4096], P(('dp', 'ty'), None, 'tx')
- w_q: bfloat16 [4096, 4096], P('tx', 'ty')
- w_k: bfloat16 [4096, 4096], P('tx', 'ty')
- w_v: bfloat16 [4096, 4096], P('tx', 'ty')
- w_o: bfloat16 [4096, 4096], P('ty', 'tx')
- w_gate: bfloat16 [4096, 11008], P('tx', 'ty')
- w_up: bfloat16 [4096, 11008], P('tx', 'ty')
- w_down: bfloat16 [11008, 4096], P('ty', 'tx')
Outputs:
- output: bfloat16 [2, 128, 4096], P(('dp', 'ty'), None, 'tx')
All inputs are finite; a program needn't handle non-finite values.
Results may differ from the reference program's by a relative error of at most 0.02.
Values are sent between devices in bfloat16 or wider.
A program may use at most 1 GiB of HBM per device.

```python
import jax
import jax.numpy as jnp
from jax import lax

NSEQ = 2
SEQ = 128
D = 4096
FF = 11008
HEADS = 32

HEAD_DIM = D // HEADS
EPS = 1e-5
THETA = 10000.0


def setup_inputs(seed: int = 0, part: int = 0) -> dict:
    root_key = jax.random.key(seed)
    act_root, weight_root = jax.random.split(root_key)
    part_key = jax.random.fold_in(act_root, part)
    key_tok, key_scale, key_shift, key_slope, key_walk = jax.random.split(part_key, 5)
    tok_noise = jax.random.normal(key_tok, (NSEQ, SEQ, D), jnp.float32)
    tok_scale = jax.random.uniform(key_scale, (NSEQ, SEQ, 1), jnp.float32, 0.5, 2.0)
    tok_shift = 0.5 * jax.random.normal(key_shift, (NSEQ, SEQ, 1), jnp.float32)
    col_slope = jax.random.uniform(key_slope, (), jnp.float32, 1.0, 2.0)
    col_pos = jnp.arange(D, dtype=jnp.float32) / D - 0.5
    col_walk = jnp.cumsum(jax.random.normal(key_walk, (D,), jnp.float32)) * (1.5 * D ** -0.5)
    col_offset = 2.0 * col_slope * col_pos + col_walk
    x_in = (tok_scale * tok_noise + tok_shift + col_offset).astype(jnp.bfloat16)
    weight_keys = jax.random.split(weight_root, 7)

    def draw_weight(key_w, fan_in, fan_out, gain_mul):
        return (gain_mul * fan_in ** -0.5 * jax.random.normal(key_w, (fan_in, fan_out), jnp.float32)).astype(jnp.bfloat16)

    return {
        "x_in": x_in,
        "w_q": draw_weight(weight_keys[0], D, D, 1.5),
        "w_k": draw_weight(weight_keys[1], D, D, 1.5),
        "w_v": draw_weight(weight_keys[2], D, D, 1.0),
        "w_o": draw_weight(weight_keys[3], D, D, 2.5),
        "w_gate": draw_weight(weight_keys[4], D, FF, 1.0),
        "w_up": draw_weight(weight_keys[5], D, FF, 1.0),
        "w_down": draw_weight(weight_keys[6], FF, D, 2.0),
    }


def layer_norm(values_bf):
    values = values_bf.astype(jnp.float32)
    mean_val = jnp.mean(values, axis=-1, keepdims=True)
    var_val = jnp.mean(values * values, axis=-1, keepdims=True) - mean_val * mean_val
    return ((values - mean_val) * lax.rsqrt(var_val + EPS)).astype(jnp.bfloat16)


def rotary(heads_bf):
    seq_len = heads_bf.shape[1]
    half_dim = HEAD_DIM // 2
    inv_freq = THETA ** (-2.0 * jnp.arange(half_dim, dtype=jnp.float32) / HEAD_DIM)
    angles = jnp.arange(seq_len, dtype=jnp.float32)[:, None] * inv_freq[None, :]
    cos_t = jnp.cos(angles)[:, None, :]
    sin_t = jnp.sin(angles)[:, None, :]
    values = heads_bf.astype(jnp.float32)
    lower_half = values[..., :half_dim]
    upper_half = values[..., half_dim:]
    return jnp.concatenate([lower_half * cos_t - upper_half * sin_t, upper_half * cos_t + lower_half * sin_t], axis=-1).astype(jnp.bfloat16)


def causal_attention(q_heads, k_heads, v_heads):
    seq_len = q_heads.shape[1]
    q_block = min(seq_len, 128)
    key_pos = jnp.arange(seq_len)
    k_vals = k_heads.astype(jnp.float32)
    v_vals = v_heads.astype(jnp.float32)

    def one_block(block_idx, out_acc):
        q_start = block_idx * q_block
        q_blk = lax.dynamic_slice_in_dim(q_heads, q_start, q_block, axis=1).astype(jnp.float32)
        scores = jnp.einsum("nqhd,nkhd->nhqk", q_blk, k_vals) * HEAD_DIM ** -0.5
        q_pos = q_start + jnp.arange(q_block)
        allowed = q_pos[:, None] >= key_pos[None, :]
        scores = jnp.where(allowed, scores, -1e30)
        prob_blk = jax.nn.softmax(scores, axis=-1).astype(jnp.bfloat16).astype(jnp.float32)
        blk_out = jnp.einsum("nhqk,nkhd->nqhd", prob_blk, v_vals).astype(jnp.bfloat16)
        return lax.dynamic_update_slice_in_dim(out_acc, blk_out, q_start, axis=1)

    return lax.fori_loop(0, seq_len // q_block, one_block, jnp.zeros_like(q_heads))


def project(rows_bf, weight):
    return jnp.dot(rows_bf, weight, preferred_element_type=jnp.float32).astype(jnp.bfloat16)


def reference(x_in, w_q, w_k, w_v, w_o, w_gate, w_up, w_down):
    n_seqs, seq_len, d_model = x_in.shape
    head_shape = (n_seqs, seq_len, HEADS, HEAD_DIM)
    x_rows = x_in.reshape(n_seqs * seq_len, d_model)
    normed = layer_norm(x_rows)
    q_heads = rotary(project(normed, w_q).reshape(head_shape))
    k_heads = rotary(project(normed, w_k).reshape(head_shape))
    v_heads = project(normed, w_v).reshape(head_shape)
    attn_heads = causal_attention(q_heads, k_heads, v_heads)
    attn_out = project(attn_heads.reshape(n_seqs * seq_len, d_model), w_o)
    resid_h = (x_rows.astype(jnp.float32) + attn_out.astype(jnp.float32)).astype(jnp.bfloat16)
    normed_mlp = layer_norm(resid_h)
    gate_val = project(normed_mlp, w_gate)
    up_val = project(normed_mlp, w_up)
    act_val = (jax.nn.silu(gate_val.astype(jnp.float32)) * up_val.astype(jnp.float32)).astype(jnp.bfloat16)
    mlp_out = project(act_val, w_down)
    y_out = (resid_h.astype(jnp.float32) + mlp_out.astype(jnp.float32)).astype(jnp.bfloat16)
    return y_out.reshape(n_seqs, seq_len, d_model)
```

```python
import numpy as np

import jax
import jax.numpy as jnp
from jax import lax
from jax.experimental import pallas as pl
from jax.experimental.pallas import tpu as pltpu
from jax.sharding import PartitionSpec as P

HEAD_DIM = 128
EPS = 1e-5
THETA = 10000.0
BF = jnp.bfloat16
F32 = jnp.float32
MESH = pl.DeviceIdType.MESH

HALF = 64
ROWS = 128
SUB = 32
FW = 1024


def dot(a, b):
    return jnp.dot(a, b, preferred_element_type=F32)


def dot_t(a, b):
    return lax.dot_general(a, b, (((1,), (1,)), ((), ())), preferred_element_type=F32)


def rotary_tables(seq_len):
    half_dim = HEAD_DIM // 2
    inv_freq = (np.float32(THETA) ** (np.float32(-2.0) * np.arange(half_dim, dtype=np.float32) / np.float32(HEAD_DIM))).astype(np.float32)
    angles = np.arange(seq_len, dtype=np.float32)[:, None] * inv_freq[None, :]
    cos_t = np.cos(angles.astype(np.float64)).astype(np.float32)
    sin_t = np.sin(angles.astype(np.float64)).astype(np.float32)
    return np.concatenate([cos_t, cos_t], 1), np.concatenate([-sin_t, sin_t], 1)


def layer_kernel(x_hbm, wq_hbm, wk_hbm, wv_hbm, wo_hbm, wg_hbm, wu_hbm, wd_hbm, cos_hbm, sin_hbm, out_hbm,
                 wbuf, wo_v, wg_v, wu_v, cos_v, sin_v, x_all, n_buf, d_send, d_recv, x_recv, k_buf, v_buf, o_all,
                 p_send, p_recv, h_buf, g_send, g_recv, g_own, gx_recv, a_all, acc, f_send, f_recv, y_buf, st1, st2,
                 ld_sem, w_sem, xy_s, xy_r, s1_s, s1_r, d_s, d_r, x_s, x_r, o_s, o_r, p_s, p_r, s2_s, s2_r,
                 g_s, g_r, gx_s, gx_r, a_s, a_r, f_s, f_r):
    dp = lax.axis_index("dp")
    y = lax.axis_index("ty")
    t = lax.axis_index("tx")
    xc = lax.div(t, 2)
    c = lax.rem(t, 2)
    width = x_hbm.shape[2]
    cols = wq_hbm.shape[1] // 4
    ff = wg_hbm.shape[1]
    n_full = ff // FW
    last_w = ff - n_full * FW
    full_width = 4 * width
    rel = [t, t + 1 - 2 * c, t + 2 - 4 * xc, 3 - t]
    peer = [(dp, y, r) for r in rel]
    other = [(dp, 1 - y, r) for r in rel]
    core_peer, x_peer, y_peer = peer[1], peer[2], other[0]

    def remote(src, dst, ss, rs, dev):
        return pltpu.make_async_remote_copy(src_ref=src, dst_ref=dst, send_sem=ss, recv_sem=rs, device_id=dev, device_id_type=MESH)

    def x_load(h):
        return pltpu.make_async_copy(x_hbm.at[0, pl.ds(h * HALF, HALF)], x_all.at[h, y], ld_sem.at[h])

    tables = [pltpu.make_async_copy(cos_hbm, cos_v, ld_sem.at[2]), pltpu.make_async_copy(sin_hbm, sin_v, ld_sem.at[3])]

    def qkv_load(r, m):
        src = (wq_hbm, wk_hbm, wv_hbm)[m].at[:, pl.ds(pl.multiple_of(rel[r] * cols, cols), cols)]
        return pltpu.make_async_copy(src, wbuf.at[r * 3 + m], w_sem.at[r * 3 + m])

    def qkv_wait(r, m):
        pltpu.make_async_copy(wq_hbm.at[:, pl.ds(0, cols)], wbuf.at[r * 3 + m], w_sem.at[r * 3 + m]).wait()

    wo_load = pltpu.make_async_copy(wo_hbm, wo_v, w_sem.at[12])

    def gu_load(i, j, w):
        src, dst = ((wg_hbm, wg_v), (wu_hbm, wu_v))[i]
        start = j * FW if isinstance(j, int) else pl.multiple_of(j * FW, FW)
        return pltpu.make_async_copy(src.at[:, pl.ds(start, w)], dst.at[:, pl.ds(start, w)], w_sem.at[16 + i * 8 + j])

    def down_load(j, nh, w):
        start = j * FW if isinstance(j, int) else pl.multiple_of(j * FW, FW)
        return pltpu.make_async_copy(wd_hbm.at[pl.ds(start, w), pl.ds(nh * 512, 512)], wbuf.at[j * 2 + nh, pl.ds(0, w)], w_sem.at[32 + j * 2 + nh])

    def xy_copy(h):
        return remote(x_all.at[h, y], x_all.at[h, y], xy_s.at[h], xy_r.at[h], y_peer)

    def s1_copy(k):
        return remote(st1.at[0], st1.at[k], s1_s.at[k], s1_r.at[k], peer[k] if k < 4 else other[k - 4])

    def d_copy(h, z, m):
        i = (h * 2 + z) * 3 + m
        return remote(d_send.at[i], d_recv.at[i], d_s.at[i], d_r.at[i], core_peer)

    def x_copy(h, m):
        i = h * 3 + m
        return remote(d_recv.at[h * 6 + m], x_recv.at[i], x_s.at[i], x_r.at[i], x_peer)

    def o_copy(h, kind):
        slot = (t, t, rel[2])[kind]
        i = h * 3 + kind
        return remote(o_all.at[h, slot], o_all.at[h, slot], o_s.at[i], o_r.at[i], (core_peer, x_peer, core_peer)[kind])

    def p_copy(h):
        return remote(p_send.at[h], p_recv.at[h], p_s.at[h], p_r.at[h], y_peer)

    def s2_copy(h, k):
        i = h * 4 + k
        return remote(st2.at[h, 0], st2.at[h, k], s2_s.at[i], s2_r.at[i], peer[k])

    def g_copy(h, j, w):
        i = h * 6 + j
        return remote(g_send.at[i, :, :, pl.ds(0, w)], g_recv.at[i, :, :, pl.ds(0, w)], g_s.at[i], g_r.at[i], core_peer)

    def gx_copy(h, j, w):
        i = h * 6 + j
        return remote(g_recv.at[i, :, pl.ds(0, SUB), pl.ds(0, w)], gx_recv.at[i, :, :, pl.ds(0, w)], gx_s.at[i], gx_r.at[i], x_peer)

    def a_copy(h, j, w, kind):
        own = c * 2 + xc
        slot = (own, own, c * 2 + 1 - xc)[kind]
        i = h * 6 + j
        ref = a_all.at[i, slot, :, pl.ds(0, w)]
        return remote(ref, ref, a_s.at[i * 3 + kind], a_r.at[i * 3 + kind], (core_peer, x_peer, core_peer)[kind])

    def f_copy(h):
        return remote(f_send.at[h], f_recv.at[h], f_s.at[h], f_r.at[h], y_peer)

    lane = lax.broadcasted_iota(jnp.int32, (128, 128), 1)
    sublane = lax.broadcasted_iota(jnp.int32, (128, 128), 0)

    def local_stats(v):
        s = jnp.sum(v, axis=1, keepdims=True)
        q = jnp.sum(v * v, axis=1, keepdims=True)
        m = jnp.where(lane == 0, s, jnp.where(lane == 1, q, 0.0))
        return m.T[0:8]

    def moments(total):
        mean = total[0:1] / full_width
        var = total[1:2] / full_width - mean * mean
        rstd = lax.rsqrt(var + EPS)
        m = jnp.where(sublane == 0, mean, jnp.where(sublane == 1, rstd, 0.0)).T
        return m[:, 0:1], m[:, 1:2]

    def x_own(h, s):
        return x_all[h, s].astype(F32)

    for h in range(2):
        x_load(h).start()
    for r in (3, 2, 1, 0):
        for m in range(3):
            qkv_load(r, m).start()
    for tb in tables:
        tb.start()
    barrier = pltpu.get_barrier_semaphore()
    for dev in peer[1:] + other:
        pl.semaphore_signal(barrier, inc=1, device_id=dev, device_id_type=MESH)
    for h in range(2):
        x_load(h).wait()
    st1[0] = local_stats(jnp.concatenate([x_own(0, y), x_own(1, y)], axis=0))
    pl.semaphore_wait(barrier, 7)
    for k in range(1, 8):
        s1_copy(k).start()
    for h in range(2):
        xy_copy(h).start()
    wo_load.start()
    for k in range(1, 4):
        s1_copy(k).wait_recv()
    mean_o, rstd_o = moments((st1[0] + st1[1]) + (st1[2] + st1[3]))
    for k in range(4, 8):
        s1_copy(k).wait_recv()
    mean_p, rstd_p = moments((st1[4] + st1[5]) + (st1[6] + st1[7]))

    def norm_rows(h, s, mean, rstd):
        sl = slice(h * HALF, (h + 1) * HALF)
        n = ((x_own(h, s) - mean[sl]) * rstd[sl]).astype(BF)
        n_buf[h, pl.ds(pl.multiple_of(s * HALF, HALF), HALF)] = n

    def qkv_block(h, r, after):
        def body(m, carry):
            if h == 0:
                qkv_wait(r, m)
            after(m, dot(n_buf[h], wbuf[r * 3 + m]))
            return carry

        lax.fori_loop(0, 3, body, 0)

    def qkv_send(h):
        def give(z):
            def after(m, res):
                d_send[(h * 2 + z) * 3 + m] = res.astype(BF)
                d_copy(h, z, m).start()
            return after

        def take(z):
            def after(m, res):
                d_copy(h, z, m).wait_recv()
                i = (h * 2 + z) * 3 + m
                d_recv[i] = (res + d_recv[i].astype(F32)).astype(BF)
                if z == 0:
                    x_copy(h, m).start()
            return after

        qkv_block(h, 3, give(0))
        qkv_block(h, 2, take(0))
        qkv_block(h, 1, give(1))
        qkv_block(h, 0, take(1))

    def rotate(v, cos2, sin2):
        f = v.astype(F32)
        return (f * cos2 + pltpu.roll(f, HEAD_DIM // 2, 1) * sin2).astype(BF)

    def attention(h):
        for m in range(3):
            x_copy(h, m).wait_recv()

        def final(m):
            return (d_recv[h * 6 + 3 + m].astype(F32) + x_recv[h * 3 + m].astype(F32)).astype(BF)

        sl = slice(h * HALF, (h + 1) * HALF)
        n_keys = (h + 1) * HALF
        cos2 = jnp.concatenate([cos_v[sl], cos_v[sl]], axis=0)
        sin2 = jnp.concatenate([sin_v[sl], sin_v[sl]], axis=0)
        q, k, v = final(0), final(1), final(2)
        for s in range(2):
            v_buf[s, sl] = v[s * HALF:(s + 1) * HALF]
        q_pos = h * HALF + lax.broadcasted_iota(jnp.int32, (HALF, n_keys), 0)
        k_pos = lax.broadcasted_iota(jnp.int32, (HALF, n_keys), 1)
        allowed = q_pos >= k_pos
        for hd in range(cols // HEAD_DIM):
            cl = slice(hd * HEAD_DIM, (hd + 1) * HEAD_DIM)
            qr = rotate(q[:, cl], cos2, sin2)
            kr = rotate(k[:, cl], cos2, sin2)
            for s in range(2):
                rs = slice(s * HALF, (s + 1) * HALF)
                k_buf[s, sl, cl] = kr[rs]
                keys = kr[rs] if h == 0 else jnp.concatenate([k_buf[s, 0:HALF, cl], kr[rs]], axis=0)
                vals = v[rs, cl] if h == 0 else jnp.concatenate([v_buf[s, 0:HALF, cl], v[rs, cl]], axis=0)
                scores = dot_t(qr[rs], keys) * (HEAD_DIM ** -0.5)
                scores = jnp.where(allowed, scores, -1e30)
                e = jnp.exp(scores - jnp.max(scores, axis=1, keepdims=True))
                prob = (e / jnp.sum(e, axis=1, keepdims=True)).astype(BF)
                o_all[h, t, rs, cl] = dot(prob, vals).astype(BF)
        o_copy(h, 1).start()
        o_copy(h, 0).start()

    def relay_o(h):
        o_copy(h, 1).wait_recv()
        o_copy(h, 2).start()

    def project_o(h):
        o_copy(h, 0).wait_recv()
        o_copy(h, 2).wait_recv()
        for nh in range(2):
            cl = slice(nh * 512, (nh + 1) * 512)
            res = jnp.zeros((ROWS, 512), F32)
            for b in range(4):
                res = res + dot(o_all[h, b], wo_v[b * cols:(b + 1) * cols, cl])
            p_send[h, :, cl] = res.astype(BF)
        p_copy(h).start()

    def residual(h):
        p_copy(h).wait_recv()
        attn = (p_send[h].astype(F32) + p_recv[h].astype(F32)).astype(BF).astype(F32)
        xv = jnp.concatenate([x_own(h, 0), x_own(h, 1)], axis=0)
        hv = (xv + attn).astype(BF)
        h_buf[h] = hv
        st2[h, 0] = local_stats(hv.astype(F32))
        for k in range(1, 4):
            s2_copy(h, k).start()

    def norm2(h):
        for k in range(1, 4):
            s2_copy(h, k).wait_recv()
        mean, rstd = moments((st2[h, 0] + st2[h, 1]) + (st2[h, 2] + st2[h, 3]))
        n = ((h_buf[h].astype(F32) - mean) * rstd).astype(BF)
        for b in range(4):
            e_c = c if b // 2 == 1 else 1 - c
            e_x = xc if b % 2 == 1 else 1 - xc
            n_buf[h, pl.ds(pl.multiple_of(64 * e_c + 32 * e_x, SUB), SUB)] = n[b * SUB:(b + 1) * SUB]

    def gu_mul(h, j, w):
        slot = lax.rem(j, 2)
        for i, wv in enumerate((wg_v, wu_v)):
            if h == 0:
                gu_load(i, j, w).wait()
            for n0 in range(0, w, 512):
                nw = min(512, w - n0)
                start = j * FW + n0 if isinstance(j, int) else pl.multiple_of(j * FW + n0, 512)
                res = dot(n_buf[h], wv[:, pl.ds(start, nw)])
                g_send[h * 6 + j, i, :, n0:n0 + nw] = res[0:64].astype(BF)
                g_own[slot, i, :, n0:n0 + nw] = res[64:128]
        g_copy(h, j, w).start()

    def gu_add(h, j, w):
        slot = lax.rem(j, 2)
        g_copy(h, j, w).wait_recv()
        i = h * 6 + j
        for k in range(2):
            g_recv[i, k, :, 0:w] = (g_own[slot, k, :, 0:w] + g_recv[i, k, :, 0:w].astype(F32)).astype(BF)
        gx_copy(h, j, w).start()

    def gate_up(h):
        gu_mul(h, 0, FW)

        def body(j, carry):
            gu_mul(h, j, FW)
            gu_add(h, j - 1, FW)
            return carry

        lax.fori_loop(1, n_full, body, 0)
        gu_mul(h, n_full, last_w)
        gu_add(h, n_full - 1, FW)
        gu_add(h, n_full, last_w)

    def act(h, j, w):
        gx_copy(h, j, w).wait_recv()
        i = h * 6 + j
        g, u = [
            (g_recv[i, k, SUB:2 * SUB, 0:w].astype(F32) + gx_recv[i, k, :, 0:w].astype(F32)).astype(BF).astype(F32)
            for k in range(2)
        ]
        a_all[i, c * 2 + xc, :, 0:w] = (g * (1.0 / (1.0 + jnp.exp(-g))) * u).astype(BF)
        a_copy(h, j, w, 1).start()
        a_copy(h, j, w, 0).start()

    def relay_a(h, j, w):
        a_copy(h, j, w, 1).wait_recv()
        a_copy(h, j, w, 2).start()

    def down(h, j, w):
        a_copy(h, j, w, 0).wait_recv()
        a_copy(h, j, w, 2).wait_recv()
        lhs = a_all[h * 6 + j, :, :, 0:w].reshape(ROWS, w)
        for nh in range(2):
            if h == 0:
                down_load(j, nh, w).wait()
            acc[h, :, nh * 512:(nh + 1) * 512] += dot(lhs, wbuf[j * 2 + nh, 0:w])

    def mlp_out(h):
        acc[h] = jnp.zeros((ROWS, width), F32)
        act(h, 0, FW)
        act(h, 1, FW)
        relay_a(h, 0, FW)

        def body(j, carry):
            act(h, j, FW)
            relay_a(h, j - 1, FW)
            down(h, j - 2, FW)
            return carry

        lax.fori_loop(2, n_full, body, 0)
        act(h, n_full, last_w)
        relay_a(h, n_full - 1, FW)
        down(h, n_full - 2, FW)
        relay_a(h, n_full, last_w)
        down(h, n_full - 1, FW)
        down(h, n_full, last_w)
        f_send[h] = acc[h, pl.ds(pl.multiple_of((1 - y) * HALF, HALF), HALF)].astype(BF)
        f_copy(h).start()

    def store_out(h):
        own = pl.ds(pl.multiple_of(y * HALF, HALF), HALF)
        f_copy(h).wait_recv()
        mlp = (acc[h, own].astype(BF).astype(F32) + f_recv[h].astype(F32)).astype(BF).astype(F32)
        y_buf[h] = (h_buf[h, own].astype(F32) + mlp).astype(BF)
        return pltpu.make_async_copy(y_buf.at[h], out_hbm.at[0, pl.ds(h * HALF, HALF)], ld_sem.at[h])

    norm_rows(0, y, mean_o, rstd_o)
    xy_copy(0).wait_recv()
    norm_rows(0, 1 - y, mean_p, rstd_p)
    qkv_send(0)
    for j in range(n_full + 1):
        for i in range(2):
            gu_load(i, j, FW if j < n_full else last_w).start()
    norm_rows(1, y, mean_o, rstd_o)
    xy_copy(1).wait_recv()
    norm_rows(1, 1 - y, mean_p, rstd_p)
    qkv_send(1)
    for j in range(n_full + 1):
        for nh in range(2):
            down_load(j, nh, FW if j < n_full else last_w).start()
    for tb in tables:
        tb.wait()
    attention(0)
    wo_load.wait()
    relay_o(0)
    project_o(0)
    attention(1)
    residual(0)
    relay_o(1)
    project_o(1)
    norm2(0)
    gate_up(0)
    residual(1)
    norm2(1)
    gate_up(1)
    mlp_out(0)
    mlp_out(1)
    stores = []
    for h in range(2):
        cp = store_out(h)
        cp.start()
        stores.append(cp)

    for k in range(1, 8):
        s1_copy(k).wait_send()
    for h in range(2):
        xy_copy(h).wait_send()
        for m in range(3):
            d_copy(h, 0, m).wait_send()
            d_copy(h, 1, m).wait_send()
            x_copy(h, m).wait_send()
            o_copy(h, m).wait_send()
            s2_copy(h, m + 1).wait_send()
        p_copy(h).wait_send()
        for j in range(n_full + 1):
            w = FW if j < n_full else last_w
            g_copy(h, j, w).wait_send()
            gx_copy(h, j, w).wait_send()
            for kind in range(3):
                a_copy(h, j, w, kind).wait_send()
        f_copy(h).wait_send()
    for cp in stores:
        cp.wait()


def solution(mesh):
    act_spec = P(("dp", "ty"), None, "tx")
    col_spec = P("tx", "ty")
    row_spec = P("ty", "tx")

    def layer_fn(x_blk, w_q, w_k, w_v, w_o, w_gate, w_up, w_down):
        seq_len, width = x_blk.shape[1:]
        cols = w_q.shape[1] // 4
        ff = w_gate.shape[1]
        cos_t, sin_t = (jnp.asarray(a) for a in rotary_tables(seq_len))
        dma = pltpu.SemaphoreType.DMA
        vm = pltpu.VMEM
        return pl.pallas_call(
            layer_kernel,
            out_shape=jax.ShapeDtypeStruct(x_blk.shape, BF),
            in_specs=[pl.BlockSpec(memory_space=pl.ANY)] * 10,
            out_specs=pl.BlockSpec(memory_space=pl.ANY),
            scratch_shapes=[
                vm((12, width, cols), BF),
                vm(w_o.shape, BF),
                vm(w_gate.shape, BF),
                vm(w_up.shape, BF),
                vm((seq_len, HEAD_DIM), F32),
                vm((seq_len, HEAD_DIM), F32),
                vm((2, 2, HALF, width), BF),
                vm((2, ROWS, width), BF),
                vm((12, ROWS, cols), BF),
                vm((12, ROWS, cols), BF),
                vm((6, ROWS, cols), BF),
                vm((2, seq_len, cols), BF),
                vm((2, seq_len, cols), BF),
                vm((2, 4, ROWS, cols), BF),
                vm((2, ROWS, width), BF),
                vm((2, ROWS, width), BF),
                vm((2, ROWS, width), BF),
                vm((12, 2, 2 * SUB, FW), BF),
                vm((12, 2, 2 * SUB, FW), BF),
                vm((2, 2, 2 * SUB, FW), F32),
                vm((12, 2, SUB, FW), BF),
                vm((12, 4, SUB, FW), BF),
                vm((2, ROWS, width), F32),
                vm((2, HALF, width), BF),
                vm((2, HALF, width), BF),
                vm((2, HALF, width), BF),
                vm((8, 8, 128), F32),
                vm((2, 4, 8, 128), F32),
                dma((4,)), dma((48,)),
                dma((2,)), dma((2,)), dma((8,)), dma((8,)), dma((12,)), dma((12,)), dma((6,)), dma((6,)),
                dma((6,)), dma((6,)), dma((2,)), dma((2,)), dma((8,)), dma((8,)), dma((12,)), dma((12,)),
                dma((12,)), dma((12,)), dma((36,)), dma((36,)), dma((2,)), dma((2,)),
            ],
            compiler_params=pltpu.CompilerParams(collective_id=0, has_side_effects=True, vmem_limit_bytes=67043328),
            name="layer",
        )(x_blk, w_q, w_k, w_v, w_o, w_gate, w_up, w_down, cos_t, sin_t)

    return jax.shard_map(layer_fn, mesh=mesh, in_specs=(act_spec, col_spec, col_spec, col_spec, row_spec, col_spec, col_spec, row_spec), out_specs=act_spec, check_vma=False)
```

```python
import numpy as np

import jax
import jax.numpy as jnp
from jax import lax
from jax.experimental import pallas as pl
from jax.experimental.pallas import tpu as pltpu
from jax.sharding import PartitionSpec as P

HEAD_DIM = 128
EPS = 1e-5
THETA = 10000.0
BF = jnp.bfloat16
F32 = jnp.float32
MESH = pl.DeviceIdType.MESH

HALF = 64
ROWS = 128
SUB = 32
FW = 1024


def dot(a, b):
    return jnp.dot(a, b, preferred_element_type=F32)


def dot_t(a, b):
    return lax.dot_general(a, b, (((1,), (1,)), ((), ())), preferred_element_type=F32)


def rotary_tables(seq_len):
    half_dim = HEAD_DIM // 2
    inv_freq = (np.float32(THETA) ** (np.float32(-2.0) * np.arange(half_dim, dtype=np.float32) / np.float32(HEAD_DIM))).astype(np.float32)
    angles = np.arange(seq_len, dtype=np.float32)[:, None] * inv_freq[None, :]
    cos_t = np.cos(angles.astype(np.float64)).astype(np.float32)
    sin_t = np.sin(angles.astype(np.float64)).astype(np.float32)
    return np.concatenate([cos_t, cos_t], 1), np.concatenate([-sin_t, sin_t], 1)


def layer_kernel(x_hbm, wq_hbm, wk_hbm, wv_hbm, wo_hbm, wg_hbm, wu_hbm, wd_hbm, cos_hbm, sin_hbm, out_hbm,
                 wbuf, wo_v, wg_v, wu_v, cos_v, sin_v, x_all, n_buf, d_send, d_recv, x_recv, k_buf, v_buf, o_all,
                 p_send, p_recv, h_buf, g_send, g_recv, g_own, gx_recv, a_all, acc, f_send, f_recv, y_buf, st1, st2,
                 ld_sem, w_sem, xy_s, xy_r, s1_s, s1_r, d_s, d_r, x_s, x_r, o_s, o_r, p_s, p_r, s2_s, s2_r,
                 g_s, g_r, gx_s, gx_r, a_s, a_r, f_s, f_r):
    dp = lax.axis_index("dp")
    y = lax.axis_index("ty")
    t = lax.axis_index("tx")
    xc = lax.div(t, 2)
    c = lax.rem(t, 2)
    width = x_hbm.shape[2]
    cols = wq_hbm.shape[1] // 4
    ff = wg_hbm.shape[1]
    n_full = ff // FW
    last_w = ff - n_full * FW
    full_width = 4 * width
    rel = [t, t + 1 - 2 * c, t + 2 - 4 * xc, 3 - t]
    peer = [(dp, y, r) for r in rel]
    other = [(dp, 1 - y, r) for r in rel]
    core_peer, x_peer, y_peer = peer[1], peer[2], other[0]

    def remote(src, dst, ss, rs, dev):
        return pltpu.make_async_remote_copy(src_ref=src, dst_ref=dst, send_sem=ss, recv_sem=rs, device_id=dev, device_id_type=MESH)

    def x_load(h):
        return pltpu.make_async_copy(x_hbm.at[0, pl.ds(h * HALF, HALF)], x_all.at[h, y], ld_sem.at[h])

    tables = [pltpu.make_async_copy(cos_hbm, cos_v, ld_sem.at[2]), pltpu.make_async_copy(sin_hbm, sin_v, ld_sem.at[3])]

    def qkv_load(r, m):
        src = (wq_hbm, wk_hbm, wv_hbm)[m].at[:, pl.ds(pl.multiple_of(rel[r] * cols, cols), cols)]
        return pltpu.make_async_copy(src, wbuf.at[r * 3 + m], w_sem.at[r * 3 + m])

    def qkv_wait(r, m):
        pltpu.make_async_copy(wq_hbm.at[:, pl.ds(0, cols)], wbuf.at[r * 3 + m], w_sem.at[r * 3 + m]).wait()

    wo_load = pltpu.make_async_copy(wo_hbm, wo_v, w_sem.at[12])

    def gu_load(i, j, w):
        src, dst = ((wg_hbm, wg_v), (wu_hbm, wu_v))[i]
        start = j * FW if isinstance(j, int) else pl.multiple_of(j * FW, FW)
        return pltpu.make_async_copy(src.at[:, pl.ds(start, w)], dst.at[:, pl.ds(start, w)], w_sem.at[16 + i * 8 + j])

    def down_load(j, nh, w):
        start = j * FW if isinstance(j, int) else pl.multiple_of(j * FW, FW)
        return pltpu.make_async_copy(wd_hbm.at[pl.ds(start, w), pl.ds(nh * 512, 512)], wbuf.at[j * 2 + nh, pl.ds(0, w)], w_sem.at[32 + j * 2 + nh])

    def xy_copy(h):
        return remote(x_all.at[h, y], x_all.at[h, y], xy_s.at[h], xy_r.at[h], y_peer)

    def s1_copy(k):
        return remote(st1.at[0], st1.at[k], s1_s.at[k], s1_r.at[k], peer[k] if k < 4 else other[k - 4])

    def seq_rows(s):
        return pl.ds(pl.multiple_of(s * HALF, HALF), HALF)

    def part_rows(part):
        return pl.ds(0, ROWS) if part is None else seq_rows(y if part == 0 else 1 - y)

    def d_copy(h, z, m, part=None):
        i = (h * 2 + z) * 3 + m
        k = i if part != 1 else 12 + m
        rows = part_rows(part)
        return remote(d_send.at[i, rows], d_recv.at[i, rows], d_s.at[k], d_r.at[k], core_peer)

    def x_copy(h, m, part=None):
        i = h * 3 + m
        k = i if part != 1 else 6 + m
        rows = part_rows(part)
        return remote(d_recv.at[h * 6 + m, rows], x_recv.at[i, rows], x_s.at[k], x_r.at[k], x_peer)

    def o_copy(h, kind, hh):
        slot = (t, t, rel[2])[kind]
        i = (h * 3 + kind) * 2 + hh
        ref = o_all.at[h, slot, :, pl.ds(hh * cols // 2, cols // 2)]
        return remote(ref, ref, o_s.at[i], o_r.at[i], (core_peer, x_peer, core_peer)[kind])

    def p_copy(h, nh):
        cl = pl.ds(nh * 512, 512)
        return remote(p_send.at[h, :, cl], p_recv.at[h, :, cl], p_s.at[h * 2 + nh], p_r.at[h * 2 + nh], y_peer)

    def s2_copy(h, k):
        i = h * 4 + k
        return remote(st2.at[h, 0], st2.at[h, k], s2_s.at[i], s2_r.at[i], peer[k])

    def g_copy(h, j, w):
        i = h * 6 + j
        return remote(g_send.at[i, :, :, pl.ds(0, w)], g_recv.at[i, :, :, pl.ds(0, w)], g_s.at[i], g_r.at[i], core_peer)

    def gx_copy(h, j, w):
        i = h * 6 + j
        return remote(g_recv.at[i, :, pl.ds(0, SUB), pl.ds(0, w)], gx_recv.at[i, :, :, pl.ds(0, w)], gx_s.at[i], gx_r.at[i], x_peer)

    def a_copy(h, j, w, kind):
        own = c * 2 + xc
        slot = (own, own, c * 2 + 1 - xc)[kind]
        i = h * 6 + j
        ref = a_all.at[i, slot, :, pl.ds(0, w)]
        return remote(ref, ref, a_s.at[i * 3 + kind], a_r.at[i * 3 + kind], (core_peer, x_peer, core_peer)[kind])

    def f_copy(h):
        return remote(f_send.at[h], f_recv.at[h], f_s.at[h], f_r.at[h], y_peer)

    lane = lax.broadcasted_iota(jnp.int32, (128, 128), 1)
    sublane = lax.broadcasted_iota(jnp.int32, (128, 128), 0)

    def local_stats(v):
        s = jnp.sum(v, axis=1, keepdims=True)
        q = jnp.sum(v * v, axis=1, keepdims=True)
        m = jnp.where(lane == 0, s, jnp.where(lane == 1, q, 0.0))
        return m.T[0:8]

    def moments(total):
        mean = total[0:1] / full_width
        var = total[1:2] / full_width - mean * mean
        rstd = lax.rsqrt(var + EPS)
        m = jnp.where(sublane == 0, mean, jnp.where(sublane == 1, rstd, 0.0)).T
        return m[:, 0:1], m[:, 1:2]

    def x_own(h, s):
        return x_all[h, s].astype(F32)

    for h in range(2):
        x_load(h).start()
    for r in (3, 2, 1, 0):
        for m in range(3):
            qkv_load(r, m).start()
    for tb in tables:
        tb.start()
    barrier = pltpu.get_barrier_semaphore()
    for dev in peer[1:] + other:
        pl.semaphore_signal(barrier, inc=1, device_id=dev, device_id_type=MESH)
    for h in range(2):
        x_load(h).wait()
    st1[0] = local_stats(jnp.concatenate([x_own(0, y), x_own(1, y)], axis=0))
    pl.semaphore_wait(barrier, 7)
    for k in range(1, 8):
        s1_copy(k).start()
    for h in range(2):
        xy_copy(h).start()
    wo_load.start()
    for k in range(1, 4):
        s1_copy(k).wait_recv()
    mean_o, rstd_o = moments((st1[0] + st1[1]) + (st1[2] + st1[3]))

    def norm_rows(h, s, mean, rstd):
        sl = slice(h * HALF, (h + 1) * HALF)
        n = ((x_own(h, s) - mean[sl]) * rstd[sl]).astype(BF)
        n_buf[h, pl.ds(pl.multiple_of(s * HALF, HALF), HALF)] = n

    def qkv_block(h, r, after, part=None, first=False):
        def body(m, carry):
            if first:
                qkv_wait(r, m)
            after(m, dot(n_buf[h, part_rows(part)], wbuf[r * 3 + m]))
            return carry

        lax.fori_loop(0, 3, body, 0)

    def give(h, z, part=None):
        def after(m, res):
            d_send[(h * 2 + z) * 3 + m, part_rows(part)] = res.astype(BF)
            d_copy(h, z, m, part).start()
        return after

    def take(h, z, part=None):
        def after(m, res):
            d_copy(h, z, m, part).wait_recv()
            i = (h * 2 + z) * 3 + m
            rows = part_rows(part)
            d_recv[i, rows] = (res + d_recv[i, rows].astype(F32)).astype(BF)
            if z == 0:
                if h == 0:
                    x_copy(h, m, part).start()
                else:
                    @pl.when(m < 2)
                    def _():
                        x_copy(h, m).start()
        return after

    def rotate(v, cos2, sin2):
        f = v.astype(F32)
        return (f * cos2 + pltpu.roll(f, HEAD_DIM // 2, 1) * sin2).astype(BF)

    def attention(h):
        for m in range(3):
            if h == 0:
                x_copy(h, m, 0).wait_recv()
                x_copy(h, m, 1).wait_recv()
            else:
                x_copy(h, m).wait_recv()

        def final(m):
            return (d_recv[h * 6 + 3 + m].astype(F32) + x_recv[h * 3 + m].astype(F32)).astype(BF)

        sl = slice(h * HALF, (h + 1) * HALF)
        n_keys = (h + 1) * HALF
        cos2 = jnp.concatenate([cos_v[sl], cos_v[sl]], axis=0)
        sin2 = jnp.concatenate([sin_v[sl], sin_v[sl]], axis=0)
        q, k, v = final(0), final(1), final(2)
        for s in range(2):
            v_buf[s, sl] = v[s * HALF:(s + 1) * HALF]
        q_pos = h * HALF + lax.broadcasted_iota(jnp.int32, (HALF, n_keys), 0)
        k_pos = lax.broadcasted_iota(jnp.int32, (HALF, n_keys), 1)
        allowed = q_pos >= k_pos
        for hd in range(cols // HEAD_DIM):
            cl = slice(hd * HEAD_DIM, (hd + 1) * HEAD_DIM)
            qr = rotate(q[:, cl], cos2, sin2)
            kr = rotate(k[:, cl], cos2, sin2)
            for s in range(2):
                rs = slice(s * HALF, (s + 1) * HALF)
                k_buf[s, sl, cl] = kr[rs]
                keys = kr[rs] if h == 0 else jnp.concatenate([k_buf[s, 0:HALF, cl], kr[rs]], axis=0)
                vals = v[rs, cl] if h == 0 else jnp.concatenate([v_buf[s, 0:HALF, cl], v[rs, cl]], axis=0)
                scores = dot_t(qr[rs], keys) * (HEAD_DIM ** -0.5)
                scores = jnp.where(allowed, scores, -1e30)
                e = jnp.exp(scores - jnp.max(scores, axis=1, keepdims=True))
                prob = (e / jnp.sum(e, axis=1, keepdims=True)).astype(BF)
                o_all[h, t, rs, cl] = dot(prob, vals).astype(BF)
            if hd % 2 == 1:
                o_copy(h, 1, hd // 2).start()
                o_copy(h, 0, hd // 2).start()

    def relay_o(h):
        for hh in range(2):
            o_copy(h, 1, hh).wait_recv()
            o_copy(h, 2, hh).start()

    def project_o(h):
        for hh in range(2):
            o_copy(h, 0, hh).wait_recv()
        for hh in range(2):
            o_copy(h, 2, hh).wait_recv()
        for nh in range(2):
            cl = slice(nh * 512, (nh + 1) * 512)
            res = jnp.zeros((ROWS, 512), F32)
            for b in range(4):
                res = res + dot(o_all[h, b], wo_v[b * cols:(b + 1) * cols, cl])
            p_send[h, :, cl] = res.astype(BF)
            p_copy(h, nh).start()

    def residual(h):
        for nh in range(2):
            p_copy(h, nh).wait_recv()
        attn = (p_send[h].astype(F32) + p_recv[h].astype(F32)).astype(BF).astype(F32)
        xv = jnp.concatenate([x_own(h, 0), x_own(h, 1)], axis=0)
        hv = (xv + attn).astype(BF)
        h_buf[h] = hv
        st2[h, 0] = local_stats(hv.astype(F32))
        for k in range(1, 4):
            s2_copy(h, k).start()

    def norm2(h):
        for k in range(1, 4):
            s2_copy(h, k).wait_recv()
        mean, rstd = moments((st2[h, 0] + st2[h, 1]) + (st2[h, 2] + st2[h, 3]))
        n = ((h_buf[h].astype(F32) - mean) * rstd).astype(BF)
        for b in range(4):
            e_c = c if b // 2 == 1 else 1 - c
            e_x = xc if b % 2 == 1 else 1 - xc
            n_buf[h, pl.ds(pl.multiple_of(64 * e_c + 32 * e_x, SUB), SUB)] = n[b * SUB:(b + 1) * SUB]

    def gu_mul(h, j, w):
        slot = lax.rem(j, 2)
        if h == 0:
            for i in range(2):
                gu_load(i, j, w).wait()
        for i, wv in enumerate((wg_v, wu_v)):
            for n0 in range(0, w, 512):
                nw = min(512, w - n0)
                start = j * FW + n0 if isinstance(j, int) else pl.multiple_of(j * FW + n0, 512)
                res = dot(n_buf[h], wv[:, pl.ds(start, nw)])
                g_send[h * 6 + j, i, :, n0:n0 + nw] = res[0:64].astype(BF)
                g_own[slot, i, :, n0:n0 + nw] = res[64:128]
        g_copy(h, j, w).start()

    def gu_add(h, j, w):
        slot = lax.rem(j, 2)
        g_copy(h, j, w).wait_recv()
        i = h * 6 + j
        for k in range(2):
            g_recv[i, k, :, 0:w] = (g_own[slot, k, :, 0:w] + g_recv[i, k, :, 0:w].astype(F32)).astype(BF)
        gx_copy(h, j, w).start()

    def gate_up(h, j0, j1, last):
        gu_mul(h, j0, FW)

        def body(j, carry):
            gu_mul(h, j, FW)
            gu_add(h, j - 1, FW)
            return carry

        lax.fori_loop(j0 + 1, j1, body, 0)
        if last:
            gu_mul(h, n_full, last_w)
        gu_add(h, j1 - 1, FW)
        if last:
            gu_add(h, n_full, last_w)

    def act(h, j, w):
        gx_copy(h, j, w).wait_recv()
        i = h * 6 + j
        g, u = [
            (g_recv[i, k, SUB:2 * SUB, 0:w].astype(F32) + gx_recv[i, k, :, 0:w].astype(F32)).astype(BF).astype(F32)
            for k in range(2)
        ]
        a_all[i, c * 2 + xc, :, 0:w] = (g * (1.0 / (1.0 + jnp.exp(-g))) * u).astype(BF)
        a_copy(h, j, w, 1).start()
        a_copy(h, j, w, 0).start()

    def relay_a(h, j, w):
        a_copy(h, j, w, 1).wait_recv()
        a_copy(h, j, w, 2).start()

    def down(h, j, w):
        a_copy(h, j, w, 0).wait_recv()
        a_copy(h, j, w, 2).wait_recv()
        if h == 0:
            for nh in range(2):
                down_load(j, nh, w).wait()
        lhs = a_all[h * 6 + j, :, :, 0:w].reshape(ROWS, w)
        for nh in range(2):
            acc[h, :, nh * 512:(nh + 1) * 512] += dot(lhs, wbuf[j * 2 + nh, 0:w])

    def act_all(h):
        def body(j, carry):
            act(h, j, FW)
            return carry

        lax.fori_loop(0, n_full, body, 0)
        act(h, n_full, last_w)

    def down_all(h, beside):
        acc[h] = jnp.zeros((ROWS, width), F32)

        def body(j, carry):
            if beside is not None:
                act(beside, j, FW)
            relay_a(h, j, FW)

            @pl.when(j > 0)
            def _():
                down(h, j - 1, FW)
            return carry

        lax.fori_loop(0, n_full, body, 0)
        if beside is not None:
            act(beside, n_full, last_w)
        relay_a(h, n_full, last_w)
        down(h, n_full - 1, FW)
        down(h, n_full, last_w)
        f_send[h] = acc[h, seq_rows(1 - y)].astype(BF)
        f_copy(h).start()

    def store_out(h):
        own = pl.ds(pl.multiple_of(y * HALF, HALF), HALF)
        f_copy(h).wait_recv()
        mlp = (acc[h, own].astype(BF).astype(F32) + f_recv[h].astype(F32)).astype(BF).astype(F32)
        y_buf[h] = (h_buf[h, own].astype(F32) + mlp).astype(BF)
        return pltpu.make_async_copy(y_buf.at[h], out_hbm.at[0, pl.ds(h * HALF, HALF)], ld_sem.at[h])

    norm_rows(0, y, mean_o, rstd_o)
    qkv_block(0, 3, give(0, 0, 0), 0, True)
    qkv_block(0, 2, take(0, 0, 0), 0, True)
    for k in range(4, 8):
        s1_copy(k).wait_recv()
    mean_p, rstd_p = moments((st1[4] + st1[5]) + (st1[6] + st1[7]))
    xy_copy(0).wait_recv()
    norm_rows(0, 1 - y, mean_p, rstd_p)
    qkv_block(0, 3, give(0, 0, 1), 1)
    qkv_block(0, 2, take(0, 0, 1), 1)
    qkv_block(0, 1, give(0, 1), None, True)
    qkv_block(0, 0, take(0, 1), None, True)
    for j in range(n_full + 1):
        for i in range(2):
            gu_load(i, j, FW if j < n_full else last_w).start()
    norm_rows(1, y, mean_o, rstd_o)
    xy_copy(1).wait_recv()
    norm_rows(1, 1 - y, mean_p, rstd_p)
    qkv_block(1, 3, give(1, 0))
    qkv_block(1, 2, take(1, 0))
    qkv_block(1, 1, give(1, 1))
    qkv_block(1, 0, take(1, 1))
    for j in range(n_full + 1):
        for nh in range(2):
            down_load(j, nh, FW if j < n_full else last_w).start()
    for tb in tables:
        tb.wait()
    attention(0)
    x_copy(1, 2).start()
    wo_load.wait()
    relay_o(0)
    project_o(0)
    attention(1)
    residual(0)
    relay_o(1)
    project_o(1)
    norm2(0)
    gate_up(0, 0, 3, False)
    residual(1)
    gate_up(0, 3, n_full, True)
    norm2(1)
    gate_up(1, 0, n_full, True)
    act_all(0)
    down_all(0, 1)
    down_all(1, None)
    stores = []
    for h in range(2):
        cp = store_out(h)
        cp.start()
        stores.append(cp)

    for k in range(1, 8):
        s1_copy(k).wait_send()
    for h in range(2):
        xy_copy(h).wait_send()
        for m in range(3):
            for part in (0, 1) if h == 0 else (None,):
                d_copy(h, 0, m, part).wait_send()
                x_copy(h, m, part).wait_send()
            d_copy(h, 1, m).wait_send()
            s2_copy(h, m + 1).wait_send()
            for k in range(2):
                o_copy(h, m, k).wait_send()
        for nh in range(2):
            p_copy(h, nh).wait_send()
        for j in range(n_full + 1):
            w = FW if j < n_full else last_w
            g_copy(h, j, w).wait_send()
            gx_copy(h, j, w).wait_send()
            for kind in range(3):
                a_copy(h, j, w, kind).wait_send()
        f_copy(h).wait_send()
    for cp in stores:
        cp.wait()


def solution(mesh):
    act_spec = P(("dp", "ty"), None, "tx")
    col_spec = P("tx", "ty")
    row_spec = P("ty", "tx")

    def layer_fn(x_blk, w_q, w_k, w_v, w_o, w_gate, w_up, w_down):
        seq_len, width = x_blk.shape[1:]
        cols = w_q.shape[1] // 4
        ff = w_gate.shape[1]
        cos_t, sin_t = (jnp.asarray(a) for a in rotary_tables(seq_len))
        dma = pltpu.SemaphoreType.DMA
        vm = pltpu.VMEM
        return pl.pallas_call(
            layer_kernel,
            out_shape=jax.ShapeDtypeStruct(x_blk.shape, BF),
            in_specs=[pl.BlockSpec(memory_space=pl.ANY)] * 10,
            out_specs=pl.BlockSpec(memory_space=pl.ANY),
            scratch_shapes=[
                vm((12, width, cols), BF),
                vm(w_o.shape, BF),
                vm(w_gate.shape, BF),
                vm(w_up.shape, BF),
                vm((seq_len, HEAD_DIM), F32),
                vm((seq_len, HEAD_DIM), F32),
                vm((2, 2, HALF, width), BF),
                vm((2, ROWS, width), BF),
                vm((12, ROWS, cols), BF),
                vm((12, ROWS, cols), BF),
                vm((6, ROWS, cols), BF),
                vm((2, seq_len, cols), BF),
                vm((2, seq_len, cols), BF),
                vm((2, 4, ROWS, cols), BF),
                vm((2, ROWS, width), BF),
                vm((2, ROWS, width), BF),
                vm((2, ROWS, width), BF),
                vm((12, 2, 2 * SUB, FW), BF),
                vm((12, 2, 2 * SUB, FW), BF),
                vm((2, 2, 2 * SUB, FW), F32),
                vm((12, 2, SUB, FW), BF),
                vm((12, 4, SUB, FW), BF),
                vm((2, ROWS, width), F32),
                vm((2, HALF, width), BF),
                vm((2, HALF, width), BF),
                vm((2, HALF, width), BF),
                vm((8, 8, 128), F32),
                vm((2, 4, 8, 128), F32),
                dma((4,)), dma((48,)),
                dma((2,)), dma((2,)), dma((8,)), dma((8,)), dma((15,)), dma((15,)), dma((9,)), dma((9,)),
                dma((12,)), dma((12,)), dma((4,)), dma((4,)), dma((8,)), dma((8,)), dma((12,)), dma((12,)),
                dma((12,)), dma((12,)), dma((36,)), dma((36,)), dma((2,)), dma((2,)),
            ],
            compiler_params=pltpu.CompilerParams(collective_id=0, has_side_effects=True, vmem_limit_bytes=67043328),
            name="layer",
        )(x_blk, w_q, w_k, w_v, w_o, w_gate, w_up, w_down, cos_t, sin_t)

    return jax.shard_map(layer_fn, mesh=mesh, in_specs=(act_spec, col_spec, col_spec, col_spec, row_spec, col_spec, col_spec, row_spec), out_specs=act_spec, check_vma=False)
```

```python
import numpy as np

import jax
import jax.numpy as jnp
from jax import lax
from jax.experimental import pallas as pl
from jax.experimental.pallas import tpu as pltpu
from jax.sharding import PartitionSpec as P

HEAD_DIM = 128
EPS = 1e-5
THETA = 10000.0
BF = jnp.bfloat16
F32 = jnp.float32
MESH = pl.DeviceIdType.MESH

NCH = 4
TOK = 32
ROWS = 2 * TOK
SUB = ROWS // 4
FW = 1024


def dot(a, b):
    return jnp.dot(a, b, preferred_element_type=F32)


def dot_t(a, b):
    return lax.dot_general(a, b, (((1,), (1,)), ((), ())), preferred_element_type=F32)


def rotary_tables(seq_len):
    half_dim = HEAD_DIM // 2
    inv_freq = (np.float32(THETA) ** (np.float32(-2.0) * np.arange(half_dim, dtype=np.float32) / np.float32(HEAD_DIM))).astype(np.float32)
    angles = np.arange(seq_len, dtype=np.float32)[:, None] * inv_freq[None, :]
    cos_t = np.cos(angles.astype(np.float64)).astype(np.float32)
    sin_t = np.sin(angles.astype(np.float64)).astype(np.float32)
    return np.concatenate([cos_t, cos_t], 1), np.concatenate([-sin_t, sin_t], 1)


def layer_kernel(x_hbm, wq_hbm, wk_hbm, wv_hbm, wo_hbm, wg_hbm, wu_hbm, wd_hbm, cos_hbm, sin_hbm, out_hbm,
                 wbuf, wo_v, wg_v, wu_v, cos_v, sin_v, x_all, n_buf, d_send, d_recv, x_recv, k_buf, v_buf, o_all,
                 p_send, p_recv, h_buf, g_send, g_recv, g_own, gx_recv, a_all, acc, f_send, f_recv, y_buf, st1, st2,
                 ld_sem, w_sem, xy_s, xy_r, s1_s, s1_r, d_s, d_r, x_s, x_r, o_s, o_r, p_s, p_r, s2_s, s2_r,
                 g_s, g_r, gx_s, gx_r, a_s, a_r, f_s, f_r):
    dp = lax.axis_index("dp")
    y = lax.axis_index("ty")
    t = lax.axis_index("tx")
    xc = lax.div(t, 2)
    c = lax.rem(t, 2)
    width = x_hbm.shape[2]
    cols = wq_hbm.shape[1] // 4
    ff = wg_hbm.shape[1]
    n_full = ff // FW
    last_w = ff - n_full * FW
    full_width = 4 * width
    rel = [t, t + 1 - 2 * c, t + 2 - 4 * xc, 3 - t]
    peer = [(dp, y, r) for r in rel]
    other = [(dp, 1 - y, r) for r in rel]
    core_peer, x_peer, y_peer = peer[1], peer[2], other[0]

    def remote(src, dst, ss, rs, dev):
        return pltpu.make_async_remote_copy(src_ref=src, dst_ref=dst, send_sem=ss, recv_sem=rs, device_id=dev, device_id_type=MESH)

    def x_load(h):
        return pltpu.make_async_copy(x_hbm.at[0, pl.ds(h * TOK, TOK)], x_all.at[h, y], ld_sem.at[h])

    tables = [pltpu.make_async_copy(cos_hbm, cos_v, ld_sem.at[NCH]), pltpu.make_async_copy(sin_hbm, sin_v, ld_sem.at[NCH + 1])]

    def qkv_load(r, m):
        src = (wq_hbm, wk_hbm, wv_hbm)[m].at[:, pl.ds(pl.multiple_of(rel[r] * cols, cols), cols)]
        return pltpu.make_async_copy(src, wbuf.at[r * 3 + m], w_sem.at[r * 3 + m])

    def qkv_wait(r, m):
        pltpu.make_async_copy(wq_hbm.at[:, pl.ds(0, cols)], wbuf.at[r * 3 + m], w_sem.at[r * 3 + m]).wait()

    wo_load = pltpu.make_async_copy(wo_hbm, wo_v, w_sem.at[12])

    def gu_load(i, j, w):
        src, dst = ((wg_hbm, wg_v), (wu_hbm, wu_v))[i]
        start = j * FW if isinstance(j, int) else pl.multiple_of(j * FW, FW)
        return pltpu.make_async_copy(src.at[:, pl.ds(start, w)], dst.at[:, pl.ds(start, w)], w_sem.at[16 + i * 8 + j])

    def down_load(j, nh, w):
        start = j * FW if isinstance(j, int) else pl.multiple_of(j * FW, FW)
        return pltpu.make_async_copy(wd_hbm.at[pl.ds(start, w), pl.ds(nh * 512, 512)], wbuf.at[j * 2 + nh, pl.ds(0, w)], w_sem.at[32 + j * 2 + nh])

    def xy_copy(h):
        return remote(x_all.at[h, y], x_all.at[h, y], xy_s.at[h], xy_r.at[h], y_peer)

    def s1_copy(k):
        return remote(st1.at[0], st1.at[k], s1_s.at[k], s1_r.at[k], peer[k] if k < 4 else other[k - 4])

    def seq_rows(s):
        return pl.ds(pl.multiple_of(s * TOK, TOK), TOK)

    def d_copy(h, z, m):
        i = (h * 2 + z) * 3 + m
        return remote(d_send.at[i], d_recv.at[i], d_s.at[i], d_r.at[i], core_peer)

    def x_copy(h, m):
        i = h * 3 + m
        return remote(d_recv.at[h * 6 + m], x_recv.at[i], x_s.at[i], x_r.at[i], x_peer)

    def o_copy(h, kind, hh):
        slot = (t, t, rel[2])[kind]
        i = (h * 3 + kind) * 2 + hh
        ref = o_all.at[h, slot, :, pl.ds(hh * cols // 2, cols // 2)]
        return remote(ref, ref, o_s.at[i], o_r.at[i], (core_peer, x_peer, core_peer)[kind])

    def p_copy(h, nh):
        cl = pl.ds(nh * 512, 512)
        return remote(p_send.at[h, :, cl], p_recv.at[h, :, cl], p_s.at[h * 2 + nh], p_r.at[h * 2 + nh], y_peer)

    def s2_copy(h, k):
        i = h * 4 + k
        return remote(st2.at[h, 0], st2.at[h, k], s2_s.at[i], s2_r.at[i], peer[k])

    def g_copy(h, j, w):
        i = h * 6 + j
        return remote(g_send.at[i, :, :, pl.ds(0, w)], g_recv.at[i, :, :, pl.ds(0, w)], g_s.at[i], g_r.at[i], core_peer)

    def gx_copy(h, j, w):
        i = h * 6 + j
        return remote(g_recv.at[i, :, pl.ds(0, SUB), pl.ds(0, w)], gx_recv.at[i, :, :, pl.ds(0, w)], gx_s.at[i], gx_r.at[i], x_peer)

    def a_copy(h, j, w, kind):
        own = c * 2 + xc
        slot = (own, own, c * 2 + 1 - xc)[kind]
        i = h * 6 + j
        ref = a_all.at[i, slot, :, pl.ds(0, w)]
        return remote(ref, ref, a_s.at[i * 3 + kind], a_r.at[i * 3 + kind], (core_peer, x_peer, core_peer)[kind])

    def f_copy(h):
        return remote(f_send.at[h], f_recv.at[h], f_s.at[h], f_r.at[h], y_peer)

    lane = lax.broadcasted_iota(jnp.int32, (128, 128), 1)
    sublane = lax.broadcasted_iota(jnp.int32, (128, 128), 0)

    def local_stats(v):
        s = jnp.sum(v, axis=1, keepdims=True)
        q = jnp.sum(v * v, axis=1, keepdims=True)
        n = v.shape[0]
        m = jnp.where(lane[0:n] == 0, s, jnp.where(lane[0:n] == 1, q, 0.0))
        if n < 128:
            m = jnp.concatenate([m, jnp.zeros((128 - n, 128), F32)], axis=0)
        return m.T[0:8]

    def moments(total):
        mean = total[0:1] / full_width
        var = total[1:2] / full_width - mean * mean
        rstd = lax.rsqrt(var + EPS)
        m = jnp.where(sublane == 0, mean, jnp.where(sublane == 1, rstd, 0.0)).T
        return m[:, 0:1], m[:, 1:2]

    def x_own(h, s):
        return x_all[h, s].astype(F32)

    for h in range(NCH):
        x_load(h).start()
    for r in (3, 2, 1, 0):
        for m in range(3):
            qkv_load(r, m).start()
    for tb in tables:
        tb.start()
    barrier = pltpu.get_barrier_semaphore()
    for dev in peer[1:] + other:
        pl.semaphore_signal(barrier, inc=1, device_id=dev, device_id_type=MESH)
    for h in range(NCH):
        x_load(h).wait()
    st1[0] = local_stats(jnp.concatenate([x_own(h, y) for h in range(NCH)], axis=0))
    pl.semaphore_wait(barrier, 7)
    for k in range(1, 8):
        s1_copy(k).start()
    for h in range(NCH):
        xy_copy(h).start()
    wo_load.start()
    for k in range(1, 4):
        s1_copy(k).wait_recv()
    mean_o, rstd_o = moments((st1[0] + st1[1]) + (st1[2] + st1[3]))

    def norm_rows(h, s, mean, rstd):
        sl = slice(h * TOK, (h + 1) * TOK)
        n = ((x_own(h, s) - mean[sl]) * rstd[sl]).astype(BF)
        n_buf[h, pl.ds(pl.multiple_of(s * TOK, TOK), TOK)] = n

    def qkv_block(h, r, after):
        def body(m, carry):
            if h == 0:
                qkv_wait(r, m)
            after(m, dot(n_buf[h], wbuf[r * 3 + m]))
            return carry

        lax.fori_loop(0, 3, body, 0)

    def give(h, z):
        def after(m, res):
            d_send[(h * 2 + z) * 3 + m] = res.astype(BF)
            d_copy(h, z, m).start()
        return after

    def take(h, z):
        def after(m, res):
            d_copy(h, z, m).wait_recv()
            i = (h * 2 + z) * 3 + m
            d_recv[i] = (res + d_recv[i].astype(F32)).astype(BF)
            if z == 0:
                x_copy(h, m).start()
        return after

    def qkv_far(h):
        if h == 0:
            norm_rows(0, y, mean_o, rstd_o)
        xy_copy(h).wait_recv()
        norm_rows(h, 1 - y, mean_p, rstd_p)
        if h > 0:
            norm_rows(h, y, mean_o, rstd_o)
        qkv_block(h, 3, give(h, 0))
        qkv_block(h, 2, take(h, 0))

    def qkv_near(h):
        qkv_block(h, 1, give(h, 1))
        qkv_block(h, 0, take(h, 1))

    def rotate(v, cos2, sin2):
        f = v.astype(F32)
        return (f * cos2 + pltpu.roll(f, HEAD_DIM // 2, 1) * sin2).astype(BF)

    def attention(h):
        for m in range(3):
            x_copy(h, m).wait_recv()

        def final(m):
            return (d_recv[h * 6 + 3 + m].astype(F32) + x_recv[h * 3 + m].astype(F32)).astype(BF)

        sl = slice(h * TOK, (h + 1) * TOK)
        n_keys = (h + 1) * TOK
        cos2 = jnp.concatenate([cos_v[sl], cos_v[sl]], axis=0)
        sin2 = jnp.concatenate([sin_v[sl], sin_v[sl]], axis=0)
        q, k, v = final(0), final(1), final(2)
        for s in range(2):
            v_buf[s, sl] = v[s * TOK:(s + 1) * TOK]
        q_pos = h * TOK + lax.broadcasted_iota(jnp.int32, (TOK, n_keys), 0)
        k_pos = lax.broadcasted_iota(jnp.int32, (TOK, n_keys), 1)
        allowed = q_pos >= k_pos
        for hd in range(cols // HEAD_DIM):
            cl = slice(hd * HEAD_DIM, (hd + 1) * HEAD_DIM)
            qr = rotate(q[:, cl], cos2, sin2)
            kr = rotate(k[:, cl], cos2, sin2)
            for s in range(2):
                rs = slice(s * TOK, (s + 1) * TOK)
                k_buf[s, sl, cl] = kr[rs]
                keys = k_buf[s, 0:n_keys, cl]
                vals = v_buf[s, 0:n_keys, cl]
                scores = dot_t(qr[rs], keys) * (HEAD_DIM ** -0.5)
                scores = jnp.where(allowed, scores, -1e30)
                e = jnp.exp(scores - jnp.max(scores, axis=1, keepdims=True))
                prob = (e / jnp.sum(e, axis=1, keepdims=True)).astype(BF)
                o_all[h, t, rs, cl] = dot(prob, vals).astype(BF)
            if hd % 2 == 1:
                o_copy(h, 1, hd // 2).start()
                o_copy(h, 0, hd // 2).start()

    def relay_o(h, hh):
        o_copy(h, 1, hh).wait_recv()
        o_copy(h, 2, hh).start()

    def project_o(h):
        for hh in range(2):
            o_copy(h, 0, hh).wait_recv()
        for hh in range(2):
            o_copy(h, 2, hh).wait_recv()
        for nh in range(2):
            cl = slice(nh * 512, (nh + 1) * 512)
            res = jnp.zeros((ROWS, 512), F32)
            for b in range(4):
                res = res + dot(o_all[h, b], wo_v[b * cols:(b + 1) * cols, cl])
            p_send[h, :, cl] = res.astype(BF)
            p_copy(h, nh).start()

    def residual(h):
        for nh in range(2):
            p_copy(h, nh).wait_recv()
        attn = (p_send[h].astype(F32) + p_recv[h].astype(F32)).astype(BF).astype(F32)
        xv = jnp.concatenate([x_own(h, 0), x_own(h, 1)], axis=0)
        hv = (xv + attn).astype(BF)
        h_buf[h] = hv
        st2[h, 0] = local_stats(hv.astype(F32))
        for k in range(1, 4):
            s2_copy(h, k).start()

    def norm2(h):
        for k in range(1, 4):
            s2_copy(h, k).wait_recv()
        mean, rstd = moments((st2[h, 0] + st2[h, 1]) + (st2[h, 2] + st2[h, 3]))
        n = ((h_buf[h].astype(F32) - mean[0:ROWS]) * rstd[0:ROWS]).astype(BF)
        for b in range(4):
            e_c = c if b // 2 == 1 else 1 - c
            e_x = xc if b % 2 == 1 else 1 - xc
            n_buf[h, pl.ds(pl.multiple_of(2 * SUB * e_c + SUB * e_x, SUB), SUB)] = n[b * SUB:(b + 1) * SUB]

    def gu_mul(h, j, w):
        slot = (h * 6 + j) % 4 if isinstance(j, int) else lax.rem(h * 6 + j, 4)
        if h == 0:
            for i in range(2):
                gu_load(i, j, w).wait()
        for i, wv in enumerate((wg_v, wu_v)):
            for n0 in range(0, w, 512):
                nw = min(512, w - n0)
                start = j * FW + n0 if isinstance(j, int) else pl.multiple_of(j * FW + n0, 512)
                res = dot(n_buf[h], wv[:, pl.ds(start, nw)])
                g_send[h * 6 + j, i, :, n0:n0 + nw] = res[0:2 * SUB].astype(BF)
                g_own[slot, i, :, n0:n0 + nw] = res[2 * SUB:ROWS]
        g_copy(h, j, w).start()

    def gu_add(h, j, w):
        slot = (h * 6 + j) % 4 if isinstance(j, int) else lax.rem(h * 6 + j, 4)
        g_copy(h, j, w).wait_recv()
        i = h * 6 + j
        for k in range(2):
            g_recv[i, k, :, 0:w] = (g_own[slot, k, :, 0:w] + g_recv[i, k, :, 0:w].astype(F32)).astype(BF)
        gx_copy(h, j, w).start()

    def gu_loop(h, j0, j1):
        def body(j, carry):
            gu_mul(h, j, FW)

            @pl.when(j >= 2)
            def _():
                gu_add(h, j - 2, FW)
            return carry

        lax.fori_loop(j0, j1, body, 0)

    def gu_last(h):
        gu_mul(h, n_full, last_w)
        gu_add(h, n_full - 2, FW)

    def gu_flush(h):
        gu_add(h, n_full - 1, FW)
        gu_add(h, n_full, last_w)

    def act(h, j, w):
        gx_copy(h, j, w).wait_recv()
        i = h * 6 + j
        g, u = [
            (g_recv[i, k, SUB:2 * SUB, 0:w].astype(F32) + gx_recv[i, k, :, 0:w].astype(F32)).astype(BF).astype(F32)
            for k in range(2)
        ]
        a_all[i, c * 2 + xc, :, 0:w] = (g * (1.0 / (1.0 + jnp.exp(-g))) * u).astype(BF)
        a_copy(h, j, w, 1).start()
        a_copy(h, j, w, 0).start()

    def relay_a(h, j, w):
        a_copy(h, j, w, 1).wait_recv()
        a_copy(h, j, w, 2).start()

    def down(h, j, w):
        a_copy(h, j, w, 0).wait_recv()
        a_copy(h, j, w, 2).wait_recv()
        if h == 0:
            for nh in range(2):
                down_load(j, nh, w).wait()
        lhs = a_all[h * 6 + j, :, :, 0:w].reshape(ROWS, w)
        for nh in range(2):
            acc[h, :, nh * 512:(nh + 1) * 512] += dot(lhs, wbuf[j * 2 + nh, 0:w])

    def act_all(h):
        def body(j, carry):
            act(h, j, FW)
            return carry

        lax.fori_loop(0, n_full, body, 0)
        act(h, n_full, last_w)

    def down_all(h, beside):
        acc[h] = jnp.zeros((ROWS, width), F32)

        def body(j, carry):
            if beside is not None:
                act(beside, j, FW)
            relay_a(h, j, FW)

            @pl.when(j > 0)
            def _():
                down(h, j - 1, FW)
            return carry

        lax.fori_loop(0, n_full, body, 0)
        if beside is not None:
            act(beside, n_full, last_w)
        relay_a(h, n_full, last_w)
        down(h, n_full - 1, FW)
        down(h, n_full, last_w)
        f_send[h] = acc[h, seq_rows(1 - y)].astype(BF)
        f_copy(h).start()

    def store_out(h):
        own = pl.ds(pl.multiple_of(y * TOK, TOK), TOK)
        f_copy(h).wait_recv()
        mlp = (acc[h, own].astype(BF).astype(F32) + f_recv[h].astype(F32)).astype(BF).astype(F32)
        y_buf[h] = (h_buf[h, own].astype(F32) + mlp).astype(BF)
        return pltpu.make_async_copy(y_buf.at[h], out_hbm.at[0, pl.ds(h * TOK, TOK)], ld_sem.at[h])

    for k in range(4, 8):
        s1_copy(k).wait_recv()
    mean_p, rstd_p = moments((st1[4] + st1[5]) + (st1[6] + st1[7]))
    qkv_far(0)
    qkv_near(0)
    for j in range(n_full + 1):
        for i in range(2):
            gu_load(i, j, FW if j < n_full else last_w).start()
    qkv_far(1)
    qkv_near(1)
    for tb in tables:
        tb.wait()
    attention(0)
    qkv_far(2)
    attention(1)
    relay_o(0, 0)
    qkv_near(2)
    relay_o(0, 1)
    qkv_far(3)
    wo_load.wait()
    project_o(0)
    relay_o(1, 0)
    attention(2)
    relay_o(1, 1)
    qkv_near(3)
    for j in range(n_full + 1):
        for nh in range(2):
            down_load(j, nh, FW if j < n_full else last_w).start()
    project_o(1)
    residual(0)
    attention(3)
    relay_o(2, 0)
    relay_o(2, 1)
    norm2(0)
    project_o(2)
    gu_loop(0, 0, 1)
    relay_o(3, 0)
    relay_o(3, 1)
    residual(1)
    project_o(3)
    gu_loop(0, 1, 5)
    norm2(1)
    residual(2)
    gu_last(0)
    gu_loop(1, 0, 1)
    gu_flush(0)
    residual(3)
    gu_loop(1, 1, 5)
    norm2(2)
    gu_last(1)
    gu_loop(2, 0, 1)
    gu_flush(1)
    gu_loop(2, 1, 5)
    norm2(3)
    gu_last(2)
    gu_loop(3, 0, 1)
    gu_flush(2)
    gu_loop(3, 1, 5)
    gu_last(3)
    gu_flush(3)
    act_all(0)
    act_all(1)
    down_all(0, 2)
    down_all(1, 3)
    down_all(2, None)
    down_all(3, None)
    stores = []
    for h in range(NCH):
        cp = store_out(h)
        cp.start()
        stores.append(cp)

    for k in range(1, 8):
        s1_copy(k).wait_send()
    for h in range(NCH):
        xy_copy(h).wait_send()
        for m in range(3):
            d_copy(h, 0, m).wait_send()
            d_copy(h, 1, m).wait_send()
            x_copy(h, m).wait_send()
            s2_copy(h, m + 1).wait_send()
            for k in range(2):
                o_copy(h, m, k).wait_send()
        for nh in range(2):
            p_copy(h, nh).wait_send()
        for j in range(n_full + 1):
            w = FW if j < n_full else last_w
            g_copy(h, j, w).wait_send()
            gx_copy(h, j, w).wait_send()
            for kind in range(3):
                a_copy(h, j, w, kind).wait_send()
        f_copy(h).wait_send()
    for cp in stores:
        cp.wait()


def solution(mesh):
    act_spec = P(("dp", "ty"), None, "tx")
    col_spec = P("tx", "ty")
    row_spec = P("ty", "tx")

    def layer_fn(x_blk, w_q, w_k, w_v, w_o, w_gate, w_up, w_down):
        seq_len, width = x_blk.shape[1:]
        cols = w_q.shape[1] // 4
        ff = w_gate.shape[1]
        cos_t, sin_t = (jnp.asarray(a) for a in rotary_tables(seq_len))
        dma = pltpu.SemaphoreType.DMA
        vm = pltpu.VMEM
        return pl.pallas_call(
            layer_kernel,
            out_shape=jax.ShapeDtypeStruct(x_blk.shape, BF),
            in_specs=[pl.BlockSpec(memory_space=pl.ANY)] * 10,
            out_specs=pl.BlockSpec(memory_space=pl.ANY),
            scratch_shapes=[
                vm((12, width, cols), BF),
                vm(w_o.shape, BF),
                vm(w_gate.shape, BF),
                vm(w_up.shape, BF),
                vm((seq_len, HEAD_DIM), F32),
                vm((seq_len, HEAD_DIM), F32),
                vm((NCH, 2, TOK, width), BF),
                vm((NCH, ROWS, width), BF),
                vm((6 * NCH, ROWS, cols), BF),
                vm((6 * NCH, ROWS, cols), BF),
                vm((3 * NCH, ROWS, cols), BF),
                vm((2, seq_len, cols), BF),
                vm((2, seq_len, cols), BF),
                vm((NCH, 4, ROWS, cols), BF),
                vm((NCH, ROWS, width), BF),
                vm((NCH, ROWS, width), BF),
                vm((NCH, ROWS, width), BF),
                vm((6 * NCH, 2, 2 * SUB, FW), BF),
                vm((6 * NCH, 2, 2 * SUB, FW), BF),
                vm((4, 2, 2 * SUB, FW), F32),
                vm((6 * NCH, 2, SUB, FW), BF),
                vm((6 * NCH, 4, SUB, FW), BF),
                vm((NCH, ROWS, width), F32),
                vm((NCH, TOK, width), BF),
                vm((NCH, TOK, width), BF),
                vm((NCH, TOK, width), BF),
                vm((8, 8, 128), F32),
                vm((NCH, 4, 8, 128), F32),
                dma((NCH + 2,)), dma((48,)),
                *(dma((n,)) for n in (NCH, 8, 6 * NCH, 3 * NCH, 6 * NCH, 2 * NCH, 4 * NCH, 6 * NCH, 6 * NCH, 18 * NCH, NCH) for _ in range(2)),
            ],
            compiler_params=pltpu.CompilerParams(collective_id=0, has_side_effects=True, vmem_limit_bytes=67043328),
            name="layer",
        )(x_blk, w_q, w_k, w_v, w_o, w_gate, w_up, w_down, cos_t, sin_t)

    return jax.shard_map(layer_fn, mesh=mesh, in_specs=(act_spec, col_spec, col_spec, col_spec, row_spec, col_spec, col_spec, row_spec), out_specs=act_spec, check_vma=False)
```

```python
import numpy as np

import jax
import jax.numpy as jnp
from jax import lax
from jax.experimental import pallas as pl
from jax.experimental.pallas import tpu as pltpu
from jax.sharding import PartitionSpec as P

HEAD_DIM = 128
EPS = 1e-5
THETA = 10000.0
BF = jnp.bfloat16
F32 = jnp.float32
MESH = pl.DeviceIdType.MESH

NCH = 4
TOK = 32
ROWS = 2 * TOK
SUB = ROWS // 4
FW = 1024


def dot(a, b):
    return jnp.dot(a, b, preferred_element_type=F32)


def dot_t(a, b):
    return lax.dot_general(a, b, (((1,), (1,)), ((), ())), preferred_element_type=F32)


def rotary_tables(seq_len):
    half_dim = HEAD_DIM // 2
    inv_freq = (np.float32(THETA) ** (np.float32(-2.0) * np.arange(half_dim, dtype=np.float32) / np.float32(HEAD_DIM))).astype(np.float32)
    angles = np.arange(seq_len, dtype=np.float32)[:, None] * inv_freq[None, :]
    cos_t = np.cos(angles.astype(np.float64)).astype(np.float32)
    sin_t = np.sin(angles.astype(np.float64)).astype(np.float32)
    return np.concatenate([cos_t, cos_t], 1), np.concatenate([-sin_t, sin_t], 1)


def layer_kernel(x_hbm, wq_hbm, wk_hbm, wv_hbm, wo_hbm, wg_hbm, wu_hbm, wd_hbm, cos_hbm, sin_hbm, out_hbm,
                 wbuf, wo_v, wg_v, wu_v, cos_v, sin_v, x_all, n_buf, d_send, d_recv, x_recv, k_buf, v_buf, o_all,
                 p_send, p_recv, h_buf, g_send, g_recv, g_own, gx_recv, a_all, acc, f_send, f_recv, y_buf, st1, st2,
                 ld_sem, w_sem, xy_s, xy_r, s1_s, s1_r, d_s, d_r, x_s, x_r, o_s, o_r, p_s, p_r, s2_s, s2_r,
                 g_s, g_r, gx_s, gx_r, a_s, a_r, f_s, f_r):
    dp = lax.axis_index("dp")
    y = lax.axis_index("ty")
    t = lax.axis_index("tx")
    xc = lax.div(t, 2)
    c = lax.rem(t, 2)
    width = x_hbm.shape[2]
    cols = wq_hbm.shape[1] // 4
    ff = wg_hbm.shape[1]
    n_full = ff // FW
    last_w = ff - n_full * FW
    full_width = 4 * width
    rel = [t, t + 1 - 2 * c, t + 2 - 4 * xc, 3 - t]
    peer = [(dp, y, r) for r in rel]
    other = [(dp, 1 - y, r) for r in rel]
    core_peer, x_peer, y_peer = peer[1], peer[2], other[0]

    def remote(src, dst, ss, rs, dev):
        return pltpu.make_async_remote_copy(src_ref=src, dst_ref=dst, send_sem=ss, recv_sem=rs, device_id=dev, device_id_type=MESH)

    def x_load(h):
        return pltpu.make_async_copy(x_hbm.at[0, pl.ds(h * TOK, TOK)], x_all.at[h, y], ld_sem.at[h])

    tables = [pltpu.make_async_copy(cos_hbm, cos_v, ld_sem.at[NCH]), pltpu.make_async_copy(sin_hbm, sin_v, ld_sem.at[NCH + 1])]

    def qkv_load(r, m):
        src = (wq_hbm, wk_hbm, wv_hbm)[m].at[:, pl.ds(pl.multiple_of(rel[r] * cols, cols), cols)]
        return pltpu.make_async_copy(src, wbuf.at[r * 3 + m], w_sem.at[r * 3 + m])

    def qkv_wait(r, m):
        pltpu.make_async_copy(wq_hbm.at[:, pl.ds(0, cols)], wbuf.at[r * 3 + m], w_sem.at[r * 3 + m]).wait()

    wo_load = pltpu.make_async_copy(wo_hbm, wo_v, w_sem.at[12])

    def gu_load(i, j, w):
        src, dst = ((wg_hbm, wg_v), (wu_hbm, wu_v))[i]
        start = j * FW if isinstance(j, int) else pl.multiple_of(j * FW, FW)
        return pltpu.make_async_copy(src.at[:, pl.ds(start, w)], dst.at[:, pl.ds(start, w)], w_sem.at[16 + i * 8 + j])

    def down_load(j, nh, w):
        start = j * FW if isinstance(j, int) else pl.multiple_of(j * FW, FW)
        return pltpu.make_async_copy(wd_hbm.at[pl.ds(start, w), pl.ds(nh * 512, 512)], wbuf.at[j * 2 + nh, pl.ds(0, w)], w_sem.at[32 + j * 2 + nh])

    def xy_copy(h):
        return remote(x_all.at[h, y], x_all.at[h, y], xy_s.at[h], xy_r.at[h], y_peer)

    def s1_copy(k):
        return remote(st1.at[0], st1.at[k], s1_s.at[k], s1_r.at[k], peer[k] if k < 4 else other[k - 4])

    def seq_rows(s):
        return pl.ds(pl.multiple_of(s * TOK, TOK), TOK)

    def d_copy(h, z, m):
        i = (h * 2 + z) * 3 + m
        return remote(d_send.at[i], d_recv.at[i], d_s.at[i], d_r.at[i], core_peer)

    def x_copy(h, m):
        i = h * 3 + m
        return remote(d_recv.at[h * 6 + m], x_recv.at[i], x_s.at[i], x_r.at[i], x_peer)

    def o_copy(h, kind):
        slot = (t, t, rel[2])[kind]
        i = h * 3 + kind
        ref = o_all.at[h, slot]
        return remote(ref, ref, o_s.at[i], o_r.at[i], (core_peer, x_peer, core_peer)[kind])

    def p_copy(h, nh):
        cl = pl.ds(nh * 512, 512)
        return remote(p_send.at[h, :, cl], p_recv.at[h, :, cl], p_s.at[h * 2 + nh], p_r.at[h * 2 + nh], y_peer)

    def s2_copy(h, k):
        i = h * 4 + k
        return remote(st2.at[h, 0], st2.at[h, k], s2_s.at[i], s2_r.at[i], peer[k])

    def g_copy(h, j, w):
        i = h * 6 + j
        return remote(g_send.at[i, :, :, pl.ds(0, w)], g_recv.at[i, :, :, pl.ds(0, w)], g_s.at[i], g_r.at[i], core_peer)

    def gx_copy(h, j, w):
        i = h * 6 + j
        return remote(g_recv.at[i, :, pl.ds(0, SUB), pl.ds(0, w)], gx_recv.at[i, :, :, pl.ds(0, w)], gx_s.at[i], gx_r.at[i], x_peer)

    def a_copy(h, j, w, kind):
        own = c * 2 + xc
        slot = (own, own, c * 2 + 1 - xc)[kind]
        i = h * 6 + j
        ref = a_all.at[i, slot, :, pl.ds(0, w)]
        return remote(ref, ref, a_s.at[i * 3 + kind], a_r.at[i * 3 + kind], (core_peer, x_peer, core_peer)[kind])

    def f_copy(h):
        return remote(f_send.at[h], f_recv.at[h], f_s.at[h], f_r.at[h], y_peer)

    lane = lax.broadcasted_iota(jnp.int32, (128, 128), 1)
    sublane = lax.broadcasted_iota(jnp.int32, (128, 128), 0)

    def local_stats(v):
        s = jnp.sum(v, axis=1, keepdims=True)
        q = jnp.sum(v * v, axis=1, keepdims=True)
        n = v.shape[0]
        m = jnp.where(lane[0:n] == 0, s, jnp.where(lane[0:n] == 1, q, 0.0))
        if n < 128:
            m = jnp.concatenate([m, jnp.zeros((128 - n, 128), F32)], axis=0)
        return m.T[0:8]

    def moments(total):
        mean = total[0:1] / full_width
        var = total[1:2] / full_width - mean * mean
        rstd = lax.rsqrt(var + EPS)
        m = jnp.where(sublane == 0, mean, jnp.where(sublane == 1, rstd, 0.0)).T
        return m[:, 0:1], m[:, 1:2]

    def x_own(h, s):
        return x_all[h, s].astype(F32)

    for h in range(NCH):
        x_load(h).start()
    for r in (3, 2, 1, 0):
        for m in range(3):
            qkv_load(r, m).start()
    for tb in tables:
        tb.start()
    barrier = pltpu.get_barrier_semaphore()
    for dev in peer[1:] + other:
        pl.semaphore_signal(barrier, inc=1, device_id=dev, device_id_type=MESH)
    for h in range(NCH):
        x_load(h).wait()
    st1[0] = local_stats(jnp.concatenate([x_own(h, y) for h in range(NCH)], axis=0))
    pl.semaphore_wait(barrier, 7)
    for k in range(1, 8):
        s1_copy(k).start()
    for h in range(NCH):
        xy_copy(h).start()
    wo_load.start()
    for k in range(1, 4):
        s1_copy(k).wait_recv()
    mean_o, rstd_o = moments((st1[0] + st1[1]) + (st1[2] + st1[3]))

    def norm_rows(h, s, mean, rstd):
        sl = slice(h * TOK, (h + 1) * TOK)
        n = ((x_own(h, s) - mean[sl]) * rstd[sl]).astype(BF)
        n_buf[h, pl.ds(pl.multiple_of(s * TOK, TOK), TOK)] = n

    def qkv_block(h, r, after):
        def body(m, carry):
            if h == 0:
                qkv_wait(r, m)
            after(m, dot(n_buf[h], wbuf[r * 3 + m]))
            return carry

        lax.fori_loop(0, 3, body, 0)

    def give(h, z):
        def after(m, res):
            d_send[(h * 2 + z) * 3 + m] = res.astype(BF)
            d_copy(h, z, m).start()
        return after

    def take(h, z):
        def after(m, res):
            d_copy(h, z, m).wait_recv()
            i = (h * 2 + z) * 3 + m
            d_recv[i] = (res + d_recv[i].astype(F32)).astype(BF)
            if z == 0:
                x_copy(h, m).start()
        return after

    def norm_chunk(h):
        norm_rows(h, y, mean_o, rstd_o)
        xy_copy(h).wait_recv()
        norm_rows(h, 1 - y, mean_p, rstd_p)

    def qkv_first():
        norm_chunk(0)
        qkv_block(0, 3, give(0, 0))
        qkv_block(0, 2, take(0, 0))
        qkv_block(0, 1, give(0, 1))
        qkv_block(0, 0, take(0, 1))

    def qkv_give(h):
        norm_chunk(h)
        for z in range(2):
            for m in range(3):
                d_send[(h * 2 + z) * 3 + m] = dot(n_buf[h], wbuf[(3 - 2 * z) * 3 + m]).astype(BF)
            for m in range(3):
                d_copy(h, z, m).start()

    def qkv_take(h, z):
        own = [dot(n_buf[h], wbuf[(2 - 2 * z) * 3 + m]) for m in range(3)]
        for m in range(3):
            d_copy(h, z, m).wait_recv()
        for m in range(3):
            i = (h * 2 + z) * 3 + m
            d_recv[i] = (own[m] + d_recv[i].astype(F32)).astype(BF)

    def qkv_send(h):
        for m in range(3):
            x_copy(h, m).start()

    def rotate(v, cos2, sin2):
        f = v.astype(F32)
        return (f * cos2 + pltpu.roll(f, HEAD_DIM // 2, 1) * sin2).astype(BF)

    def attention(h):
        for m in range(3):
            x_copy(h, m).wait_recv()

        def final(m):
            return (d_recv[h * 6 + 3 + m].astype(F32) + x_recv[h * 3 + m].astype(F32)).astype(BF)

        sl = slice(h * TOK, (h + 1) * TOK)
        n_keys = (h + 1) * TOK
        cos2 = jnp.concatenate([cos_v[sl], cos_v[sl]], axis=0)
        sin2 = jnp.concatenate([sin_v[sl], sin_v[sl]], axis=0)
        q, k, v = final(0), final(1), final(2)
        for s in range(2):
            v_buf[s, sl] = v[s * TOK:(s + 1) * TOK]
        heads = [slice(hd * HEAD_DIM, (hd + 1) * HEAD_DIM) for hd in range(cols // HEAD_DIM)]
        blocks = [(hd, s) for hd in range(len(heads)) for s in range(2)]
        qr = [rotate(q[:, cl], cos2, sin2) for cl in heads]
        kr = [rotate(k[:, cl], cos2, sin2) for cl in heads]
        for hd, s in blocks:
            k_buf[s, sl, heads[hd]] = kr[hd][s * TOK:(s + 1) * TOK]
        scores = jnp.concatenate(
            [dot_t(qr[hd][s * TOK:(s + 1) * TOK], k_buf[s, 0:n_keys, heads[hd]]) for hd, s in blocks], axis=0
        ) * (HEAD_DIM ** -0.5)
        q_pos = h * TOK + lax.rem(lax.broadcasted_iota(jnp.int32, scores.shape, 0), TOK)
        k_pos = lax.broadcasted_iota(jnp.int32, scores.shape, 1)
        scores = jnp.where(q_pos >= k_pos, scores, -1e30)
        e = jnp.exp(scores - jnp.max(scores, axis=1, keepdims=True))
        prob = (e / jnp.sum(e, axis=1, keepdims=True)).astype(BF)
        for i, (hd, s) in enumerate(blocks):
            o = dot(prob[i * TOK:(i + 1) * TOK], v_buf[s, 0:n_keys, heads[hd]])
            o_all[h, t, s * TOK:(s + 1) * TOK, heads[hd]] = o.astype(BF)
        o_copy(h, 1).start()
        o_copy(h, 0).start()

    def relay_o(h):
        o_copy(h, 1).wait_recv()
        o_copy(h, 2).start()

    def project_o(h):
        o_copy(h, 0).wait_recv()
        o_copy(h, 2).wait_recv()
        for nh in range(2):
            cl = slice(nh * 512, (nh + 1) * 512)
            res = jnp.zeros((ROWS, 512), F32)
            for b in range(4):
                res = res + dot(o_all[h, b], wo_v[b * cols:(b + 1) * cols, cl])
            p_send[h, :, cl] = res.astype(BF)
            p_copy(h, nh).start()

    def residual(h):
        for nh in range(2):
            p_copy(h, nh).wait_recv()
        attn = (p_send[h].astype(F32) + p_recv[h].astype(F32)).astype(BF).astype(F32)
        xv = jnp.concatenate([x_own(h, 0), x_own(h, 1)], axis=0)
        hv = (xv + attn).astype(BF)
        h_buf[h] = hv
        st2[h, 0] = local_stats(hv.astype(F32))
        for k in range(1, 4):
            s2_copy(h, k).start()

    def norm2(h):
        for k in range(1, 4):
            s2_copy(h, k).wait_recv()
        mean, rstd = moments((st2[h, 0] + st2[h, 1]) + (st2[h, 2] + st2[h, 3]))
        n = ((h_buf[h].astype(F32) - mean[0:ROWS]) * rstd[0:ROWS]).astype(BF)
        for b in range(4):
            e_c = c if b // 2 == 1 else 1 - c
            e_x = xc if b % 2 == 1 else 1 - xc
            n_buf[h, pl.ds(pl.multiple_of(2 * SUB * e_c + SUB * e_x, SUB), SUB)] = n[b * SUB:(b + 1) * SUB]

    def gu_mul(h, j, w):
        slot = (h * 6 + j) % 4 if isinstance(j, int) else lax.rem(h * 6 + j, 4)
        if h == 0:
            for i in range(2):
                gu_load(i, j, w).wait()
        for i, wv in enumerate((wg_v, wu_v)):
            for n0 in range(0, w, 512):
                nw = min(512, w - n0)
                start = j * FW + n0 if isinstance(j, int) else pl.multiple_of(j * FW + n0, 512)
                res = dot(n_buf[h], wv[:, pl.ds(start, nw)])
                g_send[h * 6 + j, i, :, n0:n0 + nw] = res[0:2 * SUB].astype(BF)
                g_own[slot, i, :, n0:n0 + nw] = res[2 * SUB:ROWS]
        g_copy(h, j, w).start()

    def gu_add(h, j, w):
        slot = (h * 6 + j) % 4 if isinstance(j, int) else lax.rem(h * 6 + j, 4)
        g_copy(h, j, w).wait_recv()
        i = h * 6 + j
        for k in range(2):
            g_recv[i, k, :, 0:w] = (g_own[slot, k, :, 0:w] + g_recv[i, k, :, 0:w].astype(F32)).astype(BF)
        gx_copy(h, j, w).start()

    def gu_loop(h, j0, j1, lag=2, first=0):
        def body(j, carry):
            gu_mul(h, j, FW)

            @pl.when(j >= lag + first)
            def _():
                gu_add(h, j - lag, FW)
            return carry

        if j1 - j0 == 1 and j0 < lag + first:
            gu_mul(h, j0, FW)
        else:
            lax.fori_loop(j0, j1, body, 0)

    def gu_last(h):
        gu_mul(h, n_full, last_w)
        gu_add(h, n_full - 2, FW)

    def gu_flush(h):
        gu_add(h, n_full - 1, FW)
        gu_add(h, n_full, last_w)

    def act(h, j, w):
        gx_copy(h, j, w).wait_recv()
        i = h * 6 + j
        g, u = [
            (g_recv[i, k, SUB:2 * SUB, 0:w].astype(F32) + gx_recv[i, k, :, 0:w].astype(F32)).astype(BF).astype(F32)
            for k in range(2)
        ]
        a_all[i, c * 2 + xc, :, 0:w] = (g * (1.0 / (1.0 + jnp.exp(-g))) * u).astype(BF)
        a_copy(h, j, w, 1).start()
        a_copy(h, j, w, 0).start()

    def relay_a(h, j, w):
        a_copy(h, j, w, 1).wait_recv()
        a_copy(h, j, w, 2).start()

    def down(h, j, w):
        a_copy(h, j, w, 0).wait_recv()
        a_copy(h, j, w, 2).wait_recv()
        if h == 0:
            for nh in range(2):
                down_load(j, nh, w).wait()
        lhs = a_all[h * 6 + j, :, :, 0:w].reshape(ROWS, w)
        for nh in range(2):
            acc[h, :, nh * 512:(nh + 1) * 512] += dot(lhs, wbuf[j * 2 + nh, 0:w])

    def act_all(h):
        def body(j, carry):
            act(h, j, FW)
            return carry

        lax.fori_loop(0, n_full, body, 0)
        act(h, n_full, last_w)

    def relay_all(h):
        def body(j, carry):
            relay_a(h, j, FW)
            return carry

        lax.fori_loop(0, n_full, body, 0)
        relay_a(h, n_full, last_w)

    def down_all(h, beside):
        acc[h] = jnp.zeros((ROWS, width), F32)

        def body(j, carry):
            act(beside, j, FW)
            down(h, j, FW)
            return carry

        lax.fori_loop(0, n_full, body, 0)
        act(beside, n_full, last_w)
        down(h, n_full, last_w)
        down_send(h)

    def down_send(h):
        f_send[h] = acc[h, seq_rows(1 - y)].astype(BF)
        f_copy(h).start()

    def relay_down(h):
        acc[h] = jnp.zeros((ROWS, width), F32)
        relay_a(h, 0, FW)
        relay_a(h, 1, FW)

        def body(j, carry):
            relay_a(h, j, FW)
            down(h, j - 2, FW)
            return carry

        lax.fori_loop(2, n_full, body, 0)
        relay_a(h, n_full, last_w)
        down(h, n_full - 2, FW)
        down(h, n_full - 1, FW)
        down(h, n_full, last_w)
        down_send(h)

    def store_out(h):
        own = pl.ds(pl.multiple_of(y * TOK, TOK), TOK)
        f_copy(h).wait_recv()
        mlp = (acc[h, own].astype(BF).astype(F32) + f_recv[h].astype(F32)).astype(BF).astype(F32)
        y_buf[h] = (h_buf[h, own].astype(F32) + mlp).astype(BF)
        return pltpu.make_async_copy(y_buf.at[h], out_hbm.at[0, pl.ds(h * TOK, TOK)], ld_sem.at[h])

    for k in range(4, 8):
        s1_copy(k).wait_recv()
    mean_p, rstd_p = moments((st1[4] + st1[5]) + (st1[6] + st1[7]))
    qkv_first()
    for j in range(n_full + 1):
        for i in range(2):
            gu_load(i, j, FW if j < n_full else last_w).start()
    qkv_give(1)
    qkv_take(1, 0)
    qkv_send(1)
    qkv_take(1, 1)
    for tb in tables:
        tb.wait()
    qkv_give(2)
    qkv_take(2, 0)
    attention(0)
    qkv_send(2)
    qkv_take(2, 1)
    qkv_give(3)
    qkv_take(3, 0)
    attention(1)
    qkv_send(3)
    relay_o(0)
    qkv_take(3, 1)
    for j in range(n_full + 1):
        for nh in range(2):
            down_load(j, nh, FW if j < n_full else last_w).start()
    wo_load.wait()
    project_o(0)
    attention(2)
    relay_o(1)
    project_o(1)
    residual(0)
    attention(3)
    norm2(0)
    gu_loop(0, 0, 1)
    relay_o(2)
    gu_add(0, 0, FW)
    project_o(2)
    residual(1)
    gu_loop(0, 1, 3, 1, 1)
    relay_o(3)
    gu_add(0, 2, FW)
    norm2(1)
    project_o(3)
    gu_loop(0, 3, 5, 2, 3)
    gu_last(0)
    residual(2)
    gu_loop(1, 0, 1)
    gu_flush(0)
    gu_loop(1, 1, 3)
    residual(3)
    norm2(2)
    gu_loop(1, 3, 5)
    gu_last(1)
    gu_flush(1)
    act_all(0)
    gu_loop(2, 0, 3)
    norm2(3)
    gu_loop(2, 3, 5)
    gu_last(2)
    gu_flush(2)
    act_all(1)
    gu_loop(3, 0, 5)
    gu_last(3)
    gu_flush(3)
    relay_all(0)
    down_all(0, 2)
    relay_all(1)
    down_all(1, 3)
    relay_down(2)
    relay_down(3)
    stores = []
    for h in range(NCH):
        cp = store_out(h)
        cp.start()
        stores.append(cp)

    for k in range(1, 8):
        s1_copy(k).wait_send()
    for h in range(NCH):
        xy_copy(h).wait_send()
        for m in range(3):
            d_copy(h, 0, m).wait_send()
            d_copy(h, 1, m).wait_send()
            x_copy(h, m).wait_send()
            s2_copy(h, m + 1).wait_send()
            o_copy(h, m).wait_send()
        for nh in range(2):
            p_copy(h, nh).wait_send()
        for j in range(n_full + 1):
            w = FW if j < n_full else last_w
            g_copy(h, j, w).wait_send()
            gx_copy(h, j, w).wait_send()
            for kind in range(3):
                a_copy(h, j, w, kind).wait_send()
        f_copy(h).wait_send()
    for cp in stores:
        cp.wait()


def solution(mesh):
    act_spec = P(("dp", "ty"), None, "tx")
    col_spec = P("tx", "ty")
    row_spec = P("ty", "tx")

    def layer_fn(x_blk, w_q, w_k, w_v, w_o, w_gate, w_up, w_down):
        seq_len, width = x_blk.shape[1:]
        cols = w_q.shape[1] // 4
        ff = w_gate.shape[1]
        cos_t, sin_t = (jnp.asarray(a) for a in rotary_tables(seq_len))
        dma = pltpu.SemaphoreType.DMA
        vm = pltpu.VMEM
        return pl.pallas_call(
            layer_kernel,
            out_shape=jax.ShapeDtypeStruct(x_blk.shape, BF),
            in_specs=[pl.BlockSpec(memory_space=pl.ANY)] * 10,
            out_specs=pl.BlockSpec(memory_space=pl.ANY),
            scratch_shapes=[
                vm((12, width, cols), BF),
                vm(w_o.shape, BF),
                vm(w_gate.shape, BF),
                vm(w_up.shape, BF),
                vm((seq_len, HEAD_DIM), F32),
                vm((seq_len, HEAD_DIM), F32),
                vm((NCH, 2, TOK, width), BF),
                vm((NCH, ROWS, width), BF),
                vm((6 * NCH, ROWS, cols), BF),
                vm((6 * NCH, ROWS, cols), BF),
                vm((3 * NCH, ROWS, cols), BF),
                vm((2, seq_len, cols), BF),
                vm((2, seq_len, cols), BF),
                vm((NCH, 4, ROWS, cols), BF),
                vm((NCH, ROWS, width), BF),
                vm((NCH, ROWS, width), BF),
                vm((NCH, ROWS, width), BF),
                vm((6 * NCH, 2, 2 * SUB, FW), BF),
                vm((6 * NCH, 2, 2 * SUB, FW), BF),
                vm((4, 2, 2 * SUB, FW), F32),
                vm((6 * NCH, 2, SUB, FW), BF),
                vm((6 * NCH, 4, SUB, FW), BF),
                vm((NCH, ROWS, width), F32),
                vm((NCH, TOK, width), BF),
                vm((NCH, TOK, width), BF),
                vm((NCH, TOK, width), BF),
                vm((8, 8, 128), F32),
                vm((NCH, 4, 8, 128), F32),
                dma((NCH + 2,)), dma((48,)),
                *(dma((n,)) for n in (NCH, 8, 6 * NCH, 3 * NCH, 3 * NCH, 2 * NCH, 4 * NCH, 6 * NCH, 6 * NCH, 18 * NCH, NCH) for _ in range(2)),
            ],
            compiler_params=pltpu.CompilerParams(collective_id=0, has_side_effects=True, vmem_limit_bytes=67043328),
            name="layer",
        )(x_blk, w_q, w_k, w_v, w_o, w_gate, w_up, w_down, cos_t, sin_t)

    return jax.shard_map(layer_fn, mesh=mesh, in_specs=(act_spec, col_spec, col_spec, col_spec, row_spec, col_spec, col_spec, row_spec), out_specs=act_spec, check_vma=False)
```

```python
import numpy as np

import jax
import jax.numpy as jnp
from jax import lax
from jax.experimental import pallas as pl
from jax.experimental.pallas import tpu as pltpu
from jax.sharding import PartitionSpec as P

HEAD_DIM = 128
EPS = 1e-5
THETA = 10000.0
BF = jnp.bfloat16
F32 = jnp.float32
MESH = pl.DeviceIdType.MESH

NCH = 4
TOK = 32
ROWS = 2 * TOK
SUB = ROWS // 4
FW = 1024

PIECES = ((1024, 2048, 2432), (3072, 2432), (3072, 2432), (2048, 2048, 1408))
ORDER = (
    ('qa', 0, 0), ('qb', 0, 0), ('qc', 0, 0), ('qa', 1, 0), ('qs', 0, 0), ('qb', 1, 0),
    ('qs', 1, 0), ('at', 0, 0), ('qc', 1, 0), ('qa', 2, 0), ('qb', 2, 0), ('qs', 2, 0),
    ('qc', 2, 0), ('qa', 3, 0), ('at', 1, 0), ('qb', 3, 0), ('qs', 3, 0), ('ro', 0, 0),
    ('pr', 0, 0), ('ro', 1, 0), ('re', 0, 0), ('pr', 1, 0), ('at', 2, 0), ('qc', 3, 0),
    ('at', 3, 0), ('n2', 0, 0), ('gm', 0, 0), ('gm', 0, 1), ('ro', 2, 0), ('ga', 0, 0),
    ('re', 1, 0), ('ga', 0, 1), ('gm', 0, 2), ('pr', 2, 0), ('n2', 1, 0), ('ro', 3, 0),
    ('ac', 0, 0), ('ga', 0, 2), ('gm', 1, 0), ('gm', 1, 1), ('ga', 1, 0), ('re', 2, 0),
    ('ga', 1, 1), ('pr', 3, 0), ('ac', 1, 0), ('n2', 2, 0), ('re', 3, 0), ('ac', 0, 2),
    ('ac', 0, 1), ('gm', 2, 0), ('n2', 3, 0), ('ga', 2, 0), ('ac', 1, 1), ('gm', 2, 1),
    ('gm', 3, 0), ('ra', 0, 1), ('ra', 0, 0), ('ga', 3, 0), ('ga', 2, 1), ('ac', 2, 0),
    ('ra', 1, 0), ('dn', 1, 0), ('dn', 0, 0), ('gm', 3, 1), ('ra', 1, 1), ('ga', 3, 1),
    ('gm', 3, 2), ('ra', 0, 2), ('dn', 1, 1), ('ga', 3, 2), ('fi', 1, 0), ('ac', 3, 0),
    ('ra', 2, 0), ('ac', 2, 1), ('dn', 0, 1), ('dn', 0, 2), ('ac', 3, 1), ('ac', 3, 2),
    ('dn', 2, 0), ('fi', 0, 0), ('ra', 3, 0), ('ra', 2, 1), ('dn', 3, 0), ('ra', 3, 1),
    ('dn', 2, 1), ('ra', 3, 2), ('fi', 2, 0), ('dn', 3, 1), ('dn', 3, 2), ('fi', 3, 0),
    ('ou', 1, 0), ('ou', 0, 0), ('ou', 2, 0), ('ou', 3, 0),
)


def dot(a, b):
    return jnp.dot(a, b, preferred_element_type=F32)


def dot_t(a, b):
    return lax.dot_general(a, b, (((1,), (1,)), ((), ())), preferred_element_type=F32)


def rotary_tables(seq_len):
    half_dim = HEAD_DIM // 2
    inv_freq = (np.float32(THETA) ** (np.float32(-2.0) * np.arange(half_dim, dtype=np.float32) / np.float32(HEAD_DIM))).astype(np.float32)
    angles = np.arange(seq_len, dtype=np.float32)[:, None] * inv_freq[None, :]
    cos_t = np.cos(angles.astype(np.float64)).astype(np.float32)
    sin_t = np.sin(angles.astype(np.float64)).astype(np.float32)
    return np.concatenate([cos_t, cos_t], 1), np.concatenate([-sin_t, sin_t], 1)


def layer_kernel(x_hbm, wq_hbm, wk_hbm, wv_hbm, wo_hbm, wg_hbm, wu_hbm, wd_hbm, cos_hbm, sin_hbm, out_hbm,
                 wbuf, wo_v, wg_v, wu_v, cos_v, sin_v, x_all, n_buf, d_send, d_recv, x_recv, k_buf, v_buf, o_all,
                 p_send, p_recv, h_buf, g_send, g_recv, g_own, gx_recv, a_all, acc, f_send, f_recv, y_buf, st1, st2,
                 ld_sem, w_sem, xy_s, xy_r, s1_s, s1_r, d_s, d_r, x_s, x_r, o_s, o_r, p_s, p_r, s2_s, s2_r,
                 g_s, g_r, gx_s, gx_r, a_s, a_r, f_s, f_r):
    dp = lax.axis_index("dp")
    y = lax.axis_index("ty")
    t = lax.axis_index("tx")
    xc = lax.div(t, 2)
    c = lax.rem(t, 2)
    width = x_hbm.shape[2]
    cols = wq_hbm.shape[1] // 4
    ff = wg_hbm.shape[1]
    n_full = ff // FW
    last_w = ff - n_full * FW
    full_width = 4 * width
    rel = [t, t + 1 - 2 * c, t + 2 - 4 * xc, 3 - t]
    peer = [(dp, y, r) for r in rel]
    other = [(dp, 1 - y, r) for r in rel]
    core_peer, x_peer, y_peer = peer[1], peer[2], other[0]

    def remote(src, dst, ss, rs, dev):
        return pltpu.make_async_remote_copy(src_ref=src, dst_ref=dst, send_sem=ss, recv_sem=rs, device_id=dev, device_id_type=MESH)

    def x_load(h):
        return pltpu.make_async_copy(x_hbm.at[0, pl.ds(h * TOK, TOK)], x_all.at[h, y], ld_sem.at[h])

    tables = [pltpu.make_async_copy(cos_hbm, cos_v, ld_sem.at[NCH]), pltpu.make_async_copy(sin_hbm, sin_v, ld_sem.at[NCH + 1])]

    def qkv_load(r, m):
        src = (wq_hbm, wk_hbm, wv_hbm)[m].at[:, pl.ds(pl.multiple_of(rel[r] * cols, cols), cols)]
        return pltpu.make_async_copy(src, wbuf.at[r * 3 + m], w_sem.at[r * 3 + m])

    def qkv_wait(r, m):
        pltpu.make_async_copy(wq_hbm.at[:, pl.ds(0, cols)], wbuf.at[r * 3 + m], w_sem.at[r * 3 + m]).wait()

    wo_load = pltpu.make_async_copy(wo_hbm, wo_v, w_sem.at[12])

    def gu_load(i, j, w):
        src, dst = ((wg_hbm, wg_v), (wu_hbm, wu_v))[i]
        start = j * FW if isinstance(j, int) else pl.multiple_of(j * FW, FW)
        return pltpu.make_async_copy(src.at[:, pl.ds(start, w)], dst.at[:, pl.ds(start, w)], w_sem.at[16 + i * 8 + j])

    def down_load(j, nh, w):
        start = j * FW if isinstance(j, int) else pl.multiple_of(j * FW, FW)
        return pltpu.make_async_copy(wd_hbm.at[pl.ds(start, w), pl.ds(nh * 512, 512)], wbuf.at[j * 2 + nh, pl.ds(0, w)], w_sem.at[32 + j * 2 + nh])

    def xy_copy(h):
        return remote(x_all.at[h, y], x_all.at[h, y], xy_s.at[h], xy_r.at[h], y_peer)

    def s1_copy(k):
        return remote(st1.at[0], st1.at[k], s1_s.at[k], s1_r.at[k], peer[k] if k < 4 else other[k - 4])

    def seq_rows(s):
        return pl.ds(pl.multiple_of(s * TOK, TOK), TOK)

    def d_copy(h, z, m=None):
        i = (h * 2 + z) * 3 + (0 if m is None else m)
        sl = pl.ds(i, 3) if m is None else i
        return remote(d_send.at[sl], d_recv.at[sl], d_s.at[i], d_r.at[i], core_peer)

    def x_copy(h, m=None):
        i = h * 3 + (0 if m is None else m)
        k = h * 6 + (0 if m is None else m)
        src, dst = (d_recv.at[pl.ds(k, 3)], x_recv.at[pl.ds(i, 3)]) if m is None else (d_recv.at[k], x_recv.at[i])
        return remote(src, dst, x_s.at[i], x_r.at[i], x_peer)

    def o_copy(h, kind):
        slot = (t, t, rel[2])[kind]
        i = h * 3 + kind
        ref = o_all.at[h, slot]
        return remote(ref, ref, o_s.at[i], o_r.at[i], (core_peer, x_peer, core_peer)[kind])

    def p_copy(h, nh):
        cl = pl.ds(nh * 512, 512)
        return remote(p_send.at[h, :, cl], p_recv.at[h, :, cl], p_s.at[h * 2 + nh], p_r.at[h * 2 + nh], y_peer)

    def s2_copy(h, k):
        i = h * 4 + k
        return remote(st2.at[h, 0], st2.at[h, k], s2_s.at[i], s2_r.at[i], peer[k])

    def piece(h, j):
        start = sum(PIECES[h][:j])
        return start, PIECES[h][j]

    def g_copy(h, j):
        cl = pl.ds(*piece(h, j))
        i = h * 4 + j
        return remote(g_send.at[h, :, :, cl], g_recv.at[h, :, :, cl], g_s.at[i], g_r.at[i], core_peer)

    def gx_copy(h, j):
        cl = pl.ds(*piece(h, j))
        i = h * 4 + j
        return remote(g_recv.at[h, :, pl.ds(0, SUB), cl], gx_recv.at[h, :, :, cl], gx_s.at[i], gx_r.at[i], x_peer)

    def a_copy(h, j, kind):
        own = c * 2 + xc
        slot = (own, own, c * 2 + 1 - xc)[kind]
        i = (h * 4 + j) * 3 + kind
        ref = a_all.at[h, slot, :, pl.ds(*piece(h, j))]
        return remote(ref, ref, a_s.at[i], a_r.at[i], (core_peer, x_peer, core_peer)[kind])

    def f_copy(h):
        return remote(f_send.at[h], f_recv.at[h], f_s.at[h], f_r.at[h], y_peer)

    lane = lax.broadcasted_iota(jnp.int32, (128, 128), 1)
    sublane = lax.broadcasted_iota(jnp.int32, (128, 128), 0)

    def local_stats(v):
        s = jnp.sum(v, axis=1, keepdims=True)
        q = jnp.sum(v * v, axis=1, keepdims=True)
        n = v.shape[0]
        m = jnp.where(lane[0:n] == 0, s, jnp.where(lane[0:n] == 1, q, 0.0))
        if n < 128:
            m = jnp.concatenate([m, jnp.zeros((128 - n, 128), F32)], axis=0)
        return m.T[0:8]

    def moments(total):
        mean = total[0:1] / full_width
        var = total[1:2] / full_width - mean * mean
        rstd = lax.rsqrt(var + EPS)
        m = jnp.where(sublane == 0, mean, jnp.where(sublane == 1, rstd, 0.0)).T
        return m[:, 0:1], m[:, 1:2]

    def x_own(h, s):
        return x_all[h, s].astype(F32)

    for h in range(NCH):
        x_load(h).start()
    for r in (3, 2, 1, 0):
        for m in range(3):
            qkv_load(r, m).start()
    for tb in tables:
        tb.start()
    barrier = pltpu.get_barrier_semaphore()
    for dev in peer[1:] + other:
        pl.semaphore_signal(barrier, inc=1, device_id=dev, device_id_type=MESH)
    for h in range(NCH):
        x_load(h).wait()
    st1[0] = local_stats(jnp.concatenate([x_own(h, y) for h in range(NCH)], axis=0))
    pl.semaphore_wait(barrier, 7)
    for k in range(1, 8):
        s1_copy(k).start()
    for h in range(NCH):
        xy_copy(h).start()
    wo_load.start()
    for k in range(1, 4):
        s1_copy(k).wait_recv()
    mean_o, rstd_o = moments((st1[0] + st1[1]) + (st1[2] + st1[3]))

    def norm_rows(h, s, mean, rstd):
        sl = slice(h * TOK, (h + 1) * TOK)
        n = ((x_own(h, s) - mean[sl]) * rstd[sl]).astype(BF)
        n_buf[h, pl.ds(pl.multiple_of(s * TOK, TOK), TOK)] = n

    def norm_chunk(h):
        norm_rows(h, y, mean_o, rstd_o)
        xy_copy(h).wait_recv()
        norm_rows(h, 1 - y, mean_p, rstd_p)

    def qkv_give(h, z):
        for m in range(3):
            d_send[(h * 2 + z) * 3 + m] = dot(n_buf[h], wbuf[(3 - 2 * z) * 3 + m]).astype(BF)
        d_copy(h, z).start()

    def qkv_take(h, z):
        own = [dot(n_buf[h], wbuf[(2 - 2 * z) * 3 + m]) for m in range(3)]
        d_copy(h, z).wait_recv()
        for m in range(3):
            i = (h * 2 + z) * 3 + m
            d_recv[i] = (own[m] + d_recv[i].astype(F32)).astype(BF)

    def step_qa(h, _):
        norm_chunk(h)
        if h > 0:
            qkv_give(h, 0)
            qkv_give(h, 1)
            return

        def body(m, carry):
            qkv_wait(3, m)
            d_send[m] = dot(n_buf[0], wbuf[9 + m]).astype(BF)
            d_copy(0, 0, m).start()
            return carry

        lax.fori_loop(0, 3, body, 0)

    def step_qb(h, _):
        if h > 0:
            qkv_take(h, 0)
            return

        def body(m, carry):
            qkv_wait(2, m)
            own = dot(n_buf[0], wbuf[6 + m])
            d_copy(0, 0, m).wait_recv()
            d_recv[m] = (own + d_recv[m].astype(F32)).astype(BF)
            x_copy(0, m).start()
            return carry

        lax.fori_loop(0, 3, body, 0)
        for m in range(3):
            qkv_wait(1, m)
        qkv_give(0, 1)

    def step_qs(h, _):
        if h > 0:
            x_copy(h).start()

    def step_qc(h, _):
        if h == 0:
            for m in range(3):
                qkv_wait(0, m)
        qkv_take(h, 1)
        if h == 0:
            for j in range(n_full + 1):
                for i in range(2):
                    gu_load(i, j, FW if j < n_full else last_w).start()
        if h == NCH - 1:
            for j in range(n_full + 1):
                for nh in range(2):
                    down_load(j, nh, FW if j < n_full else last_w).start()

    def rotate(v, cos2, sin2):
        f = v.astype(F32)
        return (f * cos2 + pltpu.roll(f, HEAD_DIM // 2, 1) * sin2).astype(BF)

    def step_at(h, _):
        for m in range(3) if h == 0 else (None,):
            x_copy(h, m).wait_recv()
        if h == 0:
            for tb in tables:
                tb.wait()

        def final(m):
            return (d_recv[h * 6 + 3 + m].astype(F32) + x_recv[h * 3 + m].astype(F32)).astype(BF)

        sl = slice(h * TOK, (h + 1) * TOK)
        n_keys = (h + 1) * TOK
        cos2 = jnp.concatenate([cos_v[sl], cos_v[sl]], axis=0)
        sin2 = jnp.concatenate([sin_v[sl], sin_v[sl]], axis=0)
        q, k, v = final(0), final(1), final(2)
        for s in range(2):
            v_buf[s, sl] = v[s * TOK:(s + 1) * TOK]
        heads = [slice(hd * HEAD_DIM, (hd + 1) * HEAD_DIM) for hd in range(cols // HEAD_DIM)]
        blocks = [(hd, s) for hd in range(len(heads)) for s in range(2)]
        qr = [rotate(q[:, cl], cos2, sin2) for cl in heads]
        kr = [rotate(k[:, cl], cos2, sin2) for cl in heads]
        for hd, s in blocks:
            k_buf[s, sl, heads[hd]] = kr[hd][s * TOK:(s + 1) * TOK]
        scores = jnp.concatenate(
            [dot_t(qr[hd][s * TOK:(s + 1) * TOK], k_buf[s, 0:n_keys, heads[hd]]) for hd, s in blocks], axis=0
        ) * (HEAD_DIM ** -0.5)
        q_pos = h * TOK + lax.rem(lax.broadcasted_iota(jnp.int32, scores.shape, 0), TOK)
        k_pos = lax.broadcasted_iota(jnp.int32, scores.shape, 1)
        scores = jnp.where(q_pos >= k_pos, scores, -1e30)
        e = jnp.exp(scores - jnp.max(scores, axis=1, keepdims=True))
        prob = (e / jnp.sum(e, axis=1, keepdims=True)).astype(BF)
        for i, (hd, s) in enumerate(blocks):
            o = dot(prob[i * TOK:(i + 1) * TOK], v_buf[s, 0:n_keys, heads[hd]])
            o_all[h, t, s * TOK:(s + 1) * TOK, heads[hd]] = o.astype(BF)
        o_copy(h, 1).start()
        o_copy(h, 0).start()

    def step_ro(h, _):
        o_copy(h, 1).wait_recv()
        o_copy(h, 2).start()

    def step_pr(h, _):
        if first_time("wo"):
            wo_load.wait()
        o_copy(h, 0).wait_recv()
        o_copy(h, 2).wait_recv()
        for nh in range(2):
            cl = slice(nh * 512, (nh + 1) * 512)
            res = jnp.zeros((ROWS, 512), F32)
            for b in range(4):
                res = res + dot(o_all[h, b], wo_v[b * cols:(b + 1) * cols, cl])
            p_send[h, :, cl] = res.astype(BF)
            p_copy(h, nh).start()

    def step_re(h, _):
        for nh in range(2):
            p_copy(h, nh).wait_recv()
        attn = (p_send[h].astype(F32) + p_recv[h].astype(F32)).astype(BF).astype(F32)
        xv = jnp.concatenate([x_own(h, 0), x_own(h, 1)], axis=0)
        hv = (xv + attn).astype(BF)
        h_buf[h] = hv
        st2[h, 0] = local_stats(hv.astype(F32))
        for k in range(1, 4):
            s2_copy(h, k).start()

    def step_n2(h, _):
        for k in range(1, 4):
            s2_copy(h, k).wait_recv()
        mean, rstd = moments((st2[h, 0] + st2[h, 1]) + (st2[h, 2] + st2[h, 3]))
        n = ((h_buf[h].astype(F32) - mean[0:ROWS]) * rstd[0:ROWS]).astype(BF)
        for b in range(4):
            e_c = c if b // 2 == 1 else 1 - c
            e_x = xc if b % 2 == 1 else 1 - xc
            n_buf[h, pl.ds(pl.multiple_of(2 * SUB * e_c + SUB * e_x, SUB), SUB)] = n[b * SUB:(b + 1) * SUB]

    def steps(h, j, body):
        start, w = piece(h, j)
        lo, n = start // FW, w // FW
        if n == 1:
            body(lo, FW)
        elif n > 1:
            def step(kb, carry):
                body(kb, FW)
                return carry

            lax.fori_loop(lo, lo + n, step, 0)
        if w % FW:
            body(lo + n, w % FW)

    def step_gm(h, j):
        if first_time("gu"):
            for kb in range(n_full + 1):
                for i in range(2):
                    gu_load(i, kb, FW if kb < n_full else last_w).wait()
        slot = own_slot[h, j]
        start = piece(h, j)[0]

        def body(kb, w):
            for i, wv in enumerate((wg_v, wu_v)):
                for n0 in range(0, w, 512):
                    nw = min(512, w - n0)
                    col = kb * FW + n0
                    if not isinstance(col, int):
                        col = pl.multiple_of(col, 512)
                    res = dot(n_buf[h], wv[:, pl.ds(col, nw)])
                    g_send[h, i, :, pl.ds(col, nw)] = res[0:2 * SUB].astype(BF)
                    g_own[slot, i, :, pl.ds(col - start, nw)] = res[2 * SUB:ROWS]

        steps(h, j, body)
        g_copy(h, j).start()

    def step_ga(h, j):
        slot = own_slot[h, j]
        start, w = piece(h, j)
        cl = slice(start, start + w)
        g_copy(h, j).wait_recv()
        for k in range(2):
            g_recv[h, k, :, cl] = (g_own[slot, k, :, 0:w] + g_recv[h, k, :, cl].astype(F32)).astype(BF)
        gx_copy(h, j).start()

    def step_ac(h, j):
        start, w = piece(h, j)
        cl = slice(start, start + w)
        gx_copy(h, j).wait_recv()
        g, u = [
            (g_recv[h, k, SUB:2 * SUB, cl].astype(F32) + gx_recv[h, k, :, cl].astype(F32)).astype(BF).astype(F32)
            for k in range(2)
        ]
        a_all[h, c * 2 + xc, :, cl] = (g * (1.0 / (1.0 + jnp.exp(-g))) * u).astype(BF)
        a_copy(h, j, 1).start()
        a_copy(h, j, 0).start()

    def step_ra(h, j):
        a_copy(h, j, 1).wait_recv()
        a_copy(h, j, 2).start()

    def step_dn(h, j):
        if first_time("down"):
            for kb in range(n_full + 1):
                for nh in range(2):
                    down_load(kb, nh, FW if kb < n_full else last_w).wait()
        a_copy(h, j, 0).wait_recv()
        a_copy(h, j, 2).wait_recv()
        if j == 0:
            acc[h] = jnp.zeros((ROWS, width), F32)

        def body(kb, w):
            col = kb * FW if isinstance(kb, int) else pl.multiple_of(kb * FW, FW)
            lhs = a_all[h, :, :, pl.ds(col, w)].reshape(ROWS, w)
            for nh in range(2):
                acc[h, :, nh * 512:(nh + 1) * 512] += dot(lhs, wbuf[kb * 2 + nh, 0:w])

        steps(h, j, body)

    def step_fi(h, _):
        f_send[h] = acc[h, seq_rows(1 - y)].astype(BF)
        f_copy(h).start()

    stores = []

    def step_ou(h, _):
        cp = store_out(h)
        cp.start()
        stores.append(cp)

    def store_out(h):
        own = pl.ds(pl.multiple_of(y * TOK, TOK), TOK)
        f_copy(h).wait_recv()
        mlp = (acc[h, own].astype(BF).astype(F32) + f_recv[h].astype(F32)).astype(BF).astype(F32)
        y_buf[h] = (h_buf[h, own].astype(F32) + mlp).astype(BF)
        return pltpu.make_async_copy(y_buf.at[h], out_hbm.at[0, pl.ds(h * TOK, TOK)], ld_sem.at[h])

    for k in range(4, 8):
        s1_copy(k).wait_recv()
    mean_p, rstd_p = moments((st1[4] + st1[5]) + (st1[6] + st1[7]))
    seen = set()

    def first_time(name):
        new = name not in seen
        seen.add(name)
        return new

    own_slot, free = {}, list(range(g_own.shape[0]))
    for name, h, j in ORDER:
        if name == "gm":
            own_slot[h, j] = free.pop(0)
        if name == "ga":
            free.append(own_slot[h, j])
    step_of = dict(qa=step_qa, qb=step_qb, qs=step_qs, qc=step_qc, at=step_at, ro=step_ro, pr=step_pr, re=step_re, n2=step_n2,
                   gm=step_gm, ga=step_ga, ac=step_ac, ra=step_ra, dn=step_dn, fi=step_fi, ou=step_ou)
    for name, h, j in ORDER:
        step_of[name](h, j)

    for k in range(1, 8):
        s1_copy(k).wait_send()
    for h in range(NCH):
        xy_copy(h).wait_send()
        for m in range(3) if h == 0 else (None,):
            d_copy(h, 0, m).wait_send()
            x_copy(h, m).wait_send()
        d_copy(h, 1).wait_send()
        for m in range(3):
            s2_copy(h, m + 1).wait_send()
            o_copy(h, m).wait_send()
        for nh in range(2):
            p_copy(h, nh).wait_send()
        for j in range(len(PIECES[h])):
            g_copy(h, j).wait_send()
            gx_copy(h, j).wait_send()
            for kind in range(3):
                a_copy(h, j, kind).wait_send()
        f_copy(h).wait_send()
    for cp in stores:
        cp.wait()


def solution(mesh):
    act_spec = P(("dp", "ty"), None, "tx")
    col_spec = P("tx", "ty")
    row_spec = P("ty", "tx")

    def layer_fn(x_blk, w_q, w_k, w_v, w_o, w_gate, w_up, w_down):
        seq_len, width = x_blk.shape[1:]
        cols = w_q.shape[1] // 4
        ff = w_gate.shape[1]
        cos_t, sin_t = (jnp.asarray(a) for a in rotary_tables(seq_len))
        dma = pltpu.SemaphoreType.DMA
        vm = pltpu.VMEM
        return pl.pallas_call(
            layer_kernel,
            out_shape=jax.ShapeDtypeStruct(x_blk.shape, BF),
            in_specs=[pl.BlockSpec(memory_space=pl.ANY)] * 10,
            out_specs=pl.BlockSpec(memory_space=pl.ANY),
            scratch_shapes=[
                vm((12, width, cols), BF),
                vm(w_o.shape, BF),
                vm(w_gate.shape, BF),
                vm(w_up.shape, BF),
                vm((seq_len, HEAD_DIM), F32),
                vm((seq_len, HEAD_DIM), F32),
                vm((NCH, 2, TOK, width), BF),
                vm((NCH, ROWS, width), BF),
                vm((6 * NCH, ROWS, cols), BF),
                vm((6 * NCH, ROWS, cols), BF),
                vm((3 * NCH, ROWS, cols), BF),
                vm((2, seq_len, cols), BF),
                vm((2, seq_len, cols), BF),
                vm((NCH, 4, ROWS, cols), BF),
                vm((NCH, ROWS, width), BF),
                vm((NCH, ROWS, width), BF),
                vm((NCH, ROWS, width), BF),
                vm((NCH, 2, 2 * SUB, ff), BF),
                vm((NCH, 2, 2 * SUB, ff), BF),
                vm((3, 2, 2 * SUB, max(max(p) for p in PIECES)), F32),
                vm((NCH, 2, SUB, ff), BF),
                vm((NCH, 4, SUB, ff), BF),
                vm((NCH, ROWS, width), F32),
                vm((NCH, TOK, width), BF),
                vm((NCH, TOK, width), BF),
                vm((NCH, TOK, width), BF),
                vm((8, 8, 128), F32),
                vm((NCH, 4, 8, 128), F32),
                dma((NCH + 2,)), dma((48,)),
                *(dma((n,)) for n in (NCH, 8, 6 * NCH, 3 * NCH, 3 * NCH, 2 * NCH, 4 * NCH, 4 * NCH, 4 * NCH, 12 * NCH, NCH) for _ in range(2)),
            ],
            compiler_params=pltpu.CompilerParams(collective_id=0, has_side_effects=True, vmem_limit_bytes=67043328),
            name="layer",
        )(x_blk, w_q, w_k, w_v, w_o, w_gate, w_up, w_down, cos_t, sin_t)

    return jax.shard_map(layer_fn, mesh=mesh, in_specs=(act_spec, col_spec, col_spec, col_spec, row_spec, col_spec, col_spec, row_spec), out_specs=act_spec, check_vma=False)
```

```python
import numpy as np

import jax
import jax.numpy as jnp
from jax import lax
from jax.experimental import pallas as pl
from jax.experimental.pallas import tpu as pltpu
from jax.sharding import PartitionSpec as P

HEAD_DIM = 128
EPS = 1e-5
THETA = 10000.0
BF = jnp.bfloat16
F32 = jnp.float32
MESH = pl.DeviceIdType.MESH

NCH = 4
TOK = 32
ROWS = 2 * TOK
SUB = ROWS // 4
FW = 1024

PIECES = ((1024, 2048, 2432), (2048, 2048, 1408), (3072, 2432), (2048, 2048, 1408))
ORDER = (
    "qa0 qb0 qs0 qa1", "qb1 qs1 qc0 qa2", "at0 qb2 qc1 qs2", "qc2 qa3 ro0 at1",
    "qb3 qs3 pr0 qc3", "ro1 pr1 re0 at2", "at3 n20 gm00 gm01", "ro2 ga00 re1 ga01",
    "ro3 gm02 ac00 pr2", "ga02 pr3 n21 ac01", "gm10 re2 ga10 ac02", "gm11 ga11 gm12 ac10",
    "re3 n22 ga12 gm20", "ac11 ra00 n23 ga20", "dn00 ra10 gm21 ga21", "gm30 ra01 ga30 ra02",
    "ac20 gm31 ga31 gm32", "ac21 dn10 ga32 ac12", "ra20 dn01 dn02 dn20", "ra11 ra21 fi0 ac30",
    "dn11 ac31 ac32 ra12", "dn21 fi2 ra30 ou0", "dn12 fi1 ra31 dn30", "ra32 dn31 dn32 fi3",
    "ou1 ou2 ou3",
)


def dot(a, b):
    return jnp.dot(a, b, preferred_element_type=F32)


def dot_t(a, b):
    return lax.dot_general(a, b, (((1,), (1,)), ((), ())), preferred_element_type=F32)


def rotary_tables(seq_len):
    half_dim = HEAD_DIM // 2
    inv_freq = (np.float32(THETA) ** (np.float32(-2.0) * np.arange(half_dim, dtype=np.float32) / np.float32(HEAD_DIM))).astype(np.float32)
    angles = np.arange(seq_len, dtype=np.float32)[:, None] * inv_freq[None, :]
    cos_t = np.cos(angles.astype(np.float64)).astype(np.float32)
    sin_t = np.sin(angles.astype(np.float64)).astype(np.float32)
    return np.concatenate([cos_t, cos_t], 1), np.concatenate([-sin_t, sin_t], 1)


def layer_kernel(x_hbm, wq_hbm, wk_hbm, wv_hbm, wo_hbm, wg_hbm, wu_hbm, wd_hbm, cos_hbm, sin_hbm, out_hbm,
                 wbuf, wo_v, wg_v, wu_v, cos_v, sin_v, x_all, n_buf, d_send, d_recv, x_recv, k_buf, v_buf, o_all,
                 p_send, p_recv, h_buf, g_send, g_recv, g_own, gx_recv, a_all, acc, f_send, f_recv, y_buf, st1, st2,
                 ld_sem, w_sem, xy_s, xy_r, s1_s, s1_r, d_s, d_r, x_s, x_r, o_s, o_r, p_s, p_r, s2_s, s2_r,
                 g_s, g_r, gx_s, gx_r, a_s, a_r, f_s, f_r):
    dp = lax.axis_index("dp")
    y = lax.axis_index("ty")
    t = lax.axis_index("tx")
    xc = lax.div(t, 2)
    c = lax.rem(t, 2)
    width = x_hbm.shape[2]
    cols = wq_hbm.shape[1] // 4
    ff = wg_hbm.shape[1]
    n_full = ff // FW
    last_w = ff - n_full * FW
    full_width = 4 * width
    rel = [t, t + 1 - 2 * c, t + 2 - 4 * xc, 3 - t]
    peer = [(dp, y, r) for r in rel]
    other = [(dp, 1 - y, r) for r in rel]
    core_peer, x_peer, y_peer = peer[1], peer[2], other[0]

    def remote(src, dst, ss, rs, dev):
        return pltpu.make_async_remote_copy(src_ref=src, dst_ref=dst, send_sem=ss, recv_sem=rs, device_id=dev, device_id_type=MESH)

    def x_load(h):
        return pltpu.make_async_copy(x_hbm.at[0, pl.ds(h * TOK, TOK)], x_all.at[h, y], ld_sem.at[h])

    tables = [pltpu.make_async_copy(cos_hbm, cos_v, ld_sem.at[NCH]), pltpu.make_async_copy(sin_hbm, sin_v, ld_sem.at[NCH + 1])]

    def qkv_load(r, m):
        src = (wq_hbm, wk_hbm, wv_hbm)[m].at[:, pl.ds(pl.multiple_of(rel[r] * cols, cols), cols)]
        return pltpu.make_async_copy(src, wbuf.at[r * 3 + m], w_sem.at[r * 3 + m])

    def qkv_wait(r, m):
        pltpu.make_async_copy(wq_hbm.at[:, pl.ds(0, cols)], wbuf.at[r * 3 + m], w_sem.at[r * 3 + m]).wait()

    wo_load = pltpu.make_async_copy(wo_hbm, wo_v, w_sem.at[12])

    def gu_load(i, j, w):
        src, dst = ((wg_hbm, wg_v), (wu_hbm, wu_v))[i]
        start = j * FW if isinstance(j, int) else pl.multiple_of(j * FW, FW)
        return pltpu.make_async_copy(src.at[:, pl.ds(start, w)], dst.at[:, pl.ds(start, w)], w_sem.at[16 + i * 8 + j])

    def down_load(j, nh, w):
        start = j * FW if isinstance(j, int) else pl.multiple_of(j * FW, FW)
        return pltpu.make_async_copy(wd_hbm.at[pl.ds(start, w), pl.ds(nh * 512, 512)], wbuf.at[j * 2 + nh, pl.ds(0, w)], w_sem.at[32 + j * 2 + nh])

    def xy_copy(h):
        return remote(x_all.at[h, y], x_all.at[h, y], xy_s.at[h], xy_r.at[h], y_peer)

    def s1_copy(k):
        return remote(st1.at[0], st1.at[k], s1_s.at[k], s1_r.at[k], peer[k] if k < 4 else other[k - 4])

    def seq_rows(s):
        return pl.ds(pl.multiple_of(s * TOK, TOK), TOK)

    def part_rows(part):
        return seq_rows(y if part == 0 else 1 - y)

    def d_copy(h, z, m=None, part=None):
        i = (h * 2 + z) * 3 + (0 if m is None else m)
        src, dst = (d_send.at[pl.ds(i, 3)], d_recv.at[pl.ds(i, 3)]) if m is None else (d_send.at[i, part_rows(part)], d_recv.at[i, part_rows(part)])
        k = 6 * NCH + m if part == 1 else i
        return remote(src, dst, d_s.at[k], d_r.at[k], core_peer)

    def x_copy(h, m=None, part=None):
        i = h * 3 + (0 if m is None else m)
        k = h * 6 + (0 if m is None else m)
        src, dst = (d_recv.at[pl.ds(k, 3)], x_recv.at[pl.ds(i, 3)]) if m is None else (d_recv.at[k, part_rows(part)], x_recv.at[i, part_rows(part)])
        n = 3 * NCH + m if part == 1 else i
        return remote(src, dst, x_s.at[n], x_r.at[n], x_peer)

    def o_copy(h, kind):
        slot = (t, t, rel[2])[kind]
        i = h * 3 + kind
        ref = o_all.at[h, slot]
        return remote(ref, ref, o_s.at[i], o_r.at[i], (core_peer, x_peer, core_peer)[kind])

    def p_copy(h, nh):
        cl = pl.ds(nh * 512, 512)
        return remote(p_send.at[h, :, cl], p_recv.at[h, :, cl], p_s.at[h * 2 + nh], p_r.at[h * 2 + nh], y_peer)

    def s2_copy(h, k):
        i = h * 4 + k
        return remote(st2.at[h, 0], st2.at[h, k], s2_s.at[i], s2_r.at[i], peer[k])

    def piece(h, j):
        start = sum(PIECES[h][:j])
        return start, PIECES[h][j]

    def g_copy(h, j):
        cl = pl.ds(*piece(h, j))
        i = h * 4 + j
        return remote(g_send.at[h, :, :, cl], g_recv.at[h, :, :, cl], g_s.at[i], g_r.at[i], core_peer)

    def gx_copy(h, j):
        cl = pl.ds(*piece(h, j))
        i = h * 4 + j
        return remote(g_recv.at[h, :, pl.ds(0, SUB), cl], gx_recv.at[h, :, :, cl], gx_s.at[i], gx_r.at[i], x_peer)

    def a_copy(h, j, kind):
        own = c * 2 + xc
        slot = (own, own, c * 2 + 1 - xc)[kind]
        i = (h * 4 + j) * 3 + kind
        ref = a_all.at[h, slot, :, pl.ds(*piece(h, j))]
        return remote(ref, ref, a_s.at[i], a_r.at[i], (core_peer, x_peer, core_peer)[kind])

    def f_copy(h):
        return remote(f_send.at[h], f_recv.at[h], f_s.at[h], f_r.at[h], y_peer)

    lane = lax.broadcasted_iota(jnp.int32, (128, 128), 1)
    sublane = lax.broadcasted_iota(jnp.int32, (128, 128), 0)

    def local_stats(v):
        s = jnp.sum(v, axis=1, keepdims=True)
        q = jnp.sum(v * v, axis=1, keepdims=True)
        n = v.shape[0]
        m = jnp.where(lane[0:n] == 0, s, jnp.where(lane[0:n] == 1, q, 0.0))
        if n < 128:
            m = jnp.concatenate([m, jnp.zeros((128 - n, 128), F32)], axis=0)
        return m.T[0:2]

    def moments(total):
        mean = total[0:1] / full_width
        var = total[1:2] / full_width - mean * mean
        rstd = lax.rsqrt(var + EPS)
        m = jnp.where(sublane == 0, mean, jnp.where(sublane == 1, rstd, 0.0)).T
        return m[:, 0:1], m[:, 1:2]

    def x_own(h, s):
        return x_all[h, s].astype(F32)

    for h in range(NCH):
        x_load(h).start()
    for r in (3, 2, 1, 0):
        for m in range(3):
            qkv_load(r, m).start()
    for tb in tables:
        tb.start()
    barrier = pltpu.get_barrier_semaphore()
    for dev in peer[1:] + other:
        pl.semaphore_signal(barrier, inc=1, device_id=dev, device_id_type=MESH)
    for h in range(NCH):
        x_load(h).wait()
    st1[0] = local_stats(jnp.concatenate([x_own(h, y) for h in range(NCH)], axis=0))
    pl.semaphore_wait(barrier, 7)
    for k in range(1, 8):
        s1_copy(k).start()
    for h in range(NCH):
        xy_copy(h).start()
    wo_load.start()
    for k in range(1, 4):
        s1_copy(k).wait_recv()
    mean_o, rstd_o = moments((st1[0] + st1[1]) + (st1[2] + st1[3]))

    def norm_rows(h, s, mean, rstd):
        sl = slice(h * TOK, (h + 1) * TOK)
        n = ((x_own(h, s) - mean[sl]) * rstd[sl]).astype(BF)
        n_buf[h, pl.ds(pl.multiple_of(s * TOK, TOK), TOK)] = n

    first_parts = [(m, part) for part in range(2) for m in range(3)]

    def norm_chunk(h):
        norm_rows(h, y, mean_o, rstd_o)
        xy_copy(h).wait_recv()
        norm_rows(h, 1 - y, *other_moments)

    def qkv_give(h, z):
        for m in range(3):
            d_send[(h * 2 + z) * 3 + m] = dot(n_buf[h], wbuf[(3 - 2 * z) * 3 + m]).astype(BF)
        d_copy(h, z).start()

    def qkv_take(h, z):
        own = [dot(n_buf[h], wbuf[(2 - 2 * z) * 3 + m]) for m in range(3)]
        d_copy(h, z).wait_recv()
        for m in range(3):
            i = (h * 2 + z) * 3 + m
            d_recv[i] = (own[m] + d_recv[i].astype(F32)).astype(BF)

    def qkv_part(part):
        rows = part_rows(part)

        def give(m, carry):
            if part == 0:
                qkv_wait(3, m)
            d_send[m, rows] = dot(n_buf[0, rows], wbuf[9 + m]).astype(BF)
            d_copy(0, 0, m, part).start()
            return carry

        def take(m, carry):
            if part == 0:
                qkv_wait(2, m)
            own = dot(n_buf[0, rows], wbuf[6 + m])
            d_copy(0, 0, m, part).wait_recv()
            d_recv[m, rows] = (own + d_recv[m, rows].astype(F32)).astype(BF)
            x_copy(0, m, part).start()
            return carry

        lax.fori_loop(0, 3, give, 0)
        lax.fori_loop(0, 3, take, 0)

    def step_qa(h, _):
        if h > 0:
            norm_chunk(h)
            qkv_give(h, 0)
            qkv_give(h, 1)
        else:
            norm_rows(0, y, mean_o, rstd_o)
            qkv_part(0)

    def step_qb(h, _):
        if h > 0:
            qkv_take(h, 0)
            return
        for k in range(4, 8):
            s1_copy(k).wait_recv()
        other_moments.extend(moments((st1[4] + st1[5]) + (st1[6] + st1[7])))
        xy_copy(0).wait_recv()
        norm_rows(0, 1 - y, *other_moments)
        qkv_part(1)
        for m in range(3):
            qkv_wait(1, m)
        qkv_give(0, 1)

    def step_qs(h, _):
        if h > 0:
            x_copy(h).start()

    def step_qc(h, _):
        if h == 0:
            for m in range(3):
                qkv_wait(0, m)
        qkv_take(h, 1)
        if h == 0:
            for j in range(n_full + 1):
                for i in range(2):
                    gu_load(i, j, FW if j < n_full else last_w).start()
        if h == NCH - 1:
            for j in range(n_full + 1):
                for nh in range(2):
                    down_load(j, nh, FW if j < n_full else last_w).start()

    def rotate(v, cos2, sin2):
        f = v.astype(F32)
        return (f * cos2 + pltpu.roll(f, HEAD_DIM // 2, 1) * sin2).astype(BF)

    def step_at(h, _):
        for m, part in first_parts if h == 0 else ((None, None),):
            x_copy(h, m, part).wait_recv()
        if h == 0:
            for tb in tables:
                tb.wait()

        def final(m):
            return (d_recv[h * 6 + 3 + m].astype(F32) + x_recv[h * 3 + m].astype(F32)).astype(BF)

        sl = slice(h * TOK, (h + 1) * TOK)
        n_keys = (h + 1) * TOK
        cos2 = jnp.concatenate([cos_v[sl], cos_v[sl]], axis=0)
        sin2 = jnp.concatenate([sin_v[sl], sin_v[sl]], axis=0)
        q, k, v = final(0), final(1), final(2)
        for s in range(2):
            v_buf[s, sl] = v[s * TOK:(s + 1) * TOK]
        heads = [slice(hd * HEAD_DIM, (hd + 1) * HEAD_DIM) for hd in range(cols // HEAD_DIM)]
        blocks = [(hd, s) for hd in range(len(heads)) for s in range(2)]
        qr = [rotate(q[:, cl], cos2, sin2) for cl in heads]
        kr = [rotate(k[:, cl], cos2, sin2) for cl in heads]
        for hd, s in blocks:
            k_buf[s, sl, heads[hd]] = kr[hd][s * TOK:(s + 1) * TOK]
        scores = jnp.concatenate(
            [dot_t(qr[hd][s * TOK:(s + 1) * TOK], k_buf[s, 0:n_keys, heads[hd]]) for hd, s in blocks], axis=0
        ) * (HEAD_DIM ** -0.5)
        q_pos = h * TOK + lax.rem(lax.broadcasted_iota(jnp.int32, scores.shape, 0), TOK)
        k_pos = lax.broadcasted_iota(jnp.int32, scores.shape, 1)
        scores = jnp.where(q_pos >= k_pos, scores, -1e30)
        e = jnp.exp(scores - jnp.max(scores, axis=1, keepdims=True))
        prob = (e / jnp.sum(e, axis=1, keepdims=True)).astype(BF)
        for i, (hd, s) in enumerate(blocks):
            o = dot(prob[i * TOK:(i + 1) * TOK], v_buf[s, 0:n_keys, heads[hd]])
            o_all[h, t, s * TOK:(s + 1) * TOK, heads[hd]] = o.astype(BF)
        o_copy(h, 1).start()
        o_copy(h, 0).start()

    def step_ro(h, _):
        o_copy(h, 1).wait_recv()
        o_copy(h, 2).start()

    def step_pr(h, _):
        if first_time("wo"):
            wo_load.wait()
        o_copy(h, 0).wait_recv()
        o_copy(h, 2).wait_recv()
        for nh in range(2):
            cl = slice(nh * 512, (nh + 1) * 512)
            res = jnp.zeros((ROWS, 512), F32)
            for b in range(4):
                res = res + dot(o_all[h, b], wo_v[b * cols:(b + 1) * cols, cl])
            p_send[h, :, cl] = res.astype(BF)
            p_copy(h, nh).start()

    def step_re(h, _):
        for nh in range(2):
            p_copy(h, nh).wait_recv()
        attn = (p_send[h].astype(F32) + p_recv[h].astype(F32)).astype(BF).astype(F32)
        xv = jnp.concatenate([x_own(h, 0), x_own(h, 1)], axis=0)
        hv = (xv + attn).astype(BF)
        h_buf[h] = hv
        st2[h, 0] = local_stats(hv.astype(F32))
        for k in range(1, 4):
            s2_copy(h, k).start()

    def step_n2(h, _):
        for k in range(1, 4):
            s2_copy(h, k).wait_recv()
        mean, rstd = moments((st2[h, 0] + st2[h, 1]) + (st2[h, 2] + st2[h, 3]))
        n = ((h_buf[h].astype(F32) - mean[0:ROWS]) * rstd[0:ROWS]).astype(BF)
        for b in range(4):
            e_c = c if b // 2 == 1 else 1 - c
            e_x = xc if b % 2 == 1 else 1 - xc
            n_buf[h, pl.ds(pl.multiple_of(2 * SUB * e_c + SUB * e_x, SUB), SUB)] = n[b * SUB:(b + 1) * SUB]

    def steps(h, j, body):
        start, w = piece(h, j)
        lo, n = start // FW, w // FW
        if n == 1:
            body(lo, FW)
        elif n > 1:
            def step(kb, carry):
                body(kb, FW)
                return carry

            lax.fori_loop(lo, lo + n, step, 0)
        if w % FW:
            body(lo + n, w % FW)

    def step_gm(h, j):
        if first_time("gu"):
            for kb in range(n_full + 1):
                for i in range(2):
                    gu_load(i, kb, FW if kb < n_full else last_w).wait()
        slot = own_slot[h, j]
        start = piece(h, j)[0]

        def body(kb, w):
            for i, wv in enumerate((wg_v, wu_v)):
                for n0 in range(0, w, 512):
                    nw = min(512, w - n0)
                    col = kb * FW + n0
                    if not isinstance(col, int):
                        col = pl.multiple_of(col, 512)
                    res = dot(n_buf[h], wv[:, pl.ds(col, nw)])
                    g_send[h, i, :, pl.ds(col, nw)] = res[0:2 * SUB].astype(BF)
                    g_own[slot, i, :, pl.ds(col - start, nw)] = res[2 * SUB:ROWS]

        steps(h, j, body)
        g_copy(h, j).start()

    def step_ga(h, j):
        slot = own_slot[h, j]
        start, w = piece(h, j)
        cl = slice(start, start + w)
        g_copy(h, j).wait_recv()
        for k in range(2):
            g_recv[h, k, :, cl] = (g_own[slot, k, :, 0:w] + g_recv[h, k, :, cl].astype(F32)).astype(BF)
        gx_copy(h, j).start()

    def step_ac(h, j):
        start, w = piece(h, j)
        cl = slice(start, start + w)
        gx_copy(h, j).wait_recv()
        g, u = [
            (g_recv[h, k, SUB:2 * SUB, cl].astype(F32) + gx_recv[h, k, :, cl].astype(F32)).astype(BF).astype(F32)
            for k in range(2)
        ]
        a_all[h, c * 2 + xc, :, cl] = (g * (1.0 / (1.0 + jnp.exp(-g))) * u).astype(BF)
        a_copy(h, j, 1).start()
        a_copy(h, j, 0).start()

    def step_ra(h, j):
        a_copy(h, j, 1).wait_recv()
        a_copy(h, j, 2).start()

    def step_dn(h, j):
        if first_time("down"):
            for kb in range(n_full + 1):
                for nh in range(2):
                    down_load(kb, nh, FW if kb < n_full else last_w).wait()
        a_copy(h, j, 0).wait_recv()
        a_copy(h, j, 2).wait_recv()
        if j == 0:
            acc[h] = jnp.zeros((ROWS, width), F32)

        def body(kb, w):
            col = kb * FW if isinstance(kb, int) else pl.multiple_of(kb * FW, FW)
            lhs = a_all[h, :, :, pl.ds(col, w)].reshape(ROWS, w)
            for nh in range(2):
                acc[h, :, nh * 512:(nh + 1) * 512] += dot(lhs, wbuf[kb * 2 + nh, 0:w])

        steps(h, j, body)

    def step_fi(h, _):
        f_send[h] = acc[h, seq_rows(1 - y)].astype(BF)
        f_copy(h).start()

    stores = []

    def step_ou(h, _):
        cp = store_out(h)
        cp.start()
        stores.append(cp)

    def store_out(h):
        own = pl.ds(pl.multiple_of(y * TOK, TOK), TOK)
        f_copy(h).wait_recv()
        mlp = (acc[h, own].astype(BF).astype(F32) + f_recv[h].astype(F32)).astype(BF).astype(F32)
        y_buf[h] = (h_buf[h, own].astype(F32) + mlp).astype(BF)
        return pltpu.make_async_copy(y_buf.at[h], out_hbm.at[0, pl.ds(h * TOK, TOK)], ld_sem.at[h])

    other_moments = []
    seen = set()

    def first_time(name):
        new = name not in seen
        seen.add(name)
        return new

    own_slot, free = {}, list(range(g_own.shape[0]))
    program = [(w[:2], int(w[2]), int(w[3:] or 0)) for line in ORDER for w in line.split()]
    for name, h, j in program:
        if name == "gm":
            own_slot[h, j] = free.pop(0)
        if name == "ga":
            free.append(own_slot[h, j])
    step_of = dict(qa=step_qa, qb=step_qb, qs=step_qs, qc=step_qc, at=step_at, ro=step_ro, pr=step_pr, re=step_re, n2=step_n2,
                   gm=step_gm, ga=step_ga, ac=step_ac, ra=step_ra, dn=step_dn, fi=step_fi, ou=step_ou)
    for name, h, j in program:
        step_of[name](h, j)

    for k in range(1, 8):
        s1_copy(k).wait_send()
    for h in range(NCH):
        xy_copy(h).wait_send()
        for m, part in first_parts if h == 0 else ((None, None),):
            d_copy(h, 0, m, part).wait_send()
            x_copy(h, m, part).wait_send()
        d_copy(h, 1).wait_send()
        for m in range(3):
            s2_copy(h, m + 1).wait_send()
            o_copy(h, m).wait_send()
        for nh in range(2):
            p_copy(h, nh).wait_send()
        for j in range(len(PIECES[h])):
            g_copy(h, j).wait_send()
            gx_copy(h, j).wait_send()
            for kind in range(3):
                a_copy(h, j, kind).wait_send()
        f_copy(h).wait_send()
    for cp in stores:
        cp.wait()


def solution(mesh):
    act_spec = P(("dp", "ty"), None, "tx")
    col_spec = P("tx", "ty")
    row_spec = P("ty", "tx")

    def layer_fn(x_blk, w_q, w_k, w_v, w_o, w_gate, w_up, w_down):
        seq_len, width = x_blk.shape[1:]
        cols = w_q.shape[1] // 4
        ff = w_gate.shape[1]
        cos_t, sin_t = (jnp.asarray(a) for a in rotary_tables(seq_len))
        dma = pltpu.SemaphoreType.DMA
        vm = pltpu.VMEM
        return pl.pallas_call(
            layer_kernel,
            out_shape=jax.ShapeDtypeStruct(x_blk.shape, BF),
            in_specs=[pl.BlockSpec(memory_space=pl.ANY)] * 10,
            out_specs=pl.BlockSpec(memory_space=pl.ANY),
            scratch_shapes=[
                vm((12, width, cols), BF),
                vm(w_o.shape, BF),
                vm(w_gate.shape, BF),
                vm(w_up.shape, BF),
                vm((seq_len, HEAD_DIM), F32),
                vm((seq_len, HEAD_DIM), F32),
                vm((NCH, 2, TOK, width), BF),
                vm((NCH, ROWS, width), BF),
                vm((6 * NCH, ROWS, cols), BF),
                vm((6 * NCH, ROWS, cols), BF),
                vm((3 * NCH, ROWS, cols), BF),
                vm((2, seq_len, cols), BF),
                vm((2, seq_len, cols), BF),
                vm((NCH, 4, ROWS, cols), BF),
                vm((NCH, ROWS, width), BF),
                vm((NCH, ROWS, width), BF),
                vm((NCH, ROWS, width), BF),
                vm((NCH, 2, 2 * SUB, ff), BF),
                vm((NCH, 2, 2 * SUB, ff), BF),
                vm((3, 2, 2 * SUB, max(max(p) for p in PIECES)), F32),
                vm((NCH, 2, SUB, ff), BF),
                vm((NCH, 4, SUB, ff), BF),
                vm((NCH, ROWS, width), F32),
                vm((NCH, TOK, width), BF),
                vm((NCH, TOK, width), BF),
                vm((NCH, TOK, width), BF),
                vm((8, 2, 128), F32),
                vm((NCH, 4, 2, 128), F32),
                dma((NCH + 2,)), dma((48,)),
                *(dma((n,)) for n in (NCH, 8, 6 * NCH + 3, 3 * NCH + 3, 3 * NCH, 2 * NCH, 4 * NCH, 4 * NCH, 4 * NCH, 12 * NCH, NCH) for _ in range(2)),
            ],
            compiler_params=pltpu.CompilerParams(collective_id=0, has_side_effects=True, vmem_limit_bytes=67043328),
            name="layer",
        )(x_blk, w_q, w_k, w_v, w_o, w_gate, w_up, w_down, cos_t, sin_t)

    return jax.shard_map(layer_fn, mesh=mesh, in_specs=(act_spec, col_spec, col_spec, col_spec, row_spec, col_spec, col_spec, row_spec), out_specs=act_spec, check_vma=False)
```

```python
import numpy as np

import jax
import jax.numpy as jnp
from jax import lax
from jax.experimental import pallas as pl
from jax.experimental.pallas import tpu as pltpu
from jax.sharding import PartitionSpec as P

HEAD_DIM = 128
EPS = 1e-5
THETA = 10000.0
BF = jnp.bfloat16
F32 = jnp.float32
MESH = pl.DeviceIdType.MESH

NCH = 4
TOK = 32
ROWS = 2 * TOK
SUB = ROWS // 4
FW = 1024

PIECES = ((1024, 2048, 2432), (2048, 2048, 1408), (3072, 2432), (2048, 2048, 1408))
ORDER = (
    "qa0 qb0 qs0 qa1", "qb1 qs1 qc0 qa2", "at0 qb2 qc1 qs2", "qc2 qa3 ro0 at1",
    "qb3 qs3 pr0 qc3", "ro1 pr1 re0 at2", "at3 n20 gm00 gm01", "ro2 ga00 re1 ga01",
    "ro3 gm02 ac00 pr2", "ga02 pr3 n21 ac01", "gm10 re2 ga10 ac02", "gm11 ga11 gm12 ac10",
    "re3 n22 ga12 gm20", "ac11 ra00 n23 ga20", "dn00 ra10 gm21 ga21", "gm30 ra01 ga30 ra02",
    "ac20 gm31 ga31 gm32", "ac21 dn10 ga32 ac12", "ra20 dn01 dn02 dn20", "ra11 ra21 fi0 ac30",
    "dn11 ac31 ac32 ra12", "dn21 fi2 ra30 ou0", "dn12 fi1 ra31 dn30", "ra32 dn31 dn32 fi3",
    "ou1 ou2 ou3",
)


def dot(a, b):
    return jnp.dot(a, b, preferred_element_type=F32)


def dot_t(a, b):
    return lax.dot_general(a, b, (((1,), (1,)), ((), ())), preferred_element_type=F32)


def rotary_tables(seq_len):
    half_dim = HEAD_DIM // 2
    inv_freq = (np.float32(THETA) ** (np.float32(-2.0) * np.arange(half_dim, dtype=np.float32) / np.float32(HEAD_DIM))).astype(np.float32)
    angles = np.arange(seq_len, dtype=np.float32)[:, None] * inv_freq[None, :]
    cos_t = np.cos(angles.astype(np.float64)).astype(np.float32)
    sin_t = np.sin(angles.astype(np.float64)).astype(np.float32)
    return np.concatenate([cos_t, cos_t], 1), np.concatenate([-sin_t, sin_t], 1)


def layer_kernel(x_hbm, wq_hbm, wk_hbm, wv_hbm, wo_hbm, wg_hbm, wu_hbm, wd_hbm, cos_hbm, sin_hbm, out_ref,
                 wbuf, wo_v, wg_v, wu_v, cos_v, sin_v, x_all, n_buf, d_send, d_recv, x_recv, k_buf, v_buf, o_all,
                 p_send, p_recv, h_buf, g_send, g_recv, g_own, gx_recv, a_all, acc, f_send, f_recv, st1, st2,
                 ld_sem, w_sem, xy_s, xy_r, s1_s, s1_r, d_s, d_r, x_s, x_r, o_s, o_r, p_s, p_r, s2_s, s2_r,
                 g_s, g_r, gx_s, gx_r, a_s, a_r, f_s, f_r):
    dp = lax.axis_index("dp")
    y = lax.axis_index("ty")
    t = lax.axis_index("tx")
    xc = lax.div(t, 2)
    c = lax.rem(t, 2)
    width = x_hbm.shape[2]
    cols = wq_hbm.shape[1] // 4
    ff = wg_hbm.shape[1]
    n_full = ff // FW
    last_w = ff - n_full * FW
    full_width = 4 * width
    rel = [t, t + 1 - 2 * c, t + 2 - 4 * xc, 3 - t]
    peer = [(dp, y, r) for r in rel]
    other = [(dp, 1 - y, r) for r in rel]
    core_peer, x_peer, y_peer = peer[1], peer[2], other[0]

    def remote(src, dst, ss, rs, dev):
        return pltpu.make_async_remote_copy(src_ref=src, dst_ref=dst, send_sem=ss, recv_sem=rs, device_id=dev, device_id_type=MESH)

    def x_load(h):
        return pltpu.make_async_copy(x_hbm.at[0, pl.ds(h * TOK, TOK)], x_all.at[h, y], ld_sem.at[h])

    tables = [pltpu.make_async_copy(cos_hbm, cos_v, ld_sem.at[NCH]), pltpu.make_async_copy(sin_hbm, sin_v, ld_sem.at[NCH + 1])]

    def qkv_load(r, m):
        src = (wq_hbm, wk_hbm, wv_hbm)[m].at[:, pl.ds(pl.multiple_of(rel[r] * cols, cols), cols)]
        return pltpu.make_async_copy(src, wbuf.at[r * 3 + m], w_sem.at[r * 3 + m])

    def qkv_wait(r, m):
        pltpu.make_async_copy(wq_hbm.at[:, pl.ds(0, cols)], wbuf.at[r * 3 + m], w_sem.at[r * 3 + m]).wait()

    wo_load = pltpu.make_async_copy(wo_hbm, wo_v, w_sem.at[12])

    def gu_load(i, j, w):
        src, dst = ((wg_hbm, wg_v), (wu_hbm, wu_v))[i]
        start = j * FW if isinstance(j, int) else pl.multiple_of(j * FW, FW)
        return pltpu.make_async_copy(src.at[:, pl.ds(start, w)], dst.at[:, pl.ds(start, w)], w_sem.at[16 + i * 8 + j])

    def down_load(j, nh, w):
        start = j * FW if isinstance(j, int) else pl.multiple_of(j * FW, FW)
        return pltpu.make_async_copy(wd_hbm.at[pl.ds(start, w), pl.ds(nh * 512, 512)], wbuf.at[j * 2 + nh, pl.ds(0, w)], w_sem.at[32 + j * 2 + nh])

    def xy_copy(h):
        return remote(x_all.at[h, y], x_all.at[h, y], xy_s.at[h], xy_r.at[h], y_peer)

    def s1_copy(k):
        return remote(st1.at[0], st1.at[k], s1_s.at[k], s1_r.at[k], peer[k] if k < 4 else other[k - 4])

    def seq_rows(s):
        return pl.ds(pl.multiple_of(s * TOK, TOK), TOK)

    def part_rows(part):
        return seq_rows(y if part == 0 else 1 - y)

    def d_copy(h, z, m=None, part=None):
        i = (h * 2 + z) * 3 + (0 if m is None else m)
        src, dst = (d_send.at[pl.ds(i, 3)], d_recv.at[pl.ds(i, 3)]) if m is None else (d_send.at[i, part_rows(part)], d_recv.at[i, part_rows(part)])
        k = 6 * NCH + m if part == 1 else i
        return remote(src, dst, d_s.at[k], d_r.at[k], core_peer)

    def x_copy(h, m=None, part=None):
        i = h * 3 + (0 if m is None else m)
        k = h * 6 + (0 if m is None else m)
        src, dst = (d_recv.at[pl.ds(k, 3)], x_recv.at[pl.ds(i, 3)]) if m is None else (d_recv.at[k, part_rows(part)], x_recv.at[i, part_rows(part)])
        n = 3 * NCH + m if part == 1 else i
        return remote(src, dst, x_s.at[n], x_r.at[n], x_peer)

    def o_copy(h, kind):
        slot = (t, t, rel[2])[kind]
        i = h * 3 + kind
        ref = o_all.at[h, slot]
        return remote(ref, ref, o_s.at[i], o_r.at[i], (core_peer, x_peer, core_peer)[kind])

    def p_copy(h, nh):
        cl = pl.ds(nh * 512, 512)
        return remote(p_send.at[h, :, cl], p_recv.at[h, :, cl], p_s.at[h * 2 + nh], p_r.at[h * 2 + nh], y_peer)

    def s2_copy(h, k):
        i = h * 4 + k
        return remote(st2.at[h, 0], st2.at[h, k], s2_s.at[i], s2_r.at[i], peer[k])

    def piece(h, j):
        start = sum(PIECES[h][:j])
        return start, PIECES[h][j]

    def g_copy(h, j):
        cl = pl.ds(*piece(h, j))
        i = h * 4 + j
        return remote(g_send.at[h % 2, :, :, cl], g_recv.at[h, :, :, cl], g_s.at[i], g_r.at[i], core_peer)

    def gx_copy(h, j):
        cl = pl.ds(*piece(h, j))
        i = h * 4 + j
        return remote(g_recv.at[h, :, pl.ds(0, SUB), cl], gx_recv.at[h, :, :, cl], gx_s.at[i], gx_r.at[i], x_peer)

    def a_copy(h, j, kind):
        own = c * 2 + xc
        slot = (own, own, c * 2 + 1 - xc)[kind]
        i = (h * 4 + j) * 3 + kind
        ref = a_all.at[h, slot, :, pl.ds(*piece(h, j))]
        return remote(ref, ref, a_s.at[i], a_r.at[i], (core_peer, x_peer, core_peer)[kind])

    def f_copy(h):
        return remote(f_send.at[h], f_recv.at[h], f_s.at[h], f_r.at[h], y_peer)

    lane = lax.broadcasted_iota(jnp.int32, (128, 128), 1)
    sublane = lax.broadcasted_iota(jnp.int32, (128, 128), 0)

    def local_stats(v):
        s = jnp.sum(v, axis=1, keepdims=True)
        q = jnp.sum(v * v, axis=1, keepdims=True)
        n = v.shape[0]
        m = jnp.where(lane[0:n] == 0, s, jnp.where(lane[0:n] == 1, q, 0.0))
        if n < 128:
            m = jnp.concatenate([m, jnp.zeros((128 - n, 128), F32)], axis=0)
        return m.T[0:2]

    def moments(total):
        mean = total[0:1] / full_width
        var = total[1:2] / full_width - mean * mean
        rstd = lax.rsqrt(var + EPS)
        m = jnp.where(sublane == 0, mean, jnp.where(sublane == 1, rstd, 0.0)).T
        return m[:, 0:1], m[:, 1:2]

    def x_own(h, s):
        return x_all[h, s].astype(F32)

    for h in range(NCH):
        x_load(h).start()
    for r in (3, 2, 1, 0):
        for m in range(3):
            qkv_load(r, m).start()
    for tb in tables:
        tb.start()
    barrier = pltpu.get_barrier_semaphore()
    for dev in peer[1:] + other:
        pl.semaphore_signal(barrier, inc=1, device_id=dev, device_id_type=MESH)
    for h in range(NCH):
        x_load(h).wait()
    st1[0] = local_stats(jnp.concatenate([x_own(h, y) for h in range(NCH)], axis=0))
    pl.semaphore_wait(barrier, 7)
    for k in range(1, 8):
        s1_copy(k).start()
    for h in range(NCH):
        xy_copy(h).start()
    wo_load.start()
    for k in range(1, 4):
        s1_copy(k).wait_recv()
    mean_o, rstd_o = moments((st1[0] + st1[1]) + (st1[2] + st1[3]))

    def norm_rows(h, s, mean, rstd):
        sl = slice(h * TOK, (h + 1) * TOK)
        n = ((x_own(h, s) - mean[sl]) * rstd[sl]).astype(BF)
        n_buf[h, pl.ds(pl.multiple_of(s * TOK, TOK), TOK)] = n

    first_parts = [(m, part) for part in range(2) for m in range(3)]

    def norm_chunk(h):
        norm_rows(h, y, mean_o, rstd_o)
        xy_copy(h).wait_recv()
        norm_rows(h, 1 - y, *other_moments)

    def qkv_give(h, z):
        for m in range(3):
            d_send[(h * 2 + z) * 3 + m] = dot(n_buf[h], wbuf[(3 - 2 * z) * 3 + m]).astype(BF)
        d_copy(h, z).start()

    def qkv_take(h, z):
        own = [dot(n_buf[h], wbuf[(2 - 2 * z) * 3 + m]) for m in range(3)]
        d_copy(h, z).wait_recv()
        for m in range(3):
            i = (h * 2 + z) * 3 + m
            d_recv[i] = (own[m] + d_recv[i].astype(F32)).astype(BF)

    def qkv_part(part):
        rows = part_rows(part)

        def give(m, carry):
            if part == 0:
                qkv_wait(3, m)
            d_send[m, rows] = dot(n_buf[0, rows], wbuf[9 + m]).astype(BF)
            d_copy(0, 0, m, part).start()
            return carry

        def take(m, carry):
            if part == 0:
                qkv_wait(2, m)
            own = dot(n_buf[0, rows], wbuf[6 + m])
            d_copy(0, 0, m, part).wait_recv()
            d_recv[m, rows] = (own + d_recv[m, rows].astype(F32)).astype(BF)
            x_copy(0, m, part).start()
            return carry

        lax.fori_loop(0, 3, give, 0)
        lax.fori_loop(0, 3, take, 0)

    def step_qa(h, _):
        if h > 0:
            norm_chunk(h)
            qkv_give(h, 0)
            qkv_give(h, 1)
        else:
            norm_rows(0, y, mean_o, rstd_o)
            qkv_part(0)

    def step_qb(h, _):
        if h > 0:
            qkv_take(h, 0)
            return
        for k in range(4, 8):
            s1_copy(k).wait_recv()
        other_moments.extend(moments((st1[4] + st1[5]) + (st1[6] + st1[7])))
        xy_copy(0).wait_recv()
        norm_rows(0, 1 - y, *other_moments)
        qkv_part(1)
        for m in range(3):
            qkv_wait(1, m)
        qkv_give(0, 1)

    def step_qs(h, _):
        if h > 0:
            x_copy(h).start()

    def step_qc(h, _):
        if h == 0:
            for m in range(3):
                qkv_wait(0, m)
        qkv_take(h, 1)
        if h == 0:
            for j in range(n_full + 1):
                for i in range(2):
                    gu_load(i, j, FW if j < n_full else last_w).start()
        if h == NCH - 1:
            for j in range(n_full + 1):
                for nh in range(2):
                    down_load(j, nh, FW if j < n_full else last_w).start()

    def rotate(v, cos2, sin2):
        f = v.astype(F32)
        return (f * cos2 + pltpu.roll(f, HEAD_DIM // 2, 1) * sin2).astype(BF)

    def step_at(h, _):
        for m, part in first_parts if h == 0 else ((None, None),):
            x_copy(h, m, part).wait_recv()
        if h == 0:
            for tb in tables:
                tb.wait()

        def final(m):
            return (d_recv[h * 6 + 3 + m].astype(F32) + x_recv[h * 3 + m].astype(F32)).astype(BF)

        sl = slice(h * TOK, (h + 1) * TOK)
        n_keys = (h + 1) * TOK
        cos2 = jnp.concatenate([cos_v[sl], cos_v[sl]], axis=0)
        sin2 = jnp.concatenate([sin_v[sl], sin_v[sl]], axis=0)
        q, k, v = final(0), final(1), final(2)
        for s in range(2):
            v_buf[s, sl] = v[s * TOK:(s + 1) * TOK]
        heads = [slice(hd * HEAD_DIM, (hd + 1) * HEAD_DIM) for hd in range(cols // HEAD_DIM)]
        blocks = [(hd, s) for hd in range(len(heads)) for s in range(2)]
        qr = [rotate(q[:, cl], cos2, sin2) for cl in heads]
        kr = [rotate(k[:, cl], cos2, sin2) for cl in heads]
        for hd, s in blocks:
            k_buf[s, sl, heads[hd]] = kr[hd][s * TOK:(s + 1) * TOK]
        scores = jnp.concatenate(
            [dot_t(qr[hd][s * TOK:(s + 1) * TOK], k_buf[s, 0:n_keys, heads[hd]]) for hd, s in blocks], axis=0
        ) * (HEAD_DIM ** -0.5)
        q_pos = h * TOK + lax.rem(lax.broadcasted_iota(jnp.int32, scores.shape, 0), TOK)
        k_pos = lax.broadcasted_iota(jnp.int32, scores.shape, 1)
        scores = jnp.where(q_pos >= k_pos, scores, -1e30)
        e = jnp.exp(scores - jnp.max(scores, axis=1, keepdims=True))
        prob = (e / jnp.sum(e, axis=1, keepdims=True)).astype(BF)
        for i, (hd, s) in enumerate(blocks):
            o = dot(prob[i * TOK:(i + 1) * TOK], v_buf[s, 0:n_keys, heads[hd]])
            o_all[h, t, s * TOK:(s + 1) * TOK, heads[hd]] = o.astype(BF)
        o_copy(h, 1).start()
        o_copy(h, 0).start()

    def step_ro(h, _):
        o_copy(h, 1).wait_recv()
        o_copy(h, 2).start()

    def step_pr(h, _):
        if first_time("wo"):
            wo_load.wait()
        o_copy(h, 0).wait_recv()
        o_copy(h, 2).wait_recv()
        for nh in range(2):
            cl = slice(nh * 512, (nh + 1) * 512)
            res = jnp.zeros((ROWS, 512), F32)
            for b in range(4):
                res = res + dot(o_all[h, b], wo_v[b * cols:(b + 1) * cols, cl])
            p_send[h, :, cl] = res.astype(BF)
            p_copy(h, nh).start()

    def step_re(h, _):
        for nh in range(2):
            p_copy(h, nh).wait_recv()
        attn = (p_send[h].astype(F32) + p_recv[h].astype(F32)).astype(BF).astype(F32)
        xv = jnp.concatenate([x_own(h, 0), x_own(h, 1)], axis=0)
        hv = (xv + attn).astype(BF)
        h_buf[h] = hv
        st2[h, 0] = local_stats(hv.astype(F32))
        for k in range(1, 4):
            s2_copy(h, k).start()

    def step_n2(h, _):
        for k in range(1, 4):
            s2_copy(h, k).wait_recv()
        mean, rstd = moments((st2[h, 0] + st2[h, 1]) + (st2[h, 2] + st2[h, 3]))
        n = ((h_buf[h].astype(F32) - mean[0:ROWS]) * rstd[0:ROWS]).astype(BF)
        for b in range(4):
            e_c = c if b // 2 == 1 else 1 - c
            e_x = xc if b % 2 == 1 else 1 - xc
            n_buf[h, pl.ds(pl.multiple_of(2 * SUB * e_c + SUB * e_x, SUB), SUB)] = n[b * SUB:(b + 1) * SUB]

    def steps(h, j, body):
        start, w = piece(h, j)
        lo, n = start // FW, w // FW
        if n == 1:
            body(lo, FW)
        elif n > 1:
            def step(kb, carry):
                body(kb, FW)
                return carry

            lax.fori_loop(lo, lo + n, step, 0)
        if w % FW:
            body(lo + n, w % FW)

    def step_gm(h, j):
        if first_time("gu"):
            for kb in range(n_full + 1):
                for i in range(2):
                    gu_load(i, kb, FW if kb < n_full else last_w).wait()
        if h >= 2 and j == 0:
            for k in range(len(PIECES[h - 2])):
                g_copy(h - 2, k).wait_send()
        slot = own_slot[h, j]
        start = piece(h, j)[0]

        def body(kb, w):
            for i, wv in enumerate((wg_v, wu_v)):
                for n0 in range(0, w, 512):
                    nw = min(512, w - n0)
                    col = kb * FW + n0
                    if not isinstance(col, int):
                        col = pl.multiple_of(col, 512)
                    res = dot(n_buf[h], wv[:, pl.ds(col, nw)])
                    g_send[h % 2, i, :, pl.ds(col, nw)] = res[0:2 * SUB].astype(BF)
                    g_own[slot, i, :, pl.ds(col - start, nw)] = res[2 * SUB:ROWS]

        steps(h, j, body)
        g_copy(h, j).start()

    def step_ga(h, j):
        slot = own_slot[h, j]
        start, w = piece(h, j)
        cl = slice(start, start + w)
        g_copy(h, j).wait_recv()
        for k in range(2):
            g_recv[h, k, :, cl] = (g_own[slot, k, :, 0:w] + g_recv[h, k, :, cl].astype(F32)).astype(BF)
        gx_copy(h, j).start()

    def step_ac(h, j):
        start, w = piece(h, j)
        cl = slice(start, start + w)
        gx_copy(h, j).wait_recv()
        g, u = [
            (g_recv[h, k, SUB:2 * SUB, cl].astype(F32) + gx_recv[h, k, :, cl].astype(F32)).astype(BF).astype(F32)
            for k in range(2)
        ]
        a_all[h, c * 2 + xc, :, cl] = (g * (1.0 / (1.0 + jnp.exp(-g))) * u).astype(BF)
        a_copy(h, j, 1).start()
        a_copy(h, j, 0).start()

    def step_ra(h, j):
        a_copy(h, j, 1).wait_recv()
        a_copy(h, j, 2).start()

    def step_dn(h, j):
        if first_time("down"):
            for kb in range(n_full + 1):
                for nh in range(2):
                    down_load(kb, nh, FW if kb < n_full else last_w).wait()
        a_copy(h, j, 0).wait_recv()
        a_copy(h, j, 2).wait_recv()
        if j == 0:
            acc[h] = jnp.zeros((ROWS, width), F32)

        def body(kb, w):
            col = kb * FW if isinstance(kb, int) else pl.multiple_of(kb * FW, FW)
            lhs = a_all[h, :, :, pl.ds(col, w)].reshape(ROWS, w)
            for nh in range(2):
                acc[h, :, nh * 512:(nh + 1) * 512] += dot(lhs, wbuf[kb * 2 + nh, 0:w])

        steps(h, j, body)

    def step_fi(h, _):
        f_send[h] = acc[h, seq_rows(1 - y)].astype(BF)
        f_copy(h).start()

    def step_ou(h, _):
        own = pl.ds(pl.multiple_of(y * TOK, TOK), TOK)
        f_copy(h).wait_recv()
        mlp = (acc[h, own].astype(BF).astype(F32) + f_recv[h].astype(F32)).astype(BF).astype(F32)
        out_ref[0, h * TOK:(h + 1) * TOK] = (h_buf[h, own].astype(F32) + mlp).astype(BF)

    other_moments = []
    seen = set()

    def first_time(name):
        new = name not in seen
        seen.add(name)
        return new

    own_slot, free = {}, list(range(g_own.shape[0]))
    program = [(w[:2], int(w[2]), int(w[3:] or 0)) for line in ORDER for w in line.split()]
    for name, h, j in program:
        if name == "gm":
            own_slot[h, j] = free.pop(0)
        if name == "ga":
            free.append(own_slot[h, j])
    step_of = dict(qa=step_qa, qb=step_qb, qs=step_qs, qc=step_qc, at=step_at, ro=step_ro, pr=step_pr, re=step_re, n2=step_n2,
                   gm=step_gm, ga=step_ga, ac=step_ac, ra=step_ra, dn=step_dn, fi=step_fi, ou=step_ou)
    for name, h, j in program:
        step_of[name](h, j)

    for k in range(1, 8):
        s1_copy(k).wait_send()
    for h in range(NCH):
        xy_copy(h).wait_send()
        for m, part in first_parts if h == 0 else ((None, None),):
            d_copy(h, 0, m, part).wait_send()
            x_copy(h, m, part).wait_send()
        d_copy(h, 1).wait_send()
        for m in range(3):
            s2_copy(h, m + 1).wait_send()
            o_copy(h, m).wait_send()
        for nh in range(2):
            p_copy(h, nh).wait_send()
        for j in range(len(PIECES[h])):
            if h >= NCH - 2:
                g_copy(h, j).wait_send()
            gx_copy(h, j).wait_send()
            for kind in range(3):
                a_copy(h, j, kind).wait_send()
        f_copy(h).wait_send()


def solution(mesh):
    act_spec = P(("dp", "ty"), None, "tx")
    col_spec = P("tx", "ty")
    row_spec = P("ty", "tx")

    def layer_fn(x_blk, w_q, w_k, w_v, w_o, w_gate, w_up, w_down):
        seq_len, width = x_blk.shape[1:]
        cols = w_q.shape[1] // 4
        ff = w_gate.shape[1]
        cos_t, sin_t = (jnp.asarray(a) for a in rotary_tables(seq_len))
        dma = pltpu.SemaphoreType.DMA
        vm = pltpu.VMEM
        return pl.pallas_call(
            layer_kernel,
            out_shape=pltpu.VMEM(x_blk.shape, BF),
            in_specs=[pl.BlockSpec(memory_space=pl.ANY)] * 10,
            out_specs=pl.BlockSpec(memory_space=pltpu.VMEM),
            scratch_shapes=[
                vm((12, width, cols), BF),
                vm(w_o.shape, BF),
                vm(w_gate.shape, BF),
                vm(w_up.shape, BF),
                vm((seq_len, HEAD_DIM), F32),
                vm((seq_len, HEAD_DIM), F32),
                vm((NCH, 2, TOK, width), BF),
                vm((NCH, ROWS, width), BF),
                vm((6 * NCH, ROWS, cols), BF),
                vm((6 * NCH, ROWS, cols), BF),
                vm((3 * NCH, ROWS, cols), BF),
                vm((2, seq_len, cols), BF),
                vm((2, seq_len, cols), BF),
                vm((NCH, 4, ROWS, cols), BF),
                vm((NCH, ROWS, width), BF),
                vm((NCH, ROWS, width), BF),
                vm((NCH, ROWS, width), BF),
                vm((2, 2, 2 * SUB, ff), BF),
                vm((NCH, 2, 2 * SUB, ff), BF),
                vm((3, 2, 2 * SUB, max(max(p) for p in PIECES)), F32),
                vm((NCH, 2, SUB, ff), BF),
                vm((NCH, 4, SUB, ff), BF),
                vm((NCH, ROWS, width), F32),
                vm((NCH, TOK, width), BF),
                vm((NCH, TOK, width), BF),
                vm((8, 2, 128), F32),
                vm((NCH, 4, 2, 128), F32),
                dma((NCH + 2,)), dma((48,)),
                *(dma((n,)) for n in (NCH, 8, 6 * NCH + 3, 3 * NCH + 3, 3 * NCH, 2 * NCH, 4 * NCH, 4 * NCH, 4 * NCH, 12 * NCH, NCH) for _ in range(2)),
            ],
            compiler_params=pltpu.CompilerParams(collective_id=0, has_side_effects=True, vmem_limit_bytes=66256896),
            name="layer",
        )(x_blk, w_q, w_k, w_v, w_o, w_gate, w_up, w_down, cos_t, sin_t)

    return jax.shard_map(layer_fn, mesh=mesh, in_specs=(act_spec, col_spec, col_spec, col_spec, row_spec, col_spec, col_spec, row_spec), out_specs=act_spec, check_vma=False)
```

```python
import numpy as np

import jax
import jax.numpy as jnp
from jax import lax
from jax.experimental import pallas as pl
from jax.experimental.pallas import tpu as pltpu
from jax.sharding import PartitionSpec as P

HEAD_DIM = 128
EPS = 1e-5
THETA = 10000.0
BF = jnp.bfloat16
F32 = jnp.float32
MESH = pl.DeviceIdType.MESH

NCH = 4
TOK = 32
ROWS = 2 * TOK
SUB = ROWS // 4
FW = 1024

PIECES = ((1024, 2048, 2432), (2048, 2048, 1408), (3072, 2432), (2048, 2048, 1408))
ORDER = (
    "qa0 qb0 qa1 qx0", "qb1 qs1 qs0 qg0", "qa2 qc0 qb2 at0", "qs2 qg1 qa3 qc1",
    "qg2 ro0 qb3 pr0", "at1 qc2 at2 ro1", "re0 qg3 qs3 pr1", "n20 gm00 gm01 ga00",
    "ro2 qc3 re1 ga01", "gm02 at3 n21 ga02", "gm10 pr2 ac01 ro3", "ga10 gm11 pr3 re2",
    "gm12 ra01 ga11 re3", "ac02 n22 ac00 ga12", "ac11 ac10 n23 gm20", "ga20 gm21 ra00 gm30",
    "ac12 ra02 ga21 ga30", "ra10 gm31 ac20 dn00", "dn10 ac21 ra11 ga31", "dn11 dn01 gm32 ra20",
    "dn02 ra21 ra12 ga32", "ac30 ac31 dn20 fi0", "ac32 dn21 ra30 dn12", "fi1 fi2 ra31 dn30",
    "ra32 dn31 dn32 fi3", "ou2 ou1 ou0 ou3",
)


def dot(a, b):
    return jnp.dot(a, b, preferred_element_type=F32)


def dot_t(a, b):
    return lax.dot_general(a, b, (((1,), (1,)), ((), ())), preferred_element_type=F32)


def rotary_tables(seq_len):
    half_dim = HEAD_DIM // 2
    inv_freq = (np.float32(THETA) ** (np.float32(-2.0) * np.arange(half_dim, dtype=np.float32) / np.float32(HEAD_DIM))).astype(np.float32)
    angles = np.arange(seq_len, dtype=np.float32)[:, None] * inv_freq[None, :]
    cos_t = np.cos(angles.astype(np.float64)).astype(np.float32)
    sin_t = np.sin(angles.astype(np.float64)).astype(np.float32)
    return np.concatenate([cos_t, cos_t], 1), np.concatenate([-sin_t, sin_t], 1)


def layer_kernel(x_hbm, wq_hbm, wk_hbm, wv_hbm, wo_hbm, wg_hbm, wu_hbm, wd_hbm, cos_hbm, sin_hbm, out_ref,
                 wbuf, wo_v, wg_v, wu_v, cos_v, sin_v, x_all, n_buf, d_send, d_recv, x_recv, k_buf, v_buf, o_all,
                 p_send, p_recv, h_buf, g_send, g_recv, g_own, gx_recv, a_all, acc, f_send, f_recv, st1, st2,
                 ld_sem, w_sem, xy_s, xy_r, s1_s, s1_r, d_s, d_r, x_s, x_r, o_s, o_r, p_s, p_r, s2_s, s2_r,
                 g_s, g_r, gx_s, gx_r, a_s, a_r, f_s, f_r):
    dp = lax.axis_index("dp")
    y = lax.axis_index("ty")
    t = lax.axis_index("tx")
    xc = lax.div(t, 2)
    c = lax.rem(t, 2)
    width = x_hbm.shape[2]
    cols = wq_hbm.shape[1] // 4
    ff = wg_hbm.shape[1]
    n_full = ff // FW
    last_w = ff - n_full * FW
    full_width = 4 * width
    rel = [t, t + 1 - 2 * c, t + 2 - 4 * xc, 3 - t]
    peer = [(dp, y, r) for r in rel]
    other = [(dp, 1 - y, r) for r in rel]
    core_peer, x_peer, y_peer = peer[1], peer[2], other[0]

    def remote(src, dst, ss, rs, dev):
        return pltpu.make_async_remote_copy(src_ref=src, dst_ref=dst, send_sem=ss, recv_sem=rs, device_id=dev, device_id_type=MESH)

    def x_load(h):
        return pltpu.make_async_copy(x_hbm.at[0, pl.ds(h * TOK, TOK)], x_all.at[h, y], ld_sem.at[h])

    tables = [pltpu.make_async_copy(cos_hbm, cos_v, ld_sem.at[NCH]), pltpu.make_async_copy(sin_hbm, sin_v, ld_sem.at[NCH + 1])]

    def qkv_load(r, m):
        src = (wq_hbm, wk_hbm, wv_hbm)[m].at[:, pl.ds(pl.multiple_of(rel[r] * cols, cols), cols)]
        return pltpu.make_async_copy(src, wbuf.at[r * 3 + m], w_sem.at[r * 3 + m])

    def qkv_wait(r, m):
        pltpu.make_async_copy(wq_hbm.at[:, pl.ds(0, cols)], wbuf.at[r * 3 + m], w_sem.at[r * 3 + m]).wait()

    wo_load = pltpu.make_async_copy(wo_hbm, wo_v, w_sem.at[12])

    def gu_load(i, j, w):
        src, dst = ((wg_hbm, wg_v), (wu_hbm, wu_v))[i]
        start = j * FW if isinstance(j, int) else pl.multiple_of(j * FW, FW)
        return pltpu.make_async_copy(src.at[:, pl.ds(start, w)], dst.at[:, pl.ds(start, w)], w_sem.at[16 + i * 8 + j])

    def down_load(j, nh, w):
        start = j * FW if isinstance(j, int) else pl.multiple_of(j * FW, FW)
        return pltpu.make_async_copy(wd_hbm.at[pl.ds(start, w), pl.ds(nh * 512, 512)], wbuf.at[j * 2 + nh, pl.ds(0, w)], w_sem.at[32 + j * 2 + nh])

    def xy_copy(h):
        return remote(x_all.at[h, y], x_all.at[h, y], xy_s.at[h], xy_r.at[h], y_peer)

    def s1_copy(k):
        return remote(st1.at[0], st1.at[k], s1_s.at[k], s1_r.at[k], peer[k] if k < 4 else other[k - 4])

    def seq_rows(s):
        return pl.ds(pl.multiple_of(s * TOK, TOK), TOK)

    def part_rows(part):
        return seq_rows(y if part == 0 else 1 - y)

    def d_copy(h, z, m=None, part=None):
        i = (h * 2 + z) * 3 + (0 if m is None else m)
        sl = pl.ds(i, 3) if m is None else i
        src, dst = (d_send.at[sl], d_recv.at[sl]) if part is None else (d_send.at[sl, part_rows(part)], d_recv.at[sl, part_rows(part)])
        k = 6 * NCH if part == 1 else i
        return remote(src, dst, d_s.at[k], d_r.at[k], core_peer)

    def x_copy(h, m=None, part=None):
        i = h * 3 + (0 if m is None else m)
        k = h * 6 + (0 if m is None else m)
        ssl, dsl = (pl.ds(k, 3), pl.ds(i, 3)) if m is None else (k, i)
        src, dst = (d_recv.at[ssl], x_recv.at[dsl]) if part is None else (d_recv.at[ssl, part_rows(part)], x_recv.at[dsl, part_rows(part)])
        n = 3 * NCH if part == 1 else i
        return remote(src, dst, x_s.at[n], x_r.at[n], x_peer)

    def o_copy(h, kind):
        slot = (t, t, rel[2])[kind]
        i = h * 3 + kind
        ref = o_all.at[h, slot]
        return remote(ref, ref, o_s.at[i], o_r.at[i], (core_peer, x_peer, core_peer)[kind])

    def p_copy(h, nh):
        cl = pl.ds(nh * 512, 512)
        return remote(p_send.at[h, :, cl], p_recv.at[h, :, cl], p_s.at[h * 2 + nh], p_r.at[h * 2 + nh], y_peer)

    def s2_copy(h, k):
        i = h * 4 + k
        return remote(st2.at[h, 0], st2.at[h, k], s2_s.at[i], s2_r.at[i], peer[k])

    def piece(h, j):
        start = sum(PIECES[h][:j])
        return start, PIECES[h][j]

    def g_copy(h, j):
        cl = pl.ds(*piece(h, j))
        i = h * 4 + j
        return remote(g_send.at[h % 2, :, :, cl], g_recv.at[h, :, :, cl], g_s.at[i], g_r.at[i], core_peer)

    def gx_copy(h, j):
        cl = pl.ds(*piece(h, j))
        i = h * 4 + j
        return remote(g_recv.at[h, :, pl.ds(0, SUB), cl], gx_recv.at[h, :, :, cl], gx_s.at[i], gx_r.at[i], x_peer)

    def a_copy(h, j, kind):
        own = c * 2 + xc
        direct = kind == 2 and piece(h, j)[1] < FW
        slot = own if direct else (own, own, c * 2 + 1 - xc)[kind]
        i = (h * 4 + j) * 3 + kind
        ref = a_all.at[h, slot, :, pl.ds(*piece(h, j))]
        return remote(ref, ref, a_s.at[i], a_r.at[i], peer[3] if direct else (core_peer, x_peer, core_peer)[kind])

    def f_copy(h):
        return remote(f_send.at[h], f_recv.at[h], f_s.at[h], f_r.at[h], y_peer)

    lane = lax.broadcasted_iota(jnp.int32, (128, 128), 1)
    sublane = lax.broadcasted_iota(jnp.int32, (128, 128), 0)

    def local_stats(v):
        s = jnp.sum(v, axis=1, keepdims=True)
        q = jnp.sum(v * v, axis=1, keepdims=True)
        n = v.shape[0]
        m = jnp.where(lane[0:n] == 0, s, jnp.where(lane[0:n] == 1, q, 0.0))
        if n < 128:
            m = jnp.concatenate([m, jnp.zeros((128 - n, 128), F32)], axis=0)
        return m.T[0:2]

    def moments(total):
        mean = total[0:1] / full_width
        var = total[1:2] / full_width - mean * mean
        rstd = lax.rsqrt(var + EPS)
        m = jnp.where(sublane == 0, mean, jnp.where(sublane == 1, rstd, 0.0)).T
        return m[:, 0:1], m[:, 1:2]

    def x_own(h, s):
        return x_all[h, s].astype(F32)

    for h in range(NCH):
        x_load(h).start()
    for r in (3, 2, 1, 0):
        for m in range(3):
            qkv_load(r, m).start()
    for tb in tables:
        tb.start()
    barrier = pltpu.get_barrier_semaphore()
    for dev in peer[1:] + other:
        pl.semaphore_signal(barrier, inc=1, device_id=dev, device_id_type=MESH)
    for h in range(NCH):
        x_load(h).wait()
    st1[0] = local_stats(jnp.concatenate([x_own(h, y) for h in range(NCH)], axis=0))
    pl.semaphore_wait(barrier, 7)
    for k in range(1, 8):
        s1_copy(k).start()
    for h in range(NCH):
        xy_copy(h).start()
    wo_load.start()
    for k in range(1, 4):
        s1_copy(k).wait_recv()
    mean_o, rstd_o = moments((st1[0] + st1[1]) + (st1[2] + st1[3]))

    def norm_rows(h, s, mean, rstd):
        sl = slice(h * TOK, (h + 1) * TOK)
        n = ((x_own(h, s) - mean[sl]) * rstd[sl]).astype(BF)
        n_buf[h, pl.ds(pl.multiple_of(s * TOK, TOK), TOK)] = n

    first_parts = [(0, 0), (1, 0), (2, 0), (None, 1)]

    def norm_chunk(h):
        norm_rows(h, y, mean_o, rstd_o)
        xy_copy(h).wait_recv()
        norm_rows(h, 1 - y, *other_moments)

    def qkv_give(h, z):
        for m in range(3):
            d_send[(h * 2 + z) * 3 + m] = dot(n_buf[h], wbuf[(3 - 2 * z) * 3 + m]).astype(BF)
        d_copy(h, z).start()

    def qkv_take(h, z):
        d_copy(h, z).wait_recv()
        for m in range(3):
            i = (h * 2 + z) * 3 + m
            d_recv[i] = (dot(n_buf[h], wbuf[(2 - 2 * z) * 3 + m]) + d_recv[i].astype(F32)).astype(BF)

    def step_qa(h, _):
        if h > 0:
            norm_chunk(h)
            qkv_give(h, 0)
            return
        norm_rows(0, y, mean_o, rstd_o)
        rows = part_rows(0)

        def give(m):
            qkv_wait(3, m)
            d_send[m, rows] = dot(n_buf[0, rows], wbuf[9 + m]).astype(BF)
            d_copy(0, 0, m, 0).start()

        def take(m):
            qkv_wait(2, m)
            own = dot(n_buf[0, rows], wbuf[6 + m])
            d_copy(0, 0, m, 0).wait_recv()
            d_recv[m, rows] = (own + d_recv[m, rows].astype(F32)).astype(BF)
            x_copy(0, m, 0).start()

        give(0)
        give(1)
        take(0)
        give(2)
        take(1)
        take(2)

    def step_qb(h, _):
        if h > 0:
            qkv_take(h, 0)
            return
        for k in range(4, 8):
            s1_copy(k).wait_recv()
        other_moments.extend(moments((st1[4] + st1[5]) + (st1[6] + st1[7])))
        xy_copy(0).wait_recv()
        norm_rows(0, 1 - y, *other_moments)
        rows = part_rows(1)
        for m in range(3):
            d_send[m, rows] = dot(n_buf[0, rows], wbuf[9 + m]).astype(BF)
        d_copy(0, 0, None, 1).start()

    def step_qx(h, _):
        rows = part_rows(1)
        d_copy(0, 0, None, 1).wait_recv()
        for m in range(3):
            d_recv[m, rows] = (dot(n_buf[0, rows], wbuf[6 + m]) + d_recv[m, rows].astype(F32)).astype(BF)
        x_copy(0, None, 1).start()

    def step_qg(h, _):
        if h == 0:
            for m in range(3):
                qkv_wait(1, m)
        qkv_give(h, 1)

    def step_qs(h, _):
        if h > 0:
            x_copy(h).start()

    def step_qc(h, _):
        if h == 0:
            for m in range(3):
                qkv_wait(0, m)
        qkv_take(h, 1)
        if h == 0:
            for j in range(n_full + 1):
                for i in range(2):
                    gu_load(i, j, FW if j < n_full else last_w).start()
        if h == NCH - 1:
            for j in range(n_full + 1):
                for nh in range(2):
                    down_load(j, nh, FW if j < n_full else last_w).start()

    def rotate(v, cos2, sin2):
        f = v.astype(F32)
        return (f * cos2 + pltpu.roll(f, HEAD_DIM // 2, 1) * sin2).astype(BF)

    def step_at(h, _):
        for m, part in first_parts if h == 0 else ((None, None),):
            x_copy(h, m, part).wait_recv()
        if h == 0:
            for tb in tables:
                tb.wait()

        def final(m):
            return (d_recv[h * 6 + 3 + m].astype(F32) + x_recv[h * 3 + m].astype(F32)).astype(BF)

        sl = slice(h * TOK, (h + 1) * TOK)
        n_keys = (h + 1) * TOK
        cos2 = jnp.concatenate([cos_v[sl], cos_v[sl]], axis=0)
        sin2 = jnp.concatenate([sin_v[sl], sin_v[sl]], axis=0)
        q, k, v = final(0), final(1), final(2)
        for s in range(2):
            v_buf[s, sl] = v[s * TOK:(s + 1) * TOK]
        heads = [slice(hd * HEAD_DIM, (hd + 1) * HEAD_DIM) for hd in range(cols // HEAD_DIM)]
        blocks = [(hd, s) for hd in range(len(heads)) for s in range(2)]
        qr = [rotate(q[:, cl], cos2, sin2) for cl in heads]
        kr = [rotate(k[:, cl], cos2, sin2) for cl in heads]
        for hd, s in blocks:
            k_buf[s, sl, heads[hd]] = kr[hd][s * TOK:(s + 1) * TOK]
        scores = jnp.concatenate(
            [dot_t(qr[hd][s * TOK:(s + 1) * TOK], k_buf[s, 0:n_keys, heads[hd]]) for hd, s in blocks], axis=0
        ) * (HEAD_DIM ** -0.5)
        q_pos = h * TOK + lax.rem(lax.broadcasted_iota(jnp.int32, scores.shape, 0), TOK)
        k_pos = lax.broadcasted_iota(jnp.int32, scores.shape, 1)
        scores = jnp.where(q_pos >= k_pos, scores, -1e30)
        e = jnp.exp(scores - jnp.max(scores, axis=1, keepdims=True))
        prob = (e / jnp.sum(e, axis=1, keepdims=True)).astype(BF)
        for i, (hd, s) in enumerate(blocks):
            o = dot(prob[i * TOK:(i + 1) * TOK], v_buf[s, 0:n_keys, heads[hd]])
            o_all[h, t, s * TOK:(s + 1) * TOK, heads[hd]] = o.astype(BF)
        o_copy(h, 1).start()
        o_copy(h, 0).start()

    def step_ro(h, _):
        o_copy(h, 1).wait_recv()
        o_copy(h, 2).start()

    def step_pr(h, _):
        if first_time("wo"):
            wo_load.wait()
        o_copy(h, 0).wait_recv()
        o_copy(h, 2).wait_recv()
        for nh in range(2):
            cl = slice(nh * 512, (nh + 1) * 512)
            res = jnp.zeros((ROWS, 512), F32)
            for b in range(4):
                res = res + dot(o_all[h, b], wo_v[b * cols:(b + 1) * cols, cl])
            p_send[h, :, cl] = res.astype(BF)
            p_copy(h, nh).start()

    def step_re(h, _):
        for nh in range(2):
            p_copy(h, nh).wait_recv()
        attn = (p_send[h].astype(F32) + p_recv[h].astype(F32)).astype(BF).astype(F32)
        xv = jnp.concatenate([x_own(h, 0), x_own(h, 1)], axis=0)
        hv = (xv + attn).astype(BF)
        h_buf[h] = hv
        st2[h, 0] = local_stats(hv.astype(F32))
        for k in range(1, 4):
            s2_copy(h, k).start()

    def step_n2(h, _):
        for k in range(1, 4):
            s2_copy(h, k).wait_recv()
        mean, rstd = moments((st2[h, 0] + st2[h, 1]) + (st2[h, 2] + st2[h, 3]))
        n = ((h_buf[h].astype(F32) - mean[0:ROWS]) * rstd[0:ROWS]).astype(BF)
        for b in range(4):
            e_c = c if b // 2 == 1 else 1 - c
            e_x = xc if b % 2 == 1 else 1 - xc
            n_buf[h, pl.ds(pl.multiple_of(2 * SUB * e_c + SUB * e_x, SUB), SUB)] = n[b * SUB:(b + 1) * SUB]

    def steps(h, j, body):
        start, w = piece(h, j)
        lo, n = start // FW, w // FW
        if n <= 2:
            for kb in range(lo, lo + n):
                body(kb, FW)
        else:
            def step(kb, carry):
                body(kb, FW)
                return carry

            lax.fori_loop(lo, lo + n, step, 0)
        if w % FW:
            body(lo + n, w % FW)

    def step_gm(h, j):
        if first_time("gu"):
            for kb in range(n_full + 1):
                for i in range(2):
                    gu_load(i, kb, FW if kb < n_full else last_w).wait()
        if h >= 2 and j == 0:
            for k in range(len(PIECES[h - 2])):
                g_copy(h - 2, k).wait_send()
        slot = own_slot[h, j]
        start = piece(h, j)[0]

        def body(kb, w):
            for i, wv in enumerate((wg_v, wu_v)):
                for n0 in range(0, w, 512):
                    nw = min(512, w - n0)
                    col = kb * FW + n0
                    if not isinstance(col, int):
                        col = pl.multiple_of(col, 512)
                    res = dot(n_buf[h], wv[:, pl.ds(col, nw)])
                    g_send[h % 2, i, :, pl.ds(col, nw)] = res[0:2 * SUB].astype(BF)
                    g_own[slot, i, :, pl.ds(col - start, nw)] = res[2 * SUB:ROWS]

        steps(h, j, body)
        g_copy(h, j).start()

    def step_ga(h, j):
        slot = own_slot[h, j]
        start, w = piece(h, j)
        cl = slice(start, start + w)
        g_copy(h, j).wait_recv()
        for k in range(2):
            g_recv[h, k, :, cl] = (g_own[slot, k, :, 0:w] + g_recv[h, k, :, cl].astype(F32)).astype(BF)
        gx_copy(h, j).start()

    def step_ac(h, j):
        start, w = piece(h, j)
        cl = slice(start, start + w)
        gx_copy(h, j).wait_recv()
        g, u = [
            (g_recv[h, k, SUB:2 * SUB, cl].astype(F32) + gx_recv[h, k, :, cl].astype(F32)).astype(BF).astype(F32)
            for k in range(2)
        ]
        a_all[h, c * 2 + xc, :, cl] = (g * (1.0 / (1.0 + jnp.exp(-g))) * u).astype(BF)
        a_copy(h, j, 1).start()
        if w < FW:
            a_copy(h, j, 2).start()
        a_copy(h, j, 0).start()

    def step_ra(h, j):
        a_copy(h, j, 1).wait_recv()
        if piece(h, j)[1] >= FW:
            a_copy(h, j, 2).start()

    def step_dn(h, j):
        if first_time("down"):
            for kb in range(n_full + 1):
                for nh in range(2):
                    down_load(kb, nh, FW if kb < n_full else last_w).wait()
        a_copy(h, j, 0).wait_recv()
        a_copy(h, j, 2).wait_recv()
        if j == 0:
            acc[h] = jnp.zeros((ROWS, width), F32)

        def body(kb, w):
            col = kb * FW if isinstance(kb, int) else pl.multiple_of(kb * FW, FW)
            lhs = a_all[h, :, :, pl.ds(col, w)].reshape(ROWS, w)
            for nh in range(2):
                acc[h, :, nh * 512:(nh + 1) * 512] += dot(lhs, wbuf[kb * 2 + nh, 0:w])

        steps(h, j, body)

    def step_fi(h, _):
        f_send[h] = acc[h, seq_rows(1 - y)].astype(BF)
        f_copy(h).start()

    def step_ou(h, _):
        own = pl.ds(pl.multiple_of(y * TOK, TOK), TOK)
        f_copy(h).wait_recv()
        mlp = (acc[h, own].astype(BF).astype(F32) + f_recv[h].astype(F32)).astype(BF).astype(F32)
        out_ref[0, h * TOK:(h + 1) * TOK] = (h_buf[h, own].astype(F32) + mlp).astype(BF)

    other_moments = []
    seen = set()

    def first_time(name):
        new = name not in seen
        seen.add(name)
        return new

    own_slot, free = {}, list(range(g_own.shape[0]))
    program = [(w[:2], int(w[2]), int(w[3:] or 0)) for line in ORDER for w in line.split()]
    for name, h, j in program:
        if name == "gm":
            own_slot[h, j] = free.pop(0)
        if name == "ga":
            free.append(own_slot[h, j])
    step_of = dict(qa=step_qa, qb=step_qb, qx=step_qx, qg=step_qg, qs=step_qs, qc=step_qc, at=step_at, ro=step_ro, pr=step_pr, re=step_re, n2=step_n2,
                   gm=step_gm, ga=step_ga, ac=step_ac, ra=step_ra, dn=step_dn, fi=step_fi, ou=step_ou)
    for name, h, j in program:
        step_of[name](h, j)

    for k in range(1, 8):
        s1_copy(k).wait_send()
    for h in range(NCH):
        xy_copy(h).wait_send()
        for m, part in first_parts if h == 0 else ((None, None),):
            d_copy(h, 0, m, part).wait_send()
            x_copy(h, m, part).wait_send()
        d_copy(h, 1).wait_send()
        for m in range(3):
            s2_copy(h, m + 1).wait_send()
            o_copy(h, m).wait_send()
        for nh in range(2):
            p_copy(h, nh).wait_send()
        for j in range(len(PIECES[h])):
            if h >= NCH - 2:
                g_copy(h, j).wait_send()
            gx_copy(h, j).wait_send()
            for kind in range(3):
                a_copy(h, j, kind).wait_send()
        f_copy(h).wait_send()


def solution(mesh):
    act_spec = P(("dp", "ty"), None, "tx")
    col_spec = P("tx", "ty")
    row_spec = P("ty", "tx")

    def layer_fn(x_blk, w_q, w_k, w_v, w_o, w_gate, w_up, w_down):
        seq_len, width = x_blk.shape[1:]
        cols = w_q.shape[1] // 4
        ff = w_gate.shape[1]
        cos_t, sin_t = (jnp.asarray(a) for a in rotary_tables(seq_len))
        dma = pltpu.SemaphoreType.DMA
        vm = pltpu.VMEM
        return pl.pallas_call(
            layer_kernel,
            out_shape=pltpu.VMEM(x_blk.shape, BF),
            in_specs=[pl.BlockSpec(memory_space=pl.ANY)] * 10,
            out_specs=pl.BlockSpec(memory_space=pltpu.VMEM),
            scratch_shapes=[
                vm((12, width, cols), BF),
                vm(w_o.shape, BF),
                vm(w_gate.shape, BF),
                vm(w_up.shape, BF),
                vm((seq_len, HEAD_DIM), F32),
                vm((seq_len, HEAD_DIM), F32),
                vm((NCH, 2, TOK, width), BF),
                vm((NCH, ROWS, width), BF),
                vm((6 * NCH, ROWS, cols), BF),
                vm((6 * NCH, ROWS, cols), BF),
                vm((3 * NCH, ROWS, cols), BF),
                vm((2, seq_len, cols), BF),
                vm((2, seq_len, cols), BF),
                vm((NCH, 4, ROWS, cols), BF),
                vm((NCH, ROWS, width), BF),
                vm((NCH, ROWS, width), BF),
                vm((NCH, ROWS, width), BF),
                vm((2, 2, 2 * SUB, ff), BF),
                vm((NCH, 2, 2 * SUB, ff), BF),
                vm((3, 2, 2 * SUB, max(max(p) for p in PIECES)), F32),
                vm((NCH, 2, SUB, ff), BF),
                vm((NCH, 4, SUB, ff), BF),
                vm((NCH, ROWS, width), F32),
                vm((NCH, TOK, width), BF),
                vm((NCH, TOK, width), BF),
                vm((8, 2, 128), F32),
                vm((NCH, 4, 2, 128), F32),
                dma((NCH + 2,)), dma((48,)),
                *(dma((n,)) for n in (NCH, 8, 6 * NCH + 1, 3 * NCH + 1, 3 * NCH, 2 * NCH, 4 * NCH, 4 * NCH, 4 * NCH, 12 * NCH, NCH) for _ in range(2)),
            ],
            compiler_params=pltpu.CompilerParams(collective_id=0, has_side_effects=True, vmem_limit_bytes=66256896),
            name="layer",
        )(x_blk, w_q, w_k, w_v, w_o, w_gate, w_up, w_down, cos_t, sin_t)

    return jax.shard_map(layer_fn, mesh=mesh, in_specs=(act_spec, col_spec, col_spec, col_spec, row_spec, col_spec, col_spec, row_spec), out_specs=act_spec, check_vma=False)
```

```python
import numpy as np

import jax
import jax.numpy as jnp
from jax import lax
from jax.experimental import pallas as pl
from jax.experimental.pallas import tpu as pltpu
from jax.sharding import PartitionSpec as P

HEAD_DIM = 128
EPS = 1e-5
THETA = 10000.0
BF = jnp.bfloat16
F32 = jnp.float32
MESH = pl.DeviceIdType.MESH

NCH = 4
TOK = 32
ROWS = 2 * TOK
SUB = ROWS // 4
FW = 1024

PIECES = ((1024, 2048, 2432), (2048, 2048, 1408), (3072, 2432), (2048, 2048, 1408))
ORDER = (
    "qa0 qb0 qa1 qx0", "qb1 qs1 qs0 qg0", "qa2 qc0 qb2 at0", "qs2 qg1 qa3 qc1",
    "qg2 ro0 qb3 pr0", "at1 qc2 at2 ro1", "re0 qg3 qs3 pr1", "n20 gm00 gm01 ga00",
    "ro2 qc3 re1 ga01", "gm02 at3 n21 ga02", "gm10 pr2 ac01 ro3", "ga10 gm11 pr3 re2",
    "gm12 ra01 ga11 re3", "ac02 n22 ac00 ga12", "ac11 ac10 n23 gm20", "ga20 gm21 ra00 gm30",
    "ac12 ra02 ga21 ga30", "ra10 gm31 ac20 dn00", "dn10 ac21 ra11 ga31", "dn11 dn01 gm32 ra20",
    "dn02 ra21 ra12 ga32", "ac30 ac31 dn20 fi0", "ac32 dn21 ra30 dn12", "fi1 fi2 ra31 dn30",
    "ra32 dn31 dn32 fi3", "ou2 ou1 ou0 ou3",
)


def dot(a, b):
    return jnp.dot(a, b, preferred_element_type=F32)


def dot_t(a, b):
    return lax.dot_general(a, b, (((1,), (1,)), ((), ())), preferred_element_type=F32)


def rotary_tables(seq_len):
    half_dim = HEAD_DIM // 2
    inv_freq = (np.float32(THETA) ** (np.float32(-2.0) * np.arange(half_dim, dtype=np.float32) / np.float32(HEAD_DIM))).astype(np.float32)
    angles = np.arange(seq_len, dtype=np.float32)[:, None] * inv_freq[None, :]
    cos_t = np.cos(angles.astype(np.float64)).astype(np.float32)
    sin_t = np.sin(angles.astype(np.float64)).astype(np.float32)
    return np.concatenate([cos_t, cos_t], 1), np.concatenate([-sin_t, sin_t], 1)


def layer_kernel(x_hbm, wq_hbm, wk_hbm, wv_hbm, wo_hbm, wg_hbm, wu_hbm, wd_hbm, cos_hbm, sin_hbm, out_ref,
                 wbuf, wo_v, wg_v, wu_v, cos_v, sin_v, x_all, n_buf, d_send, d_recv, x_recv, k_buf, v_buf, o_all,
                 p_send, p_recv, h_buf, g_send, g_recv, g_own, gx_recv, a_all, acc, f_send, f_recv, st1, st2,
                 ld_sem, w_sem, xy_s, xy_r, s1_s, s1_r, d_s, d_r, x_s, x_r, o_s, o_r, p_s, p_r, s2_s, s2_r,
                 g_s, g_r, gx_s, gx_r, a_s, a_r, f_s, f_r):
    dp = lax.axis_index("dp")
    y = lax.axis_index("ty")
    t = lax.axis_index("tx")
    xc = lax.div(t, 2)
    c = lax.rem(t, 2)
    width = x_hbm.shape[2]
    cols = wq_hbm.shape[1] // 4
    ff = wg_hbm.shape[1]
    n_full = ff // FW
    last_w = ff - n_full * FW
    full_width = 4 * width
    rel = [t, t + 1 - 2 * c, t + 2 - 4 * xc, 3 - t]
    peer = [(dp, y, r) for r in rel]
    other = [(dp, 1 - y, r) for r in rel]
    core_peer, x_peer, y_peer = peer[1], peer[2], other[0]

    def remote(src, dst, ss, rs, dev):
        return pltpu.make_async_remote_copy(src_ref=src, dst_ref=dst, send_sem=ss, recv_sem=rs, device_id=dev, device_id_type=MESH)

    def x_load(h):
        return pltpu.make_async_copy(x_hbm.at[0, pl.ds(h * TOK, TOK)], x_all.at[h, y], ld_sem.at[h])

    tables = [pltpu.make_async_copy(cos_hbm, cos_v, ld_sem.at[NCH]), pltpu.make_async_copy(sin_hbm, sin_v, ld_sem.at[NCH + 1])]

    def qkv_load(r, m):
        src = (wq_hbm, wk_hbm, wv_hbm)[m].at[:, pl.ds(pl.multiple_of(rel[r] * cols, cols), cols)]
        return pltpu.make_async_copy(src, wbuf.at[r * 3 + m], w_sem.at[r * 3 + m])

    def qkv_wait(r, m):
        pltpu.make_async_copy(wq_hbm.at[:, pl.ds(0, cols)], wbuf.at[r * 3 + m], w_sem.at[r * 3 + m]).wait()

    wo_load = pltpu.make_async_copy(wo_hbm, wo_v, w_sem.at[12])

    def gu_load(i, j, w):
        src, dst = ((wg_hbm, wg_v), (wu_hbm, wu_v))[i]
        start = j * FW if isinstance(j, int) else pl.multiple_of(j * FW, FW)
        return pltpu.make_async_copy(src.at[:, pl.ds(start, w)], dst.at[:, pl.ds(start, w)], w_sem.at[16 + i * 8 + j])

    def down_load(j, nh, w):
        start = j * FW if isinstance(j, int) else pl.multiple_of(j * FW, FW)
        return pltpu.make_async_copy(wd_hbm.at[pl.ds(start, w), pl.ds(nh * 512, 512)], wbuf.at[j * 2 + nh, pl.ds(0, w)], w_sem.at[32 + j * 2 + nh])

    def xy_copy(h):
        return remote(x_all.at[h, y], x_all.at[h, y], xy_s.at[h], xy_r.at[h], y_peer)

    def s1_copy(k):
        return remote(st1.at[0], st1.at[k], s1_s.at[k], s1_r.at[k], peer[k] if k < 4 else other[k - 4])

    def seq_rows(s):
        return pl.ds(pl.multiple_of(s * TOK, TOK), TOK)

    def part_rows(part):
        return seq_rows(y if part == 0 else 1 - y)

    def d_copy(h, z, m=None, part=None):
        i = (h * 2 + z) * 3 + (0 if m is None else m)
        sl = pl.ds(i, 3) if m is None else i
        src, dst = (d_send.at[sl], d_recv.at[sl]) if part is None else (d_send.at[sl, part_rows(part)], d_recv.at[sl, part_rows(part)])
        k = 6 * NCH if part == 1 else i
        return remote(src, dst, d_s.at[k], d_r.at[k], core_peer)

    def x_copy(h, m=None, part=None):
        i = h * 3 + (0 if m is None else m)
        k = h * 6 + (0 if m is None else m)
        ssl, dsl = (pl.ds(k, 3), pl.ds(i, 3)) if m is None else (k, i)
        src, dst = (d_recv.at[ssl], x_recv.at[dsl]) if part is None else (d_recv.at[ssl, part_rows(part)], x_recv.at[dsl, part_rows(part)])
        n = 3 * NCH if part == 1 else i
        return remote(src, dst, x_s.at[n], x_r.at[n], x_peer)

    def o_copy(h, kind):
        slot = (t, t, rel[2])[kind]
        i = h * 3 + kind
        ref = o_all.at[h, slot]
        return remote(ref, ref, o_s.at[i], o_r.at[i], (core_peer, x_peer, core_peer)[kind])

    def p_copy(h, nh):
        cl = pl.ds(nh * 512, 512)
        return remote(p_send.at[h, :, cl], p_recv.at[h, :, cl], p_s.at[h * 2 + nh], p_r.at[h * 2 + nh], y_peer)

    def s2_copy(h, k):
        i = h * 4 + k
        return remote(st2.at[h, 0], st2.at[h, k], s2_s.at[i], s2_r.at[i], peer[k])

    def piece(h, j):
        start = sum(PIECES[h][:j])
        return start, PIECES[h][j]

    def g_copy(h, j):
        cl = pl.ds(*piece(h, j))
        i = h * 4 + j
        return remote(g_send.at[h % 2, :, :, cl], g_recv.at[h, :, :, cl], g_s.at[i], g_r.at[i], core_peer)

    def gx_copy(h, j):
        cl = pl.ds(*piece(h, j))
        i = h * 4 + j
        return remote(g_recv.at[h, :, pl.ds(0, SUB), cl], gx_recv.at[h, :, :, cl], gx_s.at[i], gx_r.at[i], x_peer)

    def a_copy(h, j, kind):
        own = c * 2 + xc
        direct = kind == 2 and piece(h, j)[1] < FW
        slot = own if direct else (own, own, c * 2 + 1 - xc)[kind]
        i = (h * 4 + j) * 3 + kind
        ref = a_all.at[h, slot, :, pl.ds(*piece(h, j))]
        return remote(ref, ref, a_s.at[i], a_r.at[i], peer[3] if direct else (core_peer, x_peer, core_peer)[kind])

    def f_copy(h):
        return remote(f_send.at[h], f_recv.at[h], f_s.at[h], f_r.at[h], y_peer)

    lane = lax.broadcasted_iota(jnp.int32, (128, 128), 1)
    sublane = lax.broadcasted_iota(jnp.int32, (128, 128), 0)

    def local_stats(v):
        s = jnp.sum(v, axis=1, keepdims=True)
        q = jnp.sum(v * v, axis=1, keepdims=True)
        n = v.shape[0]
        m = jnp.where(lane[0:n] == 0, s, jnp.where(lane[0:n] == 1, q, 0.0))
        if n < 128:
            m = jnp.concatenate([m, jnp.zeros((128 - n, 128), F32)], axis=0)
        return m.T[0:2]

    def moments(total):
        mean = total[0:1] / full_width
        var = total[1:2] / full_width - mean * mean
        rstd = lax.rsqrt(var + EPS)
        m = jnp.where(sublane == 0, mean, jnp.where(sublane == 1, rstd, 0.0)).T
        return m[:, 0:1], m[:, 1:2]

    def x_own(h, s):
        return x_all[h, s].astype(F32)

    for h in range(NCH):
        x_load(h).start()
    for r in (3, 2, 1, 0):
        for m in range(3):
            qkv_load(r, m).start()
    for tb in tables:
        tb.start()
    barrier = pltpu.get_barrier_semaphore()
    for dev in peer[1:] + other:
        pl.semaphore_signal(barrier, inc=1, device_id=dev, device_id_type=MESH)
    for h in range(NCH):
        x_load(h).wait()
    st1[0] = local_stats(jnp.concatenate([x_own(h, y) for h in range(NCH)], axis=0))
    pl.semaphore_wait(barrier, 7)
    for k in range(1, 8):
        s1_copy(k).start()
    for h in range(NCH):
        xy_copy(h).start()
    wo_load.start()
    for k in range(1, 4):
        s1_copy(k).wait_recv()
    mean_o, rstd_o = moments((st1[0] + st1[1]) + (st1[2] + st1[3]))

    def norm_rows(h, s, mean, rstd):
        sl = slice(h * TOK, (h + 1) * TOK)
        n = ((x_own(h, s) - mean[sl]) * rstd[sl]).astype(BF)
        n_buf[h, pl.ds(pl.multiple_of(s * TOK, TOK), TOK)] = n

    first_parts = [(0, 0), (1, 0), (2, 0), (None, 1)]

    def norm_chunk(h):
        norm_rows(h, y, mean_o, rstd_o)
        xy_copy(h).wait_recv()
        norm_rows(h, 1 - y, *other_moments)

    def qkv_give(h, z):
        for m in range(3):
            d_send[(h * 2 + z) * 3 + m] = dot(n_buf[h], wbuf[(3 - 2 * z) * 3 + m]).astype(BF)
        d_copy(h, z).start()

    def qkv_take(h, z):
        d_copy(h, z).wait_recv()
        for m in range(3):
            i = (h * 2 + z) * 3 + m
            d_recv[i] = (dot(n_buf[h], wbuf[(2 - 2 * z) * 3 + m]) + d_recv[i].astype(F32)).astype(BF)

    def step_qa(h, _):
        if h > 0:
            norm_chunk(h)
            qkv_give(h, 0)
            return
        norm_rows(0, y, mean_o, rstd_o)
        rows = part_rows(0)

        def give(m):
            qkv_wait(3, m)
            d_send[m, rows] = dot(n_buf[0, rows], wbuf[9 + m]).astype(BF)
            d_copy(0, 0, m, 0).start()

        def take(m):
            qkv_wait(2, m)
            own = dot(n_buf[0, rows], wbuf[6 + m])
            d_copy(0, 0, m, 0).wait_recv()
            d_recv[m, rows] = (own + d_recv[m, rows].astype(F32)).astype(BF)
            x_copy(0, m, 0).start()

        give(0)
        give(1)
        take(0)
        give(2)
        take(1)
        take(2)

    def step_qb(h, _):
        if h > 0:
            qkv_take(h, 0)
            return
        for k in range(4, 8):
            s1_copy(k).wait_recv()
        other_moments.extend(moments((st1[4] + st1[5]) + (st1[6] + st1[7])))
        xy_copy(0).wait_recv()
        norm_rows(0, 1 - y, *other_moments)
        rows = part_rows(1)
        for m in range(3):
            d_send[m, rows] = dot(n_buf[0, rows], wbuf[9 + m]).astype(BF)
        d_copy(0, 0, None, 1).start()

    def step_qx(h, _):
        rows = part_rows(1)
        d_copy(0, 0, None, 1).wait_recv()
        for m in range(3):
            d_recv[m, rows] = (dot(n_buf[0, rows], wbuf[6 + m]) + d_recv[m, rows].astype(F32)).astype(BF)
        x_copy(0, None, 1).start()

    def step_qg(h, _):
        if h == 0:
            for m in range(3):
                qkv_wait(1, m)
        qkv_give(h, 1)

    def step_qs(h, _):
        if h > 0:
            x_copy(h).start()

    def step_qc(h, _):
        if h == 0:
            for m in range(3):
                qkv_wait(0, m)
        qkv_take(h, 1)
        if h == 0:
            for j in range(n_full + 1):
                for i in range(2):
                    gu_load(i, j, FW if j < n_full else last_w).start()
        if h == NCH - 1:
            for j in range(n_full + 1):
                for nh in range(2):
                    down_load(j, nh, FW if j < n_full else last_w).start()

    def rotate(v, cos2, sin2):
        f = v.astype(F32)
        return (f * cos2 + pltpu.roll(f, HEAD_DIM // 2, 1) * sin2).astype(BF)

    def step_at(h, _):
        for m, part in first_parts if h == 0 else ((None, None),):
            x_copy(h, m, part).wait_recv()
        if h == 0:
            for tb in tables:
                tb.wait()

        def final(m):
            return (d_recv[h * 6 + 3 + m].astype(F32) + x_recv[h * 3 + m].astype(F32)).astype(BF)

        sl = slice(h * TOK, (h + 1) * TOK)
        n_keys = (h + 1) * TOK
        cos2 = jnp.concatenate([cos_v[sl], cos_v[sl]], axis=0)
        sin2 = jnp.concatenate([sin_v[sl], sin_v[sl]], axis=0)
        q, k, v = final(0), final(1), final(2)
        for s in range(2):
            v_buf[s, sl] = v[s * TOK:(s + 1) * TOK]
        heads = [slice(hd * HEAD_DIM, (hd + 1) * HEAD_DIM) for hd in range(cols // HEAD_DIM)]
        blocks = [(hd, s) for hd in range(len(heads)) for s in range(2)]
        qr = [rotate(q[:, cl], cos2, sin2) for cl in heads]
        kr = [rotate(k[:, cl], cos2, sin2) for cl in heads]
        for hd, s in blocks:
            k_buf[s, sl, heads[hd]] = kr[hd][s * TOK:(s + 1) * TOK]
        scores = jnp.concatenate(
            [dot_t(qr[hd][s * TOK:(s + 1) * TOK], k_buf[s, 0:n_keys, heads[hd]]) for hd, s in blocks], axis=0
        ) * (HEAD_DIM ** -0.5)
        q_pos = h * TOK + lax.rem(lax.broadcasted_iota(jnp.int32, scores.shape, 0), TOK)
        k_pos = lax.broadcasted_iota(jnp.int32, scores.shape, 1)
        scores = jnp.where(q_pos >= k_pos, scores, -1e30)
        e = jnp.exp(scores - jnp.max(scores, axis=1, keepdims=True))
        prob = (e / jnp.sum(e, axis=1, keepdims=True)).astype(BF)
        for i, (hd, s) in enumerate(blocks):
            o = dot(prob[i * TOK:(i + 1) * TOK], v_buf[s, 0:n_keys, heads[hd]])
            o_all[h, t, s * TOK:(s + 1) * TOK, heads[hd]] = o.astype(BF)
        o_copy(h, 1).start()
        o_copy(h, 0).start()

    def step_ro(h, _):
        o_copy(h, 1).wait_recv()
        o_copy(h, 2).start()

    def step_pr(h, _):
        if first_time("wo"):
            wo_load.wait()
        o_copy(h, 0).wait_recv()
        o_copy(h, 2).wait_recv()
        for nh in range(2):
            cl = slice(nh * 512, (nh + 1) * 512)
            res = jnp.zeros((ROWS, 512), F32)
            for b in range(4):
                res = res + dot(o_all[h, b], wo_v[b * cols:(b + 1) * cols, cl])
            p_send[h, :, cl] = res.astype(BF)
            p_copy(h, nh).start()

    def step_re(h, _):
        for nh in range(2):
            p_copy(h, nh).wait_recv()
        attn = (p_send[h].astype(F32) + p_recv[h].astype(F32)).astype(BF).astype(F32)
        xv = jnp.concatenate([x_own(h, 0), x_own(h, 1)], axis=0)
        hv = (xv + attn).astype(BF)
        h_buf[h] = hv
        st2[h, 0] = local_stats(hv.astype(F32))
        for k in range(1, 4):
            s2_copy(h, k).start()

    def step_n2(h, _):
        for k in range(1, 4):
            s2_copy(h, k).wait_recv()
        mean, rstd = moments((st2[h, 0] + st2[h, 1]) + (st2[h, 2] + st2[h, 3]))
        n = ((h_buf[h].astype(F32) - mean[0:ROWS]) * rstd[0:ROWS]).astype(BF)
        for b in range(4):
            e_c = c if b // 2 == 1 else 1 - c
            e_x = xc if b % 2 == 1 else 1 - xc
            n_buf[h, pl.ds(pl.multiple_of(2 * SUB * e_c + SUB * e_x, SUB), SUB)] = n[b * SUB:(b + 1) * SUB]

    def steps(h, j, body):
        start, w = piece(h, j)
        lo, n = start // FW, w // FW
        if n <= 1:
            for kb in range(lo, lo + n):
                body(kb, FW)
        else:
            def step(kb, carry):
                body(kb, FW)
                return carry

            lax.fori_loop(lo, lo + n, step, 0)
        if w % FW:
            body(lo + n, w % FW)

    def step_gm(h, j):
        if first_time("gu"):
            for kb in range(n_full + 1):
                for i in range(2):
                    gu_load(i, kb, FW if kb < n_full else last_w).wait()
        if h >= 2 and j == 0:
            for k in range(len(PIECES[h - 2])):
                g_copy(h - 2, k).wait_send()
        slot = own_slot[h, j]
        start = piece(h, j)[0]

        def body(kb, w):
            for i, wv in enumerate((wg_v, wu_v)):
                for n0 in range(0, w, 512):
                    nw = min(512, w - n0)
                    col = kb * FW + n0
                    if not isinstance(col, int):
                        col = pl.multiple_of(col, 512)
                    res = dot(n_buf[h], wv[:, pl.ds(col, nw)])
                    g_send[h % 2, i, :, pl.ds(col, nw)] = res[0:2 * SUB].astype(BF)
                    g_own[slot, i, :, pl.ds(col - start, nw)] = res[2 * SUB:ROWS]

        steps(h, j, body)
        g_copy(h, j).start()

    def step_ga(h, j):
        slot = own_slot[h, j]
        start, w = piece(h, j)
        cl = slice(start, start + w)
        g_copy(h, j).wait_recv()
        for k in range(2):
            g_recv[h, k, :, cl] = (g_own[slot, k, :, 0:w] + g_recv[h, k, :, cl].astype(F32)).astype(BF)
        gx_copy(h, j).start()

    def step_ac(h, j):
        start, w = piece(h, j)
        cl = slice(start, start + w)
        gx_copy(h, j).wait_recv()
        g, u = [
            (g_recv[h, k, SUB:2 * SUB, cl].astype(F32) + gx_recv[h, k, :, cl].astype(F32)).astype(BF).astype(F32)
            for k in range(2)
        ]
        a_all[h, c * 2 + xc, :, cl] = (g * (1.0 / (1.0 + jnp.exp(-g))) * u).astype(BF)
        a_copy(h, j, 1).start()
        if w < FW:
            a_copy(h, j, 2).start()
        a_copy(h, j, 0).start()

    def step_ra(h, j):
        a_copy(h, j, 1).wait_recv()
        if piece(h, j)[1] >= FW:
            a_copy(h, j, 2).start()

    def step_dn(h, j):
        if first_time("down"):
            for kb in range(n_full + 1):
                for nh in range(2):
                    down_load(kb, nh, FW if kb < n_full else last_w).wait()
        a_copy(h, j, 0).wait_recv()
        a_copy(h, j, 2).wait_recv()
        if j == 0:
            acc[h] = jnp.zeros((ROWS, width), F32)

        def body(kb, w):
            col = kb * FW if isinstance(kb, int) else pl.multiple_of(kb * FW, FW)
            lhs = a_all[h, :, :, pl.ds(col, w)].reshape(ROWS, w)
            for nh in range(2):
                acc[h, :, nh * 512:(nh + 1) * 512] += dot(lhs, wbuf[kb * 2 + nh, 0:w])

        steps(h, j, body)

    def step_fi(h, _):
        f_send[h] = acc[h, seq_rows(1 - y)].astype(BF)
        f_copy(h).start()

    def step_ou(h, _):
        own = pl.ds(pl.multiple_of(y * TOK, TOK), TOK)
        f_copy(h).wait_recv()
        mlp = (acc[h, own].astype(BF).astype(F32) + f_recv[h].astype(F32)).astype(BF).astype(F32)
        out_ref[0, h * TOK:(h + 1) * TOK] = (h_buf[h, own].astype(F32) + mlp).astype(BF)

    other_moments = []
    seen = set()

    def first_time(name):
        new = name not in seen
        seen.add(name)
        return new

    own_slot, free = {}, list(range(g_own.shape[0]))
    program = [(w[:2], int(w[2]), int(w[3:] or 0)) for line in ORDER for w in line.split()]
    for name, h, j in program:
        if name == "gm":
            own_slot[h, j] = free.pop(0)
        if name == "ga":
            free.append(own_slot[h, j])
    step_of = dict(qa=step_qa, qb=step_qb, qx=step_qx, qg=step_qg, qs=step_qs, qc=step_qc, at=step_at, ro=step_ro, pr=step_pr, re=step_re, n2=step_n2,
                   gm=step_gm, ga=step_ga, ac=step_ac, ra=step_ra, dn=step_dn, fi=step_fi, ou=step_ou)
    for name, h, j in program:
        step_of[name](h, j)

    for k in range(1, 8):
        s1_copy(k).wait_send()
    for h in range(NCH):
        xy_copy(h).wait_send()
        for m, part in first_parts if h == 0 else ((None, None),):
            d_copy(h, 0, m, part).wait_send()
            x_copy(h, m, part).wait_send()
        d_copy(h, 1).wait_send()
        for m in range(3):
            s2_copy(h, m + 1).wait_send()
            o_copy(h, m).wait_send()
        for nh in range(2):
            p_copy(h, nh).wait_send()
        for j in range(len(PIECES[h])):
            if h >= NCH - 2:
                g_copy(h, j).wait_send()
            gx_copy(h, j).wait_send()
            for kind in range(3):
                a_copy(h, j, kind).wait_send()
        f_copy(h).wait_send()


def solution(mesh):
    act_spec = P(("dp", "ty"), None, "tx")
    col_spec = P("tx", "ty")
    row_spec = P("ty", "tx")

    def layer_fn(x_blk, w_q, w_k, w_v, w_o, w_gate, w_up, w_down):
        seq_len, width = x_blk.shape[1:]
        cols = w_q.shape[1] // 4
        ff = w_gate.shape[1]
        cos_t, sin_t = (jnp.asarray(a) for a in rotary_tables(seq_len))
        dma = pltpu.SemaphoreType.DMA
        vm = pltpu.VMEM
        return pl.pallas_call(
            layer_kernel,
            out_shape=pltpu.VMEM(x_blk.shape, BF),
            in_specs=[pl.BlockSpec(memory_space=pl.ANY)] * 10,
            out_specs=pl.BlockSpec(memory_space=pltpu.VMEM),
            scratch_shapes=[
                vm((12, width, cols), BF),
                vm(w_o.shape, BF),
                vm(w_gate.shape, BF),
                vm(w_up.shape, BF),
                vm((seq_len, HEAD_DIM), F32),
                vm((seq_len, HEAD_DIM), F32),
                vm((NCH, 2, TOK, width), BF),
                vm((NCH, ROWS, width), BF),
                vm((6 * NCH, ROWS, cols), BF),
                vm((6 * NCH, ROWS, cols), BF),
                vm((3 * NCH, ROWS, cols), BF),
                vm((2, seq_len, cols), BF),
                vm((2, seq_len, cols), BF),
                vm((NCH, 4, ROWS, cols), BF),
                vm((NCH, ROWS, width), BF),
                vm((NCH, ROWS, width), BF),
                vm((NCH, ROWS, width), BF),
                vm((2, 2, 2 * SUB, ff), BF),
                vm((NCH, 2, 2 * SUB, ff), BF),
                vm((3, 2, 2 * SUB, max(max(p) for p in PIECES)), F32),
                vm((NCH, 2, SUB, ff), BF),
                vm((NCH, 4, SUB, ff), BF),
                vm((NCH, ROWS, width), F32),
                vm((NCH, TOK, width), BF),
                vm((NCH, TOK, width), BF),
                vm((8, 2, 128), F32),
                vm((NCH, 4, 2, 128), F32),
                dma((NCH + 2,)), dma((48,)),
                *(dma((n,)) for n in (NCH, 8, 6 * NCH + 1, 3 * NCH + 1, 3 * NCH, 2 * NCH, 4 * NCH, 4 * NCH, 4 * NCH, 12 * NCH, NCH) for _ in range(2)),
            ],
            compiler_params=pltpu.CompilerParams(collective_id=0, has_side_effects=True, vmem_limit_bytes=66256896),
            name="layer",
        )(x_blk, w_q, w_k, w_v, w_o, w_gate, w_up, w_down, cos_t, sin_t)

    return jax.shard_map(layer_fn, mesh=mesh, in_specs=(act_spec, col_spec, col_spec, col_spec, row_spec, col_spec, col_spec, row_spec), out_specs=act_spec, check_vma=False)
```

```python
import numpy as np

import jax
import jax.numpy as jnp
from jax import lax
from jax.experimental import pallas as pl
from jax.experimental.pallas import tpu as pltpu
from jax.sharding import PartitionSpec as P

HEAD_DIM = 128
EPS = 1e-5
THETA = 10000.0
BF = jnp.bfloat16
F32 = jnp.float32
MESH = pl.DeviceIdType.MESH

NCH = 4
TOK = 32
ROWS = 2 * TOK
SUB = ROWS // 4
FW = 1024

PIECES = ((1024, 2048, 2432), (2048, 2048, 1408), (3072, 2432), (2048, 2048, 1408))
ORDER = (
    "qa0 qb0 qa1 qx0", "qb1 qs1 qs0 qg0", "qa2 qc0 qb2 at0", "qs2 qg1 qa3 qc1",
    "qg2 ro0 qb3 pr0", "at1 qc2 at2 ro1", "re0 qg3 qs3 pr1", "n20 gm00 gm01 ga00",
    "ro2 qc3 re1 ga01", "gm02 at3 n21 ga02", "gm10 pr2 ac01 ro3", "ga10 gm11 pr3 re2",
    "gm12 ra01 ga11 re3", "ac02 n22 ac00 ga12", "ac11 ac10 n23 gm20", "ga20 gm21 ra00 gm30",
    "ac12 ra02 ga21 ga30", "ra10 gm31 ac20 dn00", "dn10 ac21 ra11 ga31", "dn11 dn01 gm32 ra20",
    "dn02 ra21 ra12 ga32", "ac30 ac31 dn20 fi0", "ac32 dn21 ra30 dn12", "fi1 fi2 ra31 dn30",
    "ra32 dn31 dn32 fi3", "ou2 ou1 ou0 ou3",
)


def dot(a, b):
    return jnp.dot(a, b, preferred_element_type=F32)


def dot_t(a, b):
    return lax.dot_general(a, b, (((1,), (1,)), ((), ())), preferred_element_type=F32)


def rotary_tables(seq_len):
    half_dim = HEAD_DIM // 2
    inv_freq = (np.float32(THETA) ** (np.float32(-2.0) * np.arange(half_dim, dtype=np.float32) / np.float32(HEAD_DIM))).astype(np.float32)
    angles = np.arange(seq_len, dtype=np.float32)[:, None] * inv_freq[None, :]
    cos_t = np.cos(angles.astype(np.float64)).astype(np.float32)
    sin_t = np.sin(angles.astype(np.float64)).astype(np.float32)
    return np.concatenate([cos_t, cos_t], 1), np.concatenate([-sin_t, sin_t], 1)


def layer_kernel(x_hbm, wq_hbm, wk_hbm, wv_hbm, wo_hbm, wg_hbm, wu_hbm, wd_hbm, cos_hbm, sin_hbm, out_ref,
                 wbuf, wo_v, wg_v, wu_v, cos_v, sin_v, x_all, n_buf, d_send, d_recv, x_recv, k_buf, v_buf, o_all,
                 p_send, p_recv, h_buf, g_send, g_recv, g_own, gx_recv, a_all, acc, f_send, f_recv, st1, st2,
                 ld_sem, w_sem, xy_s, xy_r, s1_s, s1_r, d_s, d_r, x_s, x_r, o_s, o_r, p_s, p_r, s2_s, s2_r,
                 g_s, g_r, gx_s, gx_r, a_s, a_r, f_s, f_r):
    dp = lax.axis_index("dp")
    y = lax.axis_index("ty")
    t = lax.axis_index("tx")
    xc = lax.div(t, 2)
    c = lax.rem(t, 2)
    width = x_hbm.shape[2]
    cols = wq_hbm.shape[1] // 4
    ff = wg_hbm.shape[1]
    n_full = ff // FW
    last_w = ff - n_full * FW
    full_width = 4 * width
    rel = [t, t + 1 - 2 * c, t + 2 - 4 * xc, 3 - t]
    peer = [(dp, y, r) for r in rel]
    other = [(dp, 1 - y, r) for r in rel]
    core_peer, x_peer, y_peer = peer[1], peer[2], other[0]

    def remote(src, dst, ss, rs, dev):
        return pltpu.make_async_remote_copy(src_ref=src, dst_ref=dst, send_sem=ss, recv_sem=rs, device_id=dev, device_id_type=MESH)

    def x_load(h):
        return pltpu.make_async_copy(x_hbm.at[0, pl.ds(h * TOK, TOK)], x_all.at[h, y], ld_sem.at[h])

    tables = [pltpu.make_async_copy(cos_hbm, cos_v, ld_sem.at[NCH]), pltpu.make_async_copy(sin_hbm, sin_v, ld_sem.at[NCH + 1])]

    def qkv_load(r, m):
        src = (wq_hbm, wk_hbm, wv_hbm)[m].at[:, pl.ds(pl.multiple_of(rel[r] * cols, cols), cols)]
        return pltpu.make_async_copy(src, wbuf.at[r * 3 + m], w_sem.at[r * 3 + m])

    def qkv_wait(r, m):
        pltpu.make_async_copy(wq_hbm.at[:, pl.ds(0, cols)], wbuf.at[r * 3 + m], w_sem.at[r * 3 + m]).wait()

    wo_load = pltpu.make_async_copy(wo_hbm, wo_v, w_sem.at[12])

    def gu_load(i, j, w):
        src, dst = ((wg_hbm, wg_v), (wu_hbm, wu_v))[i]
        start = j * FW if isinstance(j, int) else pl.multiple_of(j * FW, FW)
        return pltpu.make_async_copy(src.at[:, pl.ds(start, w)], dst.at[:, pl.ds(start, w)], w_sem.at[16 + i * 8 + j])

    def down_load(j, nh, w):
        start = j * FW if isinstance(j, int) else pl.multiple_of(j * FW, FW)
        return pltpu.make_async_copy(wd_hbm.at[pl.ds(start, w), pl.ds(nh * 512, 512)], wbuf.at[j * 2 + nh, pl.ds(0, w)], w_sem.at[32 + j * 2 + nh])

    def xy_copy(h):
        return remote(x_all.at[h, y], x_all.at[h, y], xy_s.at[h], xy_r.at[h], y_peer)

    def s1_copy(k):
        return remote(st1.at[0], st1.at[k], s1_s.at[k], s1_r.at[k], peer[k] if k < 4 else other[k - 4])

    def seq_rows(s):
        return pl.ds(pl.multiple_of(s * TOK, TOK), TOK)

    def part_rows(part):
        return seq_rows(y if part == 0 else 1 - y)

    def d_copy(h, z, m=None, part=None):
        i = (h * 2 + z) * 3 + (0 if m is None else m)
        sl = pl.ds(i, 3) if m is None else i
        src, dst = (d_send.at[sl], d_recv.at[sl]) if part is None else (d_send.at[sl, part_rows(part)], d_recv.at[sl, part_rows(part)])
        k = 6 * NCH if part == 1 else i
        return remote(src, dst, d_s.at[k], d_r.at[k], core_peer)

    def x_copy(h, m=None, part=None):
        i = h * 3 + (0 if m is None else m)
        k = h * 6 + (0 if m is None else m)
        ssl, dsl = (pl.ds(k, 3), pl.ds(i, 3)) if m is None else (k, i)
        src, dst = (d_recv.at[ssl], x_recv.at[dsl]) if part is None else (d_recv.at[ssl, part_rows(part)], x_recv.at[dsl, part_rows(part)])
        n = 3 * NCH if part == 1 else i
        return remote(src, dst, x_s.at[n], x_r.at[n], x_peer)

    def o_copy(h, kind):
        slot = (t, t, rel[2])[kind]
        i = h * 3 + kind
        ref = o_all.at[h, slot]
        return remote(ref, ref, o_s.at[i], o_r.at[i], (core_peer, x_peer, core_peer)[kind])

    def p_copy(h, nh):
        cl = pl.ds(nh * 512, 512)
        return remote(p_send.at[h, :, cl], p_recv.at[h, :, cl], p_s.at[h * 2 + nh], p_r.at[h * 2 + nh], y_peer)

    def s2_copy(h, k):
        i = h * 4 + k
        return remote(st2.at[h, 0], st2.at[h, k], s2_s.at[i], s2_r.at[i], peer[k])

    def piece(h, j):
        start = sum(PIECES[h][:j])
        return start, PIECES[h][j]

    def g_copy(h, j):
        cl = pl.ds(*piece(h, j))
        i = h * 4 + j
        return remote(g_send.at[h % 2, :, :, cl], g_recv.at[h, :, :, cl], g_s.at[i], g_r.at[i], core_peer)

    def gx_copy(h, j):
        cl = pl.ds(*piece(h, j))
        i = h * 4 + j
        return remote(g_recv.at[h, :, pl.ds(0, SUB), cl], gx_recv.at[h, :, :, cl], gx_s.at[i], gx_r.at[i], x_peer)

    def a_copy(h, j, kind):
        own = c * 2 + xc
        direct = kind == 2 and piece(h, j)[1] < FW
        slot = own if direct else (own, own, c * 2 + 1 - xc)[kind]
        i = (h * 4 + j) * 3 + kind
        ref = a_all.at[h, slot, :, pl.ds(*piece(h, j))]
        return remote(ref, ref, a_s.at[i], a_r.at[i], peer[3] if direct else (core_peer, x_peer, core_peer)[kind])

    def f_copy(h):
        return remote(f_send.at[h], f_recv.at[h], f_s.at[h], f_r.at[h], y_peer)

    lane = lax.broadcasted_iota(jnp.int32, (128, 128), 1)
    sublane = lax.broadcasted_iota(jnp.int32, (128, 128), 0)

    def local_stats(v):
        s = jnp.sum(v, axis=1, keepdims=True)
        q = jnp.sum(v * v, axis=1, keepdims=True)
        n = v.shape[0]
        m = jnp.where(lane[0:n] == 0, s, jnp.where(lane[0:n] == 1, q, 0.0))
        if n < 128:
            m = jnp.concatenate([m, jnp.zeros((128 - n, 128), F32)], axis=0)
        return m.T[0:2]

    def moments(total):
        mean = total[0:1] / full_width
        var = total[1:2] / full_width - mean * mean
        rstd = lax.rsqrt(var + EPS)
        m = jnp.where(sublane == 0, mean, jnp.where(sublane == 1, rstd, 0.0)).T
        return m[:, 0:1], m[:, 1:2]

    def x_own(h, s):
        return x_all[h, s].astype(F32)

    for h in range(NCH):
        x_load(h).start()
    for r in (3, 2, 1, 0):
        for m in range(3):
            qkv_load(r, m).start()
    for tb in tables:
        tb.start()
    barrier = pltpu.get_barrier_semaphore()
    for dev in peer[1:] + other:
        pl.semaphore_signal(barrier, inc=1, device_id=dev, device_id_type=MESH)
    for h in range(NCH):
        x_load(h).wait()
    st1[0] = local_stats(jnp.concatenate([x_own(h, y) for h in range(NCH)], axis=0))
    pl.semaphore_wait(barrier, 7)
    for k in range(1, 8):
        s1_copy(k).start()
    for h in range(NCH):
        xy_copy(h).start()
    wo_load.start()
    for k in range(1, 4):
        s1_copy(k).wait_recv()
    mean_o, rstd_o = moments((st1[0] + st1[1]) + (st1[2] + st1[3]))

    def norm_rows(h, s, mean, rstd):
        sl = slice(h * TOK, (h + 1) * TOK)
        n = ((x_own(h, s) - mean[sl]) * rstd[sl]).astype(BF)
        n_buf[h, pl.ds(pl.multiple_of(s * TOK, TOK), TOK)] = n

    first_parts = [(0, 0), (1, 0), (2, 0), (None, 1)]

    def norm_chunk(h):
        norm_rows(h, y, mean_o, rstd_o)
        xy_copy(h).wait_recv()
        norm_rows(h, 1 - y, *other_moments)

    def qkv_give(h, z):
        for m in range(3):
            d_send[(h * 2 + z) * 3 + m] = dot(n_buf[h], wbuf[(3 - 2 * z) * 3 + m]).astype(BF)
        d_copy(h, z).start()

    def qkv_take(h, z):
        d_copy(h, z).wait_recv()
        for m in range(3):
            i = (h * 2 + z) * 3 + m
            d_recv[i] = (dot(n_buf[h], wbuf[(2 - 2 * z) * 3 + m]) + d_recv[i].astype(F32)).astype(BF)

    def step_qa(h, _):
        if h > 0:
            norm_chunk(h)
            qkv_give(h, 0)
            return
        norm_rows(0, y, mean_o, rstd_o)
        rows = part_rows(0)

        def give(m):
            qkv_wait(3, m)
            d_send[m, rows] = dot(n_buf[0, rows], wbuf[9 + m]).astype(BF)
            d_copy(0, 0, m, 0).start()

        def take(m):
            qkv_wait(2, m)
            own = dot(n_buf[0, rows], wbuf[6 + m])
            d_copy(0, 0, m, 0).wait_recv()
            d_recv[m, rows] = (own + d_recv[m, rows].astype(F32)).astype(BF)
            x_copy(0, m, 0).start()

        give(0)
        give(1)
        take(0)
        give(2)
        take(1)
        take(2)

    def step_qb(h, _):
        if h > 0:
            qkv_take(h, 0)
            return
        for k in range(4, 8):
            s1_copy(k).wait_recv()
        other_moments.extend(moments((st1[4] + st1[5]) + (st1[6] + st1[7])))
        xy_copy(0).wait_recv()
        norm_rows(0, 1 - y, *other_moments)
        rows = part_rows(1)
        for m in range(3):
            d_send[m, rows] = dot(n_buf[0, rows], wbuf[9 + m]).astype(BF)
        d_copy(0, 0, None, 1).start()

    def step_qx(h, _):
        rows = part_rows(1)
        d_copy(0, 0, None, 1).wait_recv()
        for m in range(3):
            d_recv[m, rows] = (dot(n_buf[0, rows], wbuf[6 + m]) + d_recv[m, rows].astype(F32)).astype(BF)
        x_copy(0, None, 1).start()

    def step_qg(h, _):
        if h == 0:
            for m in range(3):
                qkv_wait(1, m)
        qkv_give(h, 1)

    def step_qs(h, _):
        if h > 0:
            x_copy(h).start()

    def step_qc(h, _):
        if h == 0:
            for m in range(3):
                qkv_wait(0, m)
        qkv_take(h, 1)
        if h == 0:
            for j in range(n_full + 1):
                for i in range(2):
                    gu_load(i, j, FW if j < n_full else last_w).start()
        if h == NCH - 1:
            for j in range(n_full + 1):
                for nh in range(2):
                    down_load(j, nh, FW if j < n_full else last_w).start()

    def rotate(v, cos2, sin2):
        f = v.astype(F32)
        return (f * cos2 + pltpu.roll(f, HEAD_DIM // 2, 1) * sin2).astype(BF)

    def step_at(h, _):
        for m, part in first_parts if h == 0 else ((None, None),):
            x_copy(h, m, part).wait_recv()
        if h == 0:
            for tb in tables:
                tb.wait()

        def final(m):
            return (d_recv[h * 6 + 3 + m].astype(F32) + x_recv[h * 3 + m].astype(F32)).astype(BF)

        sl = slice(h * TOK, (h + 1) * TOK)
        n_keys = (h + 1) * TOK
        cos2 = jnp.concatenate([cos_v[sl], cos_v[sl]], axis=0)
        sin2 = jnp.concatenate([sin_v[sl], sin_v[sl]], axis=0)
        q, k, v = final(0), final(1), final(2)
        for s in range(2):
            v_buf[s, sl] = v[s * TOK:(s + 1) * TOK]
        heads = [slice(hd * HEAD_DIM, (hd + 1) * HEAD_DIM) for hd in range(cols // HEAD_DIM)]
        blocks = [(hd, s) for hd in range(len(heads)) for s in range(2)]
        qr = [rotate(q[:, cl], cos2, sin2) for cl in heads]
        kr = [rotate(k[:, cl], cos2, sin2) for cl in heads]
        for hd, s in blocks:
            k_buf[s, sl, heads[hd]] = kr[hd][s * TOK:(s + 1) * TOK]
        scores = jnp.concatenate(
            [dot_t(qr[hd][s * TOK:(s + 1) * TOK], k_buf[s, 0:n_keys, heads[hd]]) for hd, s in blocks], axis=0
        ) * (HEAD_DIM ** -0.5)
        q_pos = h * TOK + lax.rem(lax.broadcasted_iota(jnp.int32, scores.shape, 0), TOK)
        k_pos = lax.broadcasted_iota(jnp.int32, scores.shape, 1)
        scores = jnp.where(q_pos >= k_pos, scores, -1e30)
        e = jnp.exp(scores - jnp.max(scores, axis=1, keepdims=True))
        prob = (e / jnp.sum(e, axis=1, keepdims=True)).astype(BF)
        for i, (hd, s) in enumerate(blocks):
            o = dot(prob[i * TOK:(i + 1) * TOK], v_buf[s, 0:n_keys, heads[hd]])
            o_all[h, t, s * TOK:(s + 1) * TOK, heads[hd]] = o.astype(BF)
        o_copy(h, 1).start()
        o_copy(h, 0).start()

    def step_ro(h, _):
        o_copy(h, 1).wait_recv()
        o_copy(h, 2).start()

    def step_pr(h, _):
        if first_time("wo"):
            wo_load.wait()
        o_copy(h, 0).wait_recv()
        o_copy(h, 2).wait_recv()
        for nh in range(2):
            cl = slice(nh * 512, (nh + 1) * 512)
            res = jnp.zeros((ROWS, 512), F32)
            for b in range(4):
                res = res + dot(o_all[h, b], wo_v[b * cols:(b + 1) * cols, cl])
            p_send[h, :, cl] = res.astype(BF)
            p_copy(h, nh).start()

    def step_re(h, _):
        for nh in range(2):
            p_copy(h, nh).wait_recv()
        attn = (p_send[h].astype(F32) + p_recv[h].astype(F32)).astype(BF).astype(F32)
        xv = jnp.concatenate([x_own(h, 0), x_own(h, 1)], axis=0)
        hv = (xv + attn).astype(BF)
        h_buf[h] = hv
        st2[h, 0] = local_stats(hv.astype(F32))
        for k in range(1, 4):
            s2_copy(h, k).start()

    def step_n2(h, _):
        for k in range(1, 4):
            s2_copy(h, k).wait_recv()
        mean, rstd = moments((st2[h, 0] + st2[h, 1]) + (st2[h, 2] + st2[h, 3]))
        n = ((h_buf[h].astype(F32) - mean[0:ROWS]) * rstd[0:ROWS]).astype(BF)
        for b in range(4):
            e_c = c if b // 2 == 1 else 1 - c
            e_x = xc if b % 2 == 1 else 1 - xc
            n_buf[h, pl.ds(pl.multiple_of(2 * SUB * e_c + SUB * e_x, SUB), SUB)] = n[b * SUB:(b + 1) * SUB]

    def steps(h, j, body):
        start, w = piece(h, j)
        lo, n = start // FW, w // FW
        if n <= 3:
            for kb in range(lo, lo + n):
                body(kb, FW)
        else:
            def step(kb, carry):
                body(kb, FW)
                return carry

            lax.fori_loop(lo, lo + n, step, 0)
        if w % FW:
            body(lo + n, w % FW)

    def step_gm(h, j):
        if first_time("gu"):
            for kb in range(n_full + 1):
                for i in range(2):
                    gu_load(i, kb, FW if kb < n_full else last_w).wait()
        if h >= 2 and j == 0:
            for k in range(len(PIECES[h - 2])):
                g_copy(h - 2, k).wait_send()
        slot = own_slot[h, j]
        start = piece(h, j)[0]

        def body(kb, w):
            for i, wv in enumerate((wg_v, wu_v)):
                for n0 in range(0, w, 512):
                    nw = min(512, w - n0)
                    col = kb * FW + n0
                    if not isinstance(col, int):
                        col = pl.multiple_of(col, 512)
                    res = dot(n_buf[h], wv[:, pl.ds(col, nw)])
                    g_send[h % 2, i, :, pl.ds(col, nw)] = res[0:2 * SUB].astype(BF)
                    g_own[slot, i, :, pl.ds(col - start, nw)] = res[2 * SUB:ROWS]

        steps(h, j, body)
        g_copy(h, j).start()

    def step_ga(h, j):
        slot = own_slot[h, j]
        start, w = piece(h, j)
        cl = slice(start, start + w)
        g_copy(h, j).wait_recv()
        for k in range(2):
            g_recv[h, k, :, cl] = (g_own[slot, k, :, 0:w] + g_recv[h, k, :, cl].astype(F32)).astype(BF)
        gx_copy(h, j).start()

    def step_ac(h, j):
        start, w = piece(h, j)
        cl = slice(start, start + w)
        gx_copy(h, j).wait_recv()
        g, u = [
            (g_recv[h, k, SUB:2 * SUB, cl].astype(F32) + gx_recv[h, k, :, cl].astype(F32)).astype(BF).astype(F32)
            for k in range(2)
        ]
        a_all[h, c * 2 + xc, :, cl] = (g * (1.0 / (1.0 + jnp.exp(-g))) * u).astype(BF)
        a_copy(h, j, 1).start()
        if w < FW:
            a_copy(h, j, 2).start()
        a_copy(h, j, 0).start()

    def step_ra(h, j):
        a_copy(h, j, 1).wait_recv()
        if piece(h, j)[1] >= FW:
            a_copy(h, j, 2).start()

    def step_dn(h, j):
        if first_time("down"):
            for kb in range(n_full + 1):
                for nh in range(2):
                    down_load(kb, nh, FW if kb < n_full else last_w).wait()
        a_copy(h, j, 0).wait_recv()
        a_copy(h, j, 2).wait_recv()
        if j == 0:
            acc[h] = jnp.zeros((ROWS, width), F32)

        def body(kb, w):
            col = kb * FW if isinstance(kb, int) else pl.multiple_of(kb * FW, FW)
            lhs = a_all[h, :, :, pl.ds(col, w)].reshape(ROWS, w)
            for nh in range(2):
                acc[h, :, nh * 512:(nh + 1) * 512] += dot(lhs, wbuf[kb * 2 + nh, 0:w])

        steps(h, j, body)

    def step_fi(h, _):
        f_send[h] = acc[h, seq_rows(1 - y)].astype(BF)
        f_copy(h).start()

    def step_ou(h, _):
        own = pl.ds(pl.multiple_of(y * TOK, TOK), TOK)
        f_copy(h).wait_recv()
        mlp = (acc[h, own].astype(BF).astype(F32) + f_recv[h].astype(F32)).astype(BF).astype(F32)
        out_ref[0, h * TOK:(h + 1) * TOK] = (h_buf[h, own].astype(F32) + mlp).astype(BF)

    other_moments = []
    seen = set()

    def first_time(name):
        new = name not in seen
        seen.add(name)
        return new

    own_slot, free = {}, list(range(g_own.shape[0]))
    program = [(w[:2], int(w[2]), int(w[3:] or 0)) for line in ORDER for w in line.split()]
    for name, h, j in program:
        if name == "gm":
            own_slot[h, j] = free.pop(0)
        if name == "ga":
            free.append(own_slot[h, j])
    step_of = dict(qa=step_qa, qb=step_qb, qx=step_qx, qg=step_qg, qs=step_qs, qc=step_qc, at=step_at, ro=step_ro, pr=step_pr, re=step_re, n2=step_n2,
                   gm=step_gm, ga=step_ga, ac=step_ac, ra=step_ra, dn=step_dn, fi=step_fi, ou=step_ou)
    for name, h, j in program:
        step_of[name](h, j)

    for k in range(1, 8):
        s1_copy(k).wait_send()
    for h in range(NCH):
        xy_copy(h).wait_send()
        for m, part in first_parts if h == 0 else ((None, None),):
            d_copy(h, 0, m, part).wait_send()
            x_copy(h, m, part).wait_send()
        d_copy(h, 1).wait_send()
        for m in range(3):
            s2_copy(h, m + 1).wait_send()
            o_copy(h, m).wait_send()
        for nh in range(2):
            p_copy(h, nh).wait_send()
        for j in range(len(PIECES[h])):
            if h >= NCH - 2:
                g_copy(h, j).wait_send()
            gx_copy(h, j).wait_send()
            for kind in range(3):
                a_copy(h, j, kind).wait_send()
        f_copy(h).wait_send()


def solution(mesh):
    act_spec = P(("dp", "ty"), None, "tx")
    col_spec = P("tx", "ty")
    row_spec = P("ty", "tx")

    def layer_fn(x_blk, w_q, w_k, w_v, w_o, w_gate, w_up, w_down):
        seq_len, width = x_blk.shape[1:]
        cols = w_q.shape[1] // 4
        ff = w_gate.shape[1]
        cos_t, sin_t = (jnp.asarray(a) for a in rotary_tables(seq_len))
        dma = pltpu.SemaphoreType.DMA
        vm = pltpu.VMEM
        return pl.pallas_call(
            layer_kernel,
            out_shape=pltpu.VMEM(x_blk.shape, BF),
            in_specs=[pl.BlockSpec(memory_space=pl.ANY)] * 10,
            out_specs=pl.BlockSpec(memory_space=pltpu.VMEM),
            scratch_shapes=[
                vm((12, width, cols), BF),
                vm(w_o.shape, BF),
                vm(w_gate.shape, BF),
                vm(w_up.shape, BF),
                vm((seq_len, HEAD_DIM), F32),
                vm((seq_len, HEAD_DIM), F32),
                vm((NCH, 2, TOK, width), BF),
                vm((NCH, ROWS, width), BF),
                vm((6 * NCH, ROWS, cols), BF),
                vm((6 * NCH, ROWS, cols), BF),
                vm((3 * NCH, ROWS, cols), BF),
                vm((2, seq_len, cols), BF),
                vm((2, seq_len, cols), BF),
                vm((NCH, 4, ROWS, cols), BF),
                vm((NCH, ROWS, width), BF),
                vm((NCH, ROWS, width), BF),
                vm((NCH, ROWS, width), BF),
                vm((2, 2, 2 * SUB, ff), BF),
                vm((NCH, 2, 2 * SUB, ff), BF),
                vm((3, 2, 2 * SUB, max(max(p) for p in PIECES)), F32),
                vm((NCH, 2, SUB, ff), BF),
                vm((NCH, 4, SUB, ff), BF),
                vm((NCH, ROWS, width), F32),
                vm((NCH, TOK, width), BF),
                vm((NCH, TOK, width), BF),
                vm((8, 2, 128), F32),
                vm((NCH, 4, 2, 128), F32),
                dma((NCH + 2,)), dma((48,)),
                *(dma((n,)) for n in (NCH, 8, 6 * NCH + 1, 3 * NCH + 1, 3 * NCH, 2 * NCH, 4 * NCH, 4 * NCH, 4 * NCH, 12 * NCH, NCH) for _ in range(2)),
            ],
            compiler_params=pltpu.CompilerParams(collective_id=0, has_side_effects=True, vmem_limit_bytes=66256896),
            name="layer",
        )(x_blk, w_q, w_k, w_v, w_o, w_gate, w_up, w_down, cos_t, sin_t)

    return jax.shard_map(layer_fn, mesh=mesh, in_specs=(act_spec, col_spec, col_spec, col_spec, row_spec, col_spec, col_spec, row_spec), out_specs=act_spec, check_vma=False)
```
